256 devices in a mesh: depth: 8 (over z), col: 4 (over y), row: 8 (over x, core).
Axes of the slice: x: 4, y: 4, z: 8, core: 2. Of those that a mesh axis runs over, the one named last changes fastest.
Arguments:
- a_mat: bfloat16 [16384, 16384], P('row', 'col')
- b_mat: bfloat16 [16384, 16384], P('row', 'col')
Outputs:
- output: bfloat16 [16384, 16384], P(('row', 'depth'), 'col')
All inputs are finite; a program needn't handle non-finite values.
Results may differ from the reference program's by a relative error of at most 0.001.
Values are sent between devices in bfloat16 or wider.
A program may use at most 768 MiB of HBM per device.

```python
import jax
import jax.numpy as jnp

D = 16384


def setup_inputs(seed: int = 0) -> dict:
    key_a, key_b = jax.random.split(jax.random.key(seed))
    a_mat = jax.random.normal(key_a, (D, D), jnp.float32) + 0.5
    b_mat = (jax.random.normal(key_b, (D, D), jnp.float32) + 2.0 * D ** -0.5) * D ** -0.5
    return {"a_mat": a_mat.astype(jnp.bfloat16), "b_mat": b_mat.astype(jnp.bfloat16)}


def reference(a_mat, b_mat):
    return jnp.dot(a_mat, b_mat, preferred_element_type=jnp.float32).astype(jnp.bfloat16)
```

```python
import functools

import jax
import jax.numpy as jnp
from jax import lax
from jax.experimental import pallas as pl
from jax.experimental.pallas import tpu as pltpu
from jax.sharding import PartitionSpec as P

MESH = pl.DeviceIdType.MESH
NX = 4
NS = 2
ORDER = [(2, 0), (2, 1), (1, 0), (3, 0), (1, 1), (3, 1), (0, 0), (0, 1)]


def chunk_order(nz):
    return sorted(range(nz), key=lambda r: -min(r, nz - r))


def kernel(nz, ny, a_ref, b_ref, o_ref, abuf, bbuf, ro, rn, pbuf, obuf,
           a_sem, s1_send, b_recv, ag_send, fw_send, op_send, op_recv, nb_send, nb_recv, out_send, out_recv):
    z = lax.axis_index("depth")
    y = lax.axis_index("col")
    i = lax.axis_index("row")
    x, c = i // 2, i % 2
    rows, depth_k = abuf.shape
    half_k = depth_k // 2
    quarter = half_k // NX
    width = depth_k // nz
    sub = width // NS
    chunk = rows // nz
    mblk = rows // 4
    order_z = chunk_order(nz)

    def dev(zz, yy, xx, cc):
        return ((zz + nz) % nz, (yy + ny) % ny, 2 * ((xx + NX) % NX) + cc)

    def remote(src, dst, send_sem, recv_sem, device):
        return pltpu.make_async_remote_copy(src_ref=src, dst_ref=dst, send_sem=send_sem, recv_sem=recv_sem,
                                            device_id=device, device_id_type=MESH)

    sibling = dev(z, y, x, 1 - c)

    a_copies = [pltpu.make_async_copy(a_ref.at[pl.ds(m * mblk, mblk)], abuf.at[pl.ds(m * mblk, mblk)], a_sem.at[m])
                for m in range(4)]
    for cp in a_copies:
        cp.start()

    barrier = pltpu.get_barrier_semaphore()
    partners = [sibling]
    partners += [dev(z, y + dy, x + dx, c) for dy in range(ny) for dx in range(NX) if dx or dy]
    partners += [dev(z + r, y, x, c) for r in range(1, nz)]
    for p in partners:
        pl.semaphore_signal(barrier, inc=1, device_id=p, device_id_type=MESH)
    pl.semaphore_wait(barrier, len(partners))

    t_me = (y - x + NX) % NX

    def piece(t, s, lane, q):
        return bbuf.at[t, s, pl.ds(lane * half_k + q * quarter, quarter)]

    def stage1(s, q, local, act):
        src = b_ref.at[pl.ds(q * quarter, quarter), pl.ds(pl.multiple_of(z * width + s * sub, sub), sub)]
        dst, sem = piece(t_me, s, c, q), b_recv.at[t_me, s, c * NX + q]
        if local:
            act(pltpu.make_async_copy(src, dst, sem))
        else:
            act(remote(src, dst, s1_send.at[s, q], sem, dev(z, x, q, c)))

    def own_piece(q):
        return (x == y) & (x == q)

    def stage1_start():
        for s in range(NS):
            for q in range(NX):
                @pl.when(jnp.logical_not(own_piece(q)))
                def _():
                    stage1(s, q, False, lambda cp: cp.start())

                @pl.when(own_piece(q))
                def _():
                    stage1(s, q, True, lambda cp: cp.start())

    def arrived(t, s, lane, q):
        ref = piece(t, s, lane, q)
        remote(ref, ref, fw_send.at[t, s, 0], b_recv.at[t, s, lane * NX + q], sibling).wait_recv()

    def gather_copies(t, s):
        ref = piece(t, s, c, x)
        sem = b_recv.at[t, s, c * NX + x]
        out = [remote(ref, ref, ag_send.at[t, s, d], sem, dev(z, y, x + d, c)) for d in (1, 3, 2)]
        out.append(remote(ref, ref, ag_send.at[t, s, 0], sem, sibling))
        return out

    def gather(t, s):
        arrived(t, s, c, x)
        for cp in gather_copies(t, s):
            cp.start()

    def forward_copies(t, s):
        for d in (1, 3, 2):
            q = (x + d) % NX
            ref = piece(t, s, c, q)
            yield q, remote(ref, ref, fw_send.at[t, s, d - 1], b_recv.at[t, s, c * NX + q], sibling)

    def forward(t, s):
        for q, cp in forward_copies(t, s):
            arrived(t, s, c, q)
            cp.start()

    def matmul(t, s, slot):
        for q in range(NX):
            arrived(t, s, 1 - c, q)

        def body(m, carry):
            r = pl.ds(pl.multiple_of(m * mblk, mblk), mblk)
            pbuf[slot, s, r, :] = jnp.dot(abuf[r, :], bbuf[t, s], preferred_element_type=jnp.float32)
            return carry

        lax.fori_loop(0, 4, body, 0)

    half = rows // 2

    def opposite_copy(s, d):
        return remote(pbuf.at[0, s, pl.ds(d * half, half)], ro.at[d, s], op_send.at[d, s], op_recv.at[d, s],
                      dev(z, y + 1 - 2 * d, x, c))

    def merge(d, s):
        opposite_copy(s, d).wait_recv()

        def body(m, carry):
            r = pl.ds(pl.multiple_of(m * (half // 4), half // 4), half // 4)
            rp = pl.ds(pl.multiple_of(d * half + m * (half // 4), half // 4), half // 4)
            pbuf[1 + d, s, rp, :] = pbuf[1 + d, s, rp, :] + ro[d, s, r, :]
            return carry

        lax.fori_loop(0, 4, body, 0)

    def chunk_rows(r):
        zz = (z + r) % nz
        return pl.ds(pl.multiple_of(zz * chunk, chunk), chunk)

    def neighbour_copy(d, s, r):
        cr = chunk_rows(r)
        return remote(pbuf.at[1 + d, s, cr], rn.at[d, s, cr], nb_send.at[d, s, r], nb_recv.at[d, s, r],
                      dev(z, y + 1 - 2 * d, x, c))

    def send_neighbours(s):
        for r in order_z:
            for d in (0, 1):
                neighbour_copy(d, s, r).start()

    def out_copy(s, r):
        cols = pl.ds(pl.multiple_of(z * width + s * sub, sub), sub)
        if r == 0:
            return pltpu.make_async_copy(obuf.at[s, chunk_rows(0)], o_ref.at[:, cols], out_recv.at[s, 0])
        return remote(obuf.at[s, chunk_rows(r)], o_ref.at[:, cols], out_send.at[s, r], out_recv.at[s, r],
                      dev(z + r, y, x, c))

    def out_arrived(s, r):
        if r == 0:
            out_copy(s, 0).wait()
            return
        src_z = (z - r + nz) % nz
        cols = pl.ds(pl.multiple_of(src_z * width + s * sub, sub), sub)
        remote(obuf.at[s, chunk_rows(r)], o_ref.at[:, cols], out_send.at[s, r], out_recv.at[s, r],
               dev(z + r, y, x, c)).wait_recv()

    def finish(s):
        for r in order_z:
            for d in (0, 1):
                neighbour_copy(d, s, r).wait_recv()
            cr = chunk_rows(r)
            total = pbuf[0, s, cr, :] + rn[0, s, cr, :] + rn[1, s, cr, :]
            obuf[s, cr, :] = total.astype(jnp.bfloat16)
            out_copy(s, r).start()

    slot_of = {2: 0, 1: 1, 3: 2, 0: 0}

    @pl.when(t_me == 2)
    def _():
        stage1_start()

    gather(*ORDER[0])

    @pl.when(t_me != 2)
    def _():
        stage1_start()

    gather(*ORDER[1])
    for cp in a_copies:
        cp.wait()
    for n, (t, s) in enumerate(ORDER):
        forward(t, s)
        if t == 0:
            for d in (0, 1):
                opposite_copy(s, d).wait_send()
        matmul(t, s, slot_of[t])
        if t == 2:
            for d in (0, 1):
                opposite_copy(s, d).start()
        if t == 3:
            merge(0, s)
            merge(1, s)
            send_neighbours(s)
        if n + 2 < len(ORDER):
            gather(*ORDER[n + 2])
    for s in range(NS):
        finish(s)

    for s in range(NS):
        for q in range(NX):
            @pl.when(jnp.logical_not(own_piece(q)))
            def _():
                stage1(s, q, False, lambda cp: cp.wait_send())
    for t, s in ORDER:
        for cp in gather_copies(t, s):
            cp.wait_send()
        for _, cp in forward_copies(t, s):
            cp.wait_send()
    for s in range(NS):
        for r in order_z:
            for d in (0, 1):
                neighbour_copy(d, s, r).wait_send()
            if r:
                out_copy(s, r).wait_send()
            out_arrived(s, r)


def local_product(nz, ny, a_blk, b_blk):
    rows, depth_k = a_blk.shape
    half_k = b_blk.shape[0]
    sub = depth_k // nz // NS
    f32, bf16 = jnp.float32, jnp.bfloat16
    dma = pltpu.SemaphoreType.DMA
    return pl.pallas_call(
        functools.partial(kernel, nz, ny),
        name="stationary_a",
        out_shape=jax.ShapeDtypeStruct((rows // nz, depth_k), bf16),
        in_specs=[pl.BlockSpec(memory_space=pl.ANY)] * 2,
        out_specs=pl.BlockSpec(memory_space=pl.ANY),
        scratch_shapes=[
            pltpu.VMEM((rows, depth_k), bf16),
            pltpu.VMEM((NX, NS, 2 * half_k, sub), bf16),
            pltpu.VMEM((2, NS, rows // 2, sub), f32),
            pltpu.VMEM((2, NS, rows, sub), f32),
            pltpu.VMEM((3, NS, rows, sub), f32),
            pltpu.VMEM((NS, rows, sub), bf16),
            dma((4,)),
            dma((NS, NX)),
            dma((NX, NS, 2 * NX)),
            dma((NX, NS, 4)),
            dma((NX, NS, 3)),
            dma((2, NS)),
            dma((2, NS)),
            dma((2, NS, nz)),
            dma((2, NS, nz)),
            dma((NS, nz)),
            dma((NS, nz)),
        ],
        compiler_params=pltpu.CompilerParams(collective_id=0, has_side_effects=True, vmem_limit_bytes=67043328),
    )(a_blk, b_blk)


def solution(mesh):
    nz, ny = mesh.shape["depth"], mesh.shape["col"]
    return jax.shard_map(
        functools.partial(local_product, nz, ny),
        mesh=mesh,
        in_specs=(P("row", "col"), P("row", "col")),
        out_specs=P(("row", "depth"), "col"),
        check_vma=False,
    )
```

```python
import functools

import jax
import jax.numpy as jnp
from jax import lax
from jax.experimental import pallas as pl
from jax.experimental.pallas import tpu as pltpu
from jax.sharding import PartitionSpec as P

MESH = pl.DeviceIdType.MESH
NX = 4
PIECES = [(2, 0, 4), (2, 4, 4), (2, 8, 8), (1, 0, 8), (3, 0, 8), (1, 8, 8), (3, 8, 8), (0, 0, 16)]
OPPOSITE = [0, 1, 2]
HALVES = [(0, 8), (8, 8)]
SLOT = {2: 0, 1: 1, 3: 2, 0: 0}
SCRIPT = """S2:0 S2:1 S2:2 G0 S1:3 S3:4 G1 L0 R0 L1 R1 O0 G2 C0a L2 R2 C0b O1 C1a S1:5 S3:6 G3 C1b G4 O2 C2a L3 R3 C2b L4 R4 O3 S0:7
C3a G5 C3b O4 C4a G6 C4b M0 L5 R5 L6 R6 O5 C5a G7 C5b O6 C6a L7 R7 C6b M1 O7 C7a C7b F0 F1"""


def chunk_order(nz):
    return sorted(range(nz), key=lambda r: -min(r, nz - r))


def kernel(nz, ny, a_ref, b_ref, o_ref, abuf, bbuf, ro, rn, pbuf, obuf,
           a_sem, s1_send, b_recv, ag_send, fw_send, op_send, op_recv, nb_send, nb_recv, out_send, out_recv):
    z = lax.axis_index("depth")
    y = lax.axis_index("col")
    i = lax.axis_index("row")
    x, c = i // 2, i % 2
    rows, depth_k = abuf.shape
    half_k = depth_k // 2
    quarter = half_k // NX
    width = depth_k // nz
    unit = width // 16
    chunk = rows // nz
    mblk = rows // 4
    half = rows // 2
    order_z = chunk_order(nz)

    def dev(zz, yy, xx, cc):
        return ((zz + nz) % nz, (yy + ny) % ny, 2 * ((xx + NX) % NX) + cc)

    def remote(src, dst, send_sem, recv_sem, device):
        return pltpu.make_async_remote_copy(src_ref=src, dst_ref=dst, send_sem=send_sem, recv_sem=recv_sem,
                                            device_id=device, device_id_type=MESH)

    sibling = dev(z, y, x, 1 - c)
    left, right = dev(z, y, x - 1, c), dev(z, y, x + 1, c)

    a_copies = [pltpu.make_async_copy(a_ref.at[pl.ds(m * mblk, mblk)], abuf.at[pl.ds(m * mblk, mblk)], a_sem.at[m])
                for m in range(4)]
    for cp in a_copies:
        cp.start()

    barrier = pltpu.get_barrier_semaphore()
    partners = [sibling]
    partners += [dev(z, y + dy, x + dx, c) for dy in range(ny) for dx in range(NX) if dx or dy]
    partners += [dev(z + r, y, x, c) for r in range(1, nz)]
    for p in partners:
        pl.semaphore_signal(barrier, inc=1, device_id=p, device_id_type=MESH)
    pl.semaphore_wait(barrier, len(partners))

    t_me = (y - x + NX) % NX

    def columns(n):
        return pl.ds(PIECES[n][1] * unit, PIECES[n][2] * unit)

    def stage1(n, q, local, act):
        t, first, wide = PIECES[n]
        cols = pl.ds(pl.multiple_of(z * width + first * unit, 4 * unit), wide * unit)
        src = b_ref.at[pl.ds(q * quarter, quarter), cols]
        dst = bbuf.at[t, pl.ds(pl.multiple_of(c * half_k + q * quarter, quarter), quarter), columns(n)]
        sem = b_recv.at[n, c * 5]
        if local:
            act(pltpu.make_async_copy(src, dst, sem))
        else:
            act(remote(src, dst, s1_send.at[n, q], sem, dev(z, x, q, c)))

    def stage1_all(n, act, with_local):
        for q in range(NX):
            if PIECES[n][0]:
                stage1(n, q, False, act)
            else:
                @pl.when(x != q)
                def _():
                    stage1(n, q, False, act)

                if with_local:
                    @pl.when(x == q)
                    def _():
                        stage1(n, q, True, act)

    def part(n, lane, k):
        q = (x + (0, 3, 1, 2, 2)[k]) % NX
        start, size = lane * half_k + q * quarter, quarter
        if k >= 3:
            size = quarter // 2
            start = start + (k - 3) * size
        return bbuf.at[PIECES[n][0], pl.ds(pl.multiple_of(start, size), size), columns(n)]

    def arrived(n, lane, k):
        ref = part(n, lane, k)
        remote(ref, ref, fw_send.at[n, 0], b_recv.at[n, lane * 5 + k], sibling).wait_recv()

    def to_sibling(n, k):
        ref = part(n, c, k)
        return remote(ref, ref, fw_send.at[n, k], b_recv.at[n, c * 5 + k], sibling)

    def to_side(n, which):
        if which < 2:
            ref = part(n, c, 0)
        else:
            q = (x + (3, 1)[which - 2]) % NX
            size = quarter // 2
            start = c * half_k + q * quarter + (which - 2) * size
            ref = bbuf.at[PIECES[n][0], pl.ds(pl.multiple_of(start, size), size), columns(n)]
        return remote(ref, ref, ag_send.at[n, which], b_recv.at[n, c * 5 + 1 + which], (right, left)[which % 2])

    def pass_own(n):
        arrived(n, c, 0)
        to_side(n, 0).start()
        to_side(n, 1).start()
        to_sibling(n, 0).start()

    def pass_side(n, k):
        arrived(n, c, k)
        to_side(n, k + 1).start()
        to_sibling(n, k).start()

    def pass_far(n):
        for k in (3, 4):
            arrived(n, c, k)
            to_sibling(n, k).start()

    def opposite_copy(n, d):
        return remote(pbuf.at[0, pl.ds(d * half, half), columns(n)], ro.at[d, :, columns(n)],
                      op_send.at[n, d], op_recv.at[n, d], dev(z, y + 1 - 2 * d, x, c))

    def half_matmul(n, h):
        t = PIECES[n][0]
        if h == 0:
            for k in range(5):
                arrived(n, 1 - c, k)
            if n == 0:
                for cp in a_copies:
                    cp.wait()
            if t == 0:
                for m in OPPOSITE:
                    for d in (0, 1):
                        opposite_copy(m, d).wait_send()

        def body(m, carry):
            r = pl.ds(pl.multiple_of(m * mblk, mblk), mblk)
            pbuf[SLOT[t], r, columns(n)] = jnp.dot(abuf[r, :], bbuf[t, :, columns(n)],
                                                   preferred_element_type=jnp.float32)
            return carry

        lax.fori_loop(2 * h, 2 * h + 2, body, 0)
        if t == 2:
            opposite_copy(n, h).start()

    def chunk_rows(r):
        zz = (z + r) % nz
        return pl.ds(pl.multiple_of(zz * chunk, chunk), chunk)

    def half_columns(s):
        return pl.ds(HALVES[s][0] * unit, HALVES[s][1] * unit)

    def neighbour_copy(d, s, r):
        cr, cols = chunk_rows(r), half_columns(s)
        return remote(pbuf.at[1 + d, cr, cols], rn.at[d, cr, cols], nb_send.at[d, s, r], nb_recv.at[d, s, r],
                      dev(z, y + 1 - 2 * d, x, c))

    def merge(s):
        first, wide = HALVES[s]
        cols = half_columns(s)
        for n in OPPOSITE:
            if first <= PIECES[n][1] < first + wide:
                for d in (0, 1):
                    opposite_copy(n, d).wait_recv()
        for d in (0, 1):
            def body(m, carry):
                r = pl.ds(pl.multiple_of(m * (half // 4), half // 4), half // 4)
                rp = pl.ds(pl.multiple_of(d * half + m * (half // 4), half // 4), half // 4)
                pbuf[1 + d, rp, cols] = pbuf[1 + d, rp, cols] + ro[d, r, cols]
                return carry

            lax.fori_loop(0, 4, body, 0)
        for r in order_z:
            for d in (0, 1):
                neighbour_copy(d, s, r).start()

    def out_columns(zz, s):
        return pl.ds(pl.multiple_of(zz * width + HALVES[s][0] * unit, 8 * unit), HALVES[s][1] * unit)

    def out_copy(s, r):
        src = obuf.at[chunk_rows(r), half_columns(s)]
        if r == 0:
            return pltpu.make_async_copy(src, o_ref.at[:, out_columns(z, s)], out_recv.at[s, 0])
        return remote(src, o_ref.at[:, out_columns(z, s)], out_send.at[s, r], out_recv.at[s, r], dev(z + r, y, x, c))

    def out_arrived(s, r):
        if r == 0:
            out_copy(s, 0).wait()
        else:
            remote(obuf.at[chunk_rows(r), half_columns(s)], o_ref.at[:, out_columns((z - r + nz) % nz, s)],
                   out_send.at[s, r], out_recv.at[s, r], dev(z + r, y, x, c)).wait_recv()

    def finish(s):
        cols = half_columns(s)
        for r in order_z:
            for d in (0, 1):
                neighbour_copy(d, s, r).wait_recv()
            cr = chunk_rows(r)
            total = pbuf[0, cr, cols] + rn[0, cr, cols] + rn[1, cr, cols]
            obuf[cr, cols] = total.astype(jnp.bfloat16)
            out_copy(s, r).start()

    for item in SCRIPT.split():
        op, rest = item[0], item[1:]
        if op == "S":
            t, n = (int(v) for v in rest.split(":"))

            @pl.when(t_me == t)
            def _():
                stage1_all(n, lambda cp: cp.start(), True)
        elif op == "G":
            pass_own(int(rest))
        elif op == "L":
            pass_side(int(rest), 1)
        elif op == "R":
            pass_side(int(rest), 2)
        elif op == "O":
            pass_far(int(rest))
        elif op == "C":
            half_matmul(int(rest[0]), "ab".index(rest[1]))
        elif op == "M":
            merge(int(rest))
        elif op == "F":
            finish(int(rest))

    for n in range(len(PIECES)):
        @pl.when(t_me == PIECES[n][0])
        def _():
            stage1_all(n, lambda cp: cp.wait_send(), False)

        for which in range(4):
            to_side(n, which).wait_send()
        for k in range(5):
            to_sibling(n, k).wait_send()
    for s in range(len(HALVES)):
        for r in order_z:
            for d in (0, 1):
                neighbour_copy(d, s, r).wait_send()
            if r:
                out_copy(s, r).wait_send()
            out_arrived(s, r)


def local_product(nz, ny, a_blk, b_blk):
    rows, depth_k = a_blk.shape
    half_k = b_blk.shape[0]
    width = depth_k // nz
    f32, bf16 = jnp.float32, jnp.bfloat16
    dma = pltpu.SemaphoreType.DMA
    n = len(PIECES)
    return pl.pallas_call(
        functools.partial(kernel, nz, ny),
        name="stationary_a",
        out_shape=jax.ShapeDtypeStruct((rows // nz, depth_k), bf16),
        in_specs=[pl.BlockSpec(memory_space=pl.ANY)] * 2,
        out_specs=pl.BlockSpec(memory_space=pl.ANY),
        scratch_shapes=[
            pltpu.VMEM((rows, depth_k), bf16),
            pltpu.VMEM((NX, 2 * half_k, width), bf16),
            pltpu.VMEM((2, rows // 2, width), f32),
            pltpu.VMEM((2, rows, width), f32),
            pltpu.VMEM((3, rows, width), f32),
            pltpu.VMEM((rows, width), bf16),
            dma((4,)),
            dma((n, NX)),
            dma((n, 10)),
            dma((n, 4)),
            dma((n, 5)),
            dma((n, 2)),
            dma((n, 2)),
            dma((2, len(HALVES), nz)),
            dma((2, len(HALVES), nz)),
            dma((len(HALVES), nz)),
            dma((len(HALVES), nz)),
        ],
        compiler_params=pltpu.CompilerParams(collective_id=0, has_side_effects=True, vmem_limit_bytes=67043328),
    )(a_blk, b_blk)


def solution(mesh):
    nz, ny = mesh.shape["depth"], mesh.shape["col"]
    return jax.shard_map(
        functools.partial(local_product, nz, ny),
        mesh=mesh,
        in_specs=(P("row", "col"), P("row", "col")),
        out_specs=P(("row", "depth"), "col"),
        check_vma=False,
    )
```

```python
import functools

import jax
import jax.numpy as jnp
from jax import lax
from jax.experimental import pallas as pl
from jax.experimental.pallas import tpu as pltpu
from jax.sharding import PartitionSpec as P

MESH = pl.DeviceIdType.MESH
NX = 4
PIECES = [(2, 0, True), (1, 0, True), (3, 0, True), (2, 1, False), (1, 1, False), (3, 1, False),
          (2, 2, False), (1, 2, False), (3, 2, False), (0, 3, False)]
GROUPS = [(0, 4), (4, 4), (8, 8), (0, 16)]
NG = 3
SLOT = {2: 0, 1: 1, 3: 2, 0: 0}
SCRIPT = """S0 G0 G1 G2 S1 L0 R0 O0 C0a L1 R1 C0b L2 R2 O1 C1a G3 O2 C1b G4 G5 C2a S2 L3 R3 C2b M0
L4 R4 O3 C3a L5 R5 C3b O4 C4a O5 G6 C4b G7 G8 C5a S3 L6 R6 C5b M1
L7 R7 O6 C6a L8 R8 C6b O7 C7a O8 G9 C7b C8a L9 C8b M2 R9 O9 C9a C9b F0 F1 F2"""


def chunk_order(nz):
    return sorted(range(nz), key=lambda r: -min(r, nz - r))


def kernel(nz, ny, a_ref, b_ref, o_ref, abuf, bbuf, ro, rn, pbuf, obuf,
           a_sem, s1_send, b_recv, ag_send, fw_send, op_send, op_recv, nb_send, nb_recv, out_send, out_recv):
    z = lax.axis_index("depth")
    y = lax.axis_index("col")
    i = lax.axis_index("row")
    x, c = i // 2, i % 2
    rows, depth_k = abuf.shape
    half_k = depth_k // 2
    quarter = half_k // NX
    width = depth_k // nz
    unit = width // 16
    chunk = rows // nz
    mblk = rows // 4
    half = rows // 2
    order_z = chunk_order(nz)

    def dev(zz, yy, xx, cc):
        return ((zz + nz) % nz, (yy + ny) % ny, 2 * ((xx + NX) % NX) + cc)

    def remote(src, dst, send_sem, recv_sem, device):
        return pltpu.make_async_remote_copy(src_ref=src, dst_ref=dst, send_sem=send_sem, recv_sem=recv_sem,
                                            device_id=device, device_id_type=MESH)

    sibling = dev(z, y, x, 1 - c)
    left, right, far = dev(z, y, x - 1, c), dev(z, y, x + 1, c), dev(z, y, x + 2, c)

    a_copies = [pltpu.make_async_copy(a_ref.at[pl.ds(m * mblk, mblk)], abuf.at[pl.ds(m * mblk, mblk)], a_sem.at[m])
                for m in range(4)]
    for cp in a_copies:
        cp.start()

    barrier = pltpu.get_barrier_semaphore()
    partners = [sibling]
    partners += [dev(z, y + dy, x + dx, c) for dy in range(ny) for dx in range(NX) if dx or dy]
    partners += [dev(z + r, y, x, c) for r in range(1, nz)]
    for p in partners:
        pl.semaphore_signal(barrier, inc=1, device_id=p, device_id_type=MESH)
    pl.semaphore_wait(barrier, len(partners))

    t_me = (y - x + NX) % NX

    def group_columns(s):
        return pl.ds(GROUPS[s][0] * unit, GROUPS[s][1] * unit)

    def columns(n):
        return group_columns(PIECES[n][1])

    def stage1(n, q, local, act):
        t = PIECES[n][0]
        first, wide = GROUPS[PIECES[n][1]]
        cols = pl.ds(pl.multiple_of(z * width + first * unit, 4 * unit), wide * unit)
        src = b_ref.at[pl.ds(q * quarter, quarter), cols]
        dst = bbuf.at[t, pl.ds(pl.multiple_of(c * half_k + q * quarter, quarter), quarter), columns(n)]
        sem = b_recv.at[n, c * 5]
        if local:
            act(pltpu.make_async_copy(src, dst, sem))
        else:
            act(remote(src, dst, s1_send.at[n, q], sem, dev(z, x, q, c)))

    def stage1_all(n, act, with_local):
        for q in range(NX):
            if PIECES[n][0]:
                stage1(n, q, False, act)
            else:
                @pl.when(x != q)
                def _():
                    stage1(n, q, False, act)

                if with_local:
                    @pl.when(x == q)
                    def _():
                        stage1(n, q, True, act)

    def part(n, lane, k):
        q = (x + (0, 3, 1, 2, 2)[k]) % NX
        start, size = lane * half_k + q * quarter, quarter
        if k >= 3:
            size = quarter // 2
            start = start + (k - 3) * size
        return bbuf.at[PIECES[n][0], pl.ds(pl.multiple_of(start, size), size), columns(n)]

    def arrived(n, lane, k):
        ref = part(n, lane, k)
        remote(ref, ref, fw_send.at[n, 0], b_recv.at[n, lane * 5 + k], sibling).wait_recv()

    def to_sibling(n, k):
        ref = part(n, c, k)
        return remote(ref, ref, fw_send.at[n, k], b_recv.at[n, c * 5 + k], sibling)

    def to_side(n, which):
        straight = PIECES[n][2]
        if which < 2:
            ref = part(n, c, 0)
        else:
            q = x if straight else (x + (3, 1)[which - 2]) % NX
            size = quarter // 2
            start = c * half_k + q * quarter + (which - 2) * size
            ref = bbuf.at[PIECES[n][0], pl.ds(pl.multiple_of(start, size), size), columns(n)]
        target = far if straight and which >= 2 else (right, left)[which % 2]
        return remote(ref, ref, ag_send.at[n, which], b_recv.at[n, c * 5 + 1 + which], target)

    def pass_own(n):
        arrived(n, c, 0)
        for which in (2, 3, 0, 1) if PIECES[n][2] else (0, 1):
            to_side(n, which).start()
        to_sibling(n, 0).start()

    def pass_side(n, k):
        arrived(n, c, k)
        if not PIECES[n][2]:
            to_side(n, k + 1).start()
        to_sibling(n, k).start()

    def pass_far(n):
        for k in (3, 4):
            arrived(n, c, k)
            to_sibling(n, k).start()

    def opposite_copy(s, d):
        return remote(pbuf.at[0, pl.ds(d * half, half), group_columns(s)], ro.at[d, :, group_columns(s)],
                      op_send.at[s, d], op_recv.at[s, d], dev(z, y + 1 - 2 * d, x, c))

    def half_matmul(n, h):
        t = PIECES[n][0]
        if h == 0:
            for k in range(5):
                arrived(n, 1 - c, k)
            if n == 0:
                for cp in a_copies:
                    cp.wait()
            if t == 0:
                for m in range(NG):
                    for d in (0, 1):
                        opposite_copy(m, d).wait_send()

        def body(m, carry):
            r = pl.ds(pl.multiple_of(m * mblk, mblk), mblk)
            pbuf[SLOT[t], r, columns(n)] = jnp.dot(abuf[r, :], bbuf[t, :, columns(n)],
                                                   preferred_element_type=jnp.float32)
            return carry

        lax.fori_loop(2 * h, 2 * h + 2, body, 0)
        if t == 2:
            opposite_copy(PIECES[n][1], h).start()

    def chunk_rows(r):
        zz = (z + r) % nz
        return pl.ds(pl.multiple_of(zz * chunk, chunk), chunk)

    def neighbour_copy(d, s, r):
        cr, cols = chunk_rows(r), group_columns(s)
        return remote(pbuf.at[1 + d, cr, cols], rn.at[d, cr, cols], nb_send.at[d, s, r], nb_recv.at[d, s, r],
                      dev(z, y + 1 - 2 * d, x, c))

    def merge(s):
        cols = group_columns(s)
        for d in (0, 1):
            opposite_copy(s, d).wait_recv()
        for d in (0, 1):
            def body(m, carry):
                r = pl.ds(pl.multiple_of(m * (half // 4), half // 4), half // 4)
                rp = pl.ds(pl.multiple_of(d * half + m * (half // 4), half // 4), half // 4)
                pbuf[1 + d, rp, cols] = pbuf[1 + d, rp, cols] + ro[d, r, cols]
                return carry

            lax.fori_loop(0, 4, body, 0)
        for r in order_z:
            for d in (0, 1):
                neighbour_copy(d, s, r).start()

    def out_columns(zz, s):
        return pl.ds(pl.multiple_of(zz * width + GROUPS[s][0] * unit, 4 * unit), GROUPS[s][1] * unit)

    def out_copy(s, r):
        src = obuf.at[chunk_rows(r), group_columns(s)]
        if r == 0:
            return pltpu.make_async_copy(src, o_ref.at[:, out_columns(z, s)], out_recv.at[s, 0])
        return remote(src, o_ref.at[:, out_columns(z, s)], out_send.at[s, r], out_recv.at[s, r], dev(z + r, y, x, c))

    def out_arrived(s, r):
        if r == 0:
            out_copy(s, 0).wait()
        else:
            remote(obuf.at[chunk_rows(r), group_columns(s)], o_ref.at[:, out_columns((z - r + nz) % nz, s)],
                   out_send.at[s, r], out_recv.at[s, r], dev(z + r, y, x, c)).wait_recv()

    def finish(s):
        cols = group_columns(s)
        for r in order_z:
            for d in (0, 1):
                neighbour_copy(d, s, r).wait_recv()
            cr = chunk_rows(r)
            total = pbuf[0, cr, cols] + rn[0, cr, cols] + rn[1, cr, cols]
            obuf[cr, cols] = total.astype(jnp.bfloat16)
            out_copy(s, r).start()

    for item in SCRIPT.split():
        op, rest = item[0], item[1:]
        if op == "S":
            for n in range(len(PIECES)):
                if PIECES[n][1] == int(rest):
                    @pl.when(t_me == PIECES[n][0])
                    def _():
                        stage1_all(n, lambda cp: cp.start(), True)
        elif op == "G":
            pass_own(int(rest))
        elif op == "L":
            pass_side(int(rest), 1)
        elif op == "R":
            pass_side(int(rest), 2)
        elif op == "O":
            pass_far(int(rest))
        elif op == "C":
            half_matmul(int(rest[0]), "ab".index(rest[1]))
        elif op == "M":
            merge(int(rest))
        elif op == "F":
            finish(int(rest))

    for n in range(len(PIECES)):
        @pl.when(t_me == PIECES[n][0])
        def _():
            stage1_all(n, lambda cp: cp.wait_send(), False)

        for which in range(4):
            to_side(n, which).wait_send()
        for k in range(5):
            to_sibling(n, k).wait_send()
    for s in range(NG):
        for r in order_z:
            for d in (0, 1):
                neighbour_copy(d, s, r).wait_send()
            if r:
                out_copy(s, r).wait_send()
            out_arrived(s, r)


def local_product(nz, ny, a_blk, b_blk):
    rows, depth_k = a_blk.shape
    half_k = b_blk.shape[0]
    width = depth_k // nz
    f32, bf16 = jnp.float32, jnp.bfloat16
    dma = pltpu.SemaphoreType.DMA
    n = len(PIECES)
    return pl.pallas_call(
        functools.partial(kernel, nz, ny),
        name="stationary_a",
        out_shape=jax.ShapeDtypeStruct((rows // nz, depth_k), bf16),
        in_specs=[pl.BlockSpec(memory_space=pl.ANY)] * 2,
        out_specs=pl.BlockSpec(memory_space=pl.ANY),
        scratch_shapes=[
            pltpu.VMEM((rows, depth_k), bf16),
            pltpu.VMEM((NX, 2 * half_k, width), bf16),
            pltpu.VMEM((2, rows // 2, width), f32),
            pltpu.VMEM((2, rows, width), f32),
            pltpu.VMEM((3, rows, width), f32),
            pltpu.VMEM((rows, width), bf16),
            dma((4,)),
            dma((n, NX)),
            dma((n, 10)),
            dma((n, 4)),
            dma((n, 5)),
            dma((NG, 2)),
            dma((NG, 2)),
            dma((2, NG, nz)),
            dma((2, NG, nz)),
            dma((NG, nz)),
            dma((NG, nz)),
        ],
        compiler_params=pltpu.CompilerParams(collective_id=0, has_side_effects=True, vmem_limit_bytes=67043328),
    )(a_blk, b_blk)


def solution(mesh):
    nz, ny = mesh.shape["depth"], mesh.shape["col"]
    return jax.shard_map(
        functools.partial(local_product, nz, ny),
        mesh=mesh,
        in_specs=(P("row", "col"), P("row", "col")),
        out_specs=P(("row", "depth"), "col"),
        check_vma=False,
    )
```

```python
import functools

import jax
import jax.numpy as jnp
from jax import lax
from jax.experimental import pallas as pl
from jax.experimental.pallas import tpu as pltpu
from jax.sharding import PartitionSpec as P

MESH = pl.DeviceIdType.MESH
NX = 4
PIECES = [(2, 0, True), (1, 0, True), (3, 0, True), (2, 1, True), (1, 1, True), (3, 1, True),
          (2, 2, True), (1, 2, True), (3, 2, True), (0, 3, True)]
GROUPS = [(0, 4), (4, 4), (8, 8), (0, 16)]
NG = 3
SLOT = {2: 0, 1: 1, 3: 2, 0: 0}
SCRIPT = """S0 G0 G1 G2 S1 L0 R0 O0 C0a L1 R1 C0b O1 L2 R2 C1a O2 C1b G3 G4 G5 S2 C2a C2b M0
L3 R3 O3 L4 R4 O4 C3a G6 G7 G8 S3 C3b L5 R5 O5 C4a C4b C5a C5b M1 G9 L6 R6 O6 C6a L7 R7 C6b O7 L8 R8 O8 C7a C7b C8a C8b M2
L9 R9 O9 C9a C9b F0 F1 F2"""


def chunk_order(nz):
    return sorted(range(nz), key=lambda r: -min(r, nz - r))


def kernel(nz, ny, a_ref, b_ref, o_ref, abuf, bbuf, ro, rn, pbuf, obuf,
           a_sem, s1_send, b_recv, ag_send, fw_send, op_send, op_recv, nb_send, nb_recv, out_send, out_recv):
    z = lax.axis_index("depth")
    y = lax.axis_index("col")
    i = lax.axis_index("row")
    x, c = i // 2, i % 2
    rows, depth_k = abuf.shape
    half_k = depth_k // 2
    quarter = half_k // NX
    width = depth_k // nz
    unit = width // 16
    chunk = rows // nz
    mblk = rows // 4
    half = rows // 2
    order_z = chunk_order(nz)

    def dev(zz, yy, xx, cc):
        return ((zz + nz) % nz, (yy + ny) % ny, 2 * ((xx + NX) % NX) + cc)

    def remote(src, dst, send_sem, recv_sem, device):
        return pltpu.make_async_remote_copy(src_ref=src, dst_ref=dst, send_sem=send_sem, recv_sem=recv_sem,
                                            device_id=device, device_id_type=MESH)

    sibling = dev(z, y, x, 1 - c)
    left, right, far = dev(z, y, x - 1, c), dev(z, y, x + 1, c), dev(z, y, x + 2, c)

    a_copies = [pltpu.make_async_copy(a_ref.at[pl.ds(m * mblk, mblk)], abuf.at[pl.ds(m * mblk, mblk)], a_sem.at[m])
                for m in range(4)]
    for cp in a_copies:
        cp.start()

    barrier = pltpu.get_barrier_semaphore()
    partners = [sibling]
    partners += [dev(z, y + dy, x + dx, c) for dy in range(ny) for dx in range(NX) if dx or dy]
    partners += [dev(z + r, y, x, c) for r in range(1, nz)]
    for p in partners:
        pl.semaphore_signal(barrier, inc=1, device_id=p, device_id_type=MESH)
    pl.semaphore_wait(barrier, len(partners))

    t_me = (y - x + NX) % NX

    def group_columns(s):
        return pl.ds(GROUPS[s][0] * unit, GROUPS[s][1] * unit)

    def columns(n):
        return group_columns(PIECES[n][1])

    def stage1(n, q, local, act):
        t = PIECES[n][0]
        first, wide = GROUPS[PIECES[n][1]]
        cols = pl.ds(pl.multiple_of(z * width + first * unit, 4 * unit), wide * unit)
        src = b_ref.at[pl.ds(q * quarter, quarter), cols]
        dst = bbuf.at[t, pl.ds(pl.multiple_of(c * half_k + q * quarter, quarter), quarter), columns(n)]
        sem = b_recv.at[n, c * 5]
        if local:
            act(pltpu.make_async_copy(src, dst, sem))
        else:
            act(remote(src, dst, s1_send.at[n, q], sem, dev(z, x, q, c)))

    def stage1_all(n, act, with_local):
        for q in range(NX):
            if PIECES[n][0]:
                stage1(n, q, False, act)
            else:
                @pl.when(x != q)
                def _():
                    stage1(n, q, False, act)

                if with_local:
                    @pl.when(x == q)
                    def _():
                        stage1(n, q, True, act)

    def part(n, lane, k):
        q = (x + (0, 3, 1, 2, 2)[k]) % NX
        start, size = lane * half_k + q * quarter, quarter
        if k >= 3:
            size = quarter // 2
            start = start + (k - 3) * size
        return bbuf.at[PIECES[n][0], pl.ds(pl.multiple_of(start, size), size), columns(n)]

    def arrived(n, lane, k):
        ref = part(n, lane, k)
        remote(ref, ref, fw_send.at[n, 0], b_recv.at[n, lane * 5 + k], sibling).wait_recv()

    def to_sibling(n, k):
        ref = part(n, c, k)
        return remote(ref, ref, fw_send.at[n, k], b_recv.at[n, c * 5 + k], sibling)

    def to_side(n, which):
        straight = PIECES[n][2]
        if which < 2:
            ref = part(n, c, 0)
        else:
            q = x if straight else (x + (3, 1)[which - 2]) % NX
            size = quarter // 2
            start = c * half_k + q * quarter + (which - 2) * size
            ref = bbuf.at[PIECES[n][0], pl.ds(pl.multiple_of(start, size), size), columns(n)]
        target = far if straight and which >= 2 else (right, left)[which % 2]
        return remote(ref, ref, ag_send.at[n, which], b_recv.at[n, c * 5 + 1 + which], target)

    def pass_own(n):
        arrived(n, c, 0)
        for which in (2, 3, 0, 1) if PIECES[n][2] else (0, 1):
            to_side(n, which).start()
        to_sibling(n, 0).start()

    def pass_side(n, k):
        arrived(n, c, k)
        if not PIECES[n][2]:
            to_side(n, k + 1).start()
        to_sibling(n, k).start()

    def pass_far(n):
        for k in (3, 4):
            arrived(n, c, k)
            to_sibling(n, k).start()

    def opposite_copy(s, d):
        return remote(pbuf.at[0, pl.ds(d * half, half), group_columns(s)], ro.at[d, :, group_columns(s)],
                      op_send.at[s, d], op_recv.at[s, d], dev(z, y + 1 - 2 * d, x, c))

    def half_matmul(n, h):
        t = PIECES[n][0]
        if h == 0:
            for k in range(5):
                arrived(n, 1 - c, k)
            if n == 0:
                for cp in a_copies:
                    cp.wait()
            if t == 0:
                for m in range(NG):
                    for d in (0, 1):
                        opposite_copy(m, d).wait_send()

        def body(m, carry):
            r = pl.ds(pl.multiple_of(m * mblk, mblk), mblk)
            pbuf[SLOT[t], r, columns(n)] = jnp.dot(abuf[r, :], bbuf[t, :, columns(n)],
                                                   preferred_element_type=jnp.float32)
            return carry

        lax.fori_loop(2 * h, 2 * h + 2, body, 0)
        if t == 2:
            opposite_copy(PIECES[n][1], h).start()

    def chunk_rows(r):
        zz = (z + r) % nz
        return pl.ds(pl.multiple_of(zz * chunk, chunk), chunk)

    def neighbour_copy(d, s, r):
        cr, cols = chunk_rows(r), group_columns(s)
        return remote(pbuf.at[1 + d, cr, cols], rn.at[d, cr, cols], nb_send.at[d, s, r], nb_recv.at[d, s, r],
                      dev(z, y + 1 - 2 * d, x, c))

    def merge(s):
        cols = group_columns(s)
        for d in (0, 1):
            opposite_copy(s, d).wait_recv()
        for d in (0, 1):
            def body(m, carry):
                r = pl.ds(pl.multiple_of(m * (half // 4), half // 4), half // 4)
                rp = pl.ds(pl.multiple_of(d * half + m * (half // 4), half // 4), half // 4)
                pbuf[1 + d, rp, cols] = pbuf[1 + d, rp, cols] + ro[d, r, cols]
                return carry

            lax.fori_loop(0, 4, body, 0)
        for r in order_z:
            for d in (0, 1):
                neighbour_copy(d, s, r).start()

    def out_columns(zz, s):
        return pl.ds(pl.multiple_of(zz * width + GROUPS[s][0] * unit, 4 * unit), GROUPS[s][1] * unit)

    def out_copy(s, r):
        src = obuf.at[chunk_rows(r), group_columns(s)]
        if r == 0:
            return pltpu.make_async_copy(src, o_ref.at[:, out_columns(z, s)], out_recv.at[s, 0])
        return remote(src, o_ref.at[:, out_columns(z, s)], out_send.at[s, r], out_recv.at[s, r], dev(z + r, y, x, c))

    def out_arrived(s, r):
        if r == 0:
            out_copy(s, 0).wait()
        else:
            remote(obuf.at[chunk_rows(r), group_columns(s)], o_ref.at[:, out_columns((z - r + nz) % nz, s)],
                   out_send.at[s, r], out_recv.at[s, r], dev(z + r, y, x, c)).wait_recv()

    def finish(s):
        cols = group_columns(s)
        for r in order_z:
            for d in (0, 1):
                neighbour_copy(d, s, r).wait_recv()
            cr = chunk_rows(r)
            total = pbuf[0, cr, cols] + rn[0, cr, cols] + rn[1, cr, cols]
            obuf[cr, cols] = total.astype(jnp.bfloat16)
            out_copy(s, r).start()

    for item in SCRIPT.split():
        op, rest = item[0], item[1:]
        if op == "S":
            for n in range(len(PIECES)):
                if PIECES[n][1] == int(rest):
                    @pl.when(t_me == PIECES[n][0])
                    def _():
                        stage1_all(n, lambda cp: cp.start(), True)
        elif op == "G":
            pass_own(int(rest))
        elif op == "L":
            pass_side(int(rest), 1)
        elif op == "R":
            pass_side(int(rest), 2)
        elif op == "O":
            pass_far(int(rest))
        elif op == "C":
            half_matmul(int(rest[0]), "ab".index(rest[1]))
        elif op == "M":
            merge(int(rest))
        elif op == "F":
            finish(int(rest))

    for n in range(len(PIECES)):
        @pl.when(t_me == PIECES[n][0])
        def _():
            stage1_all(n, lambda cp: cp.wait_send(), False)

        for which in range(4):
            to_side(n, which).wait_send()
        for k in range(5):
            to_sibling(n, k).wait_send()
    for s in range(NG):
        for r in order_z:
            for d in (0, 1):
                neighbour_copy(d, s, r).wait_send()
            if r:
                out_copy(s, r).wait_send()
            out_arrived(s, r)


def local_product(nz, ny, a_blk, b_blk):
    rows, depth_k = a_blk.shape
    half_k = b_blk.shape[0]
    width = depth_k // nz
    f32, bf16 = jnp.float32, jnp.bfloat16
    dma = pltpu.SemaphoreType.DMA
    n = len(PIECES)
    return pl.pallas_call(
        functools.partial(kernel, nz, ny),
        name="stationary_a",
        out_shape=jax.ShapeDtypeStruct((rows // nz, depth_k), bf16),
        in_specs=[pl.BlockSpec(memory_space=pl.ANY)] * 2,
        out_specs=pl.BlockSpec(memory_space=pl.ANY),
        scratch_shapes=[
            pltpu.VMEM((rows, depth_k), bf16),
            pltpu.VMEM((NX, 2 * half_k, width), bf16),
            pltpu.VMEM((2, rows // 2, width), f32),
            pltpu.VMEM((2, rows, width), f32),
            pltpu.VMEM((3, rows, width), f32),
            pltpu.VMEM((rows, width), bf16),
            dma((4,)),
            dma((n, NX)),
            dma((n, 10)),
            dma((n, 4)),
            dma((n, 5)),
            dma((NG, 2)),
            dma((NG, 2)),
            dma((2, NG, nz)),
            dma((2, NG, nz)),
            dma((NG, nz)),
            dma((NG, nz)),
        ],
        compiler_params=pltpu.CompilerParams(collective_id=0, has_side_effects=True, vmem_limit_bytes=67043328),
    )(a_blk, b_blk)


def solution(mesh):
    nz, ny = mesh.shape["depth"], mesh.shape["col"]
    return jax.shard_map(
        functools.partial(local_product, nz, ny),
        mesh=mesh,
        in_specs=(P("row", "col"), P("row", "col")),
        out_specs=P(("row", "depth"), "col"),
        check_vma=False,
    )
```

```python
import functools

import jax
import jax.numpy as jnp
from jax import lax
from jax.experimental import pallas as pl
from jax.experimental.pallas import tpu as pltpu
from jax.sharding import PartitionSpec as P

MESH = pl.DeviceIdType.MESH
NX = 4
PIECES = [(2, 0, True), (1, 0, True), (3, 0, True), (2, 1, True), (2, 2, True), (1, 1, True), (3, 1, True),
          (1, 2, True), (3, 2, True), (0, 3, True)]
GROUPS = [(0, 4), (4, 4), (8, 8), (0, 16)]
NG = 3
SLOT = {2: 0, 1: 1, 3: 2, 0: 0}
SCRIPT = """S0 S1 G0 G1 G2 S2 S3 L0 R0 O0 C0a L1 R1 C0b O1 L2 R2 O2 C1a G3 C1b C2a G5 G6 C2b U0 M0
L3 R3 O3 C3a G4 C3b L5 R5 O5 L6 R6 O6 G7 G8 C5a C5b L4 R4 O4 C4a C4b C6a C6b A1 G9 L7 R7 O7 C7a C7b L8 R8 O8 C8a C8b A2
L9 R9 O9 C9a C9b F0 F1 F2"""


def chunk_order(nz):
    return sorted(range(nz), key=lambda r: -min(r, nz - r))


def kernel(nz, ny, a_ref, b_ref, o_ref, abuf, bbuf, ro, rn, pbuf, obuf,
           a_sem, s1_send, b_recv, ag_send, fw_send, op_send, op_recv, nb_send, nb_recv, out_send, out_recv):
    z = lax.axis_index("depth")
    y = lax.axis_index("col")
    i = lax.axis_index("row")
    x, c = i // 2, i % 2
    rows, depth_k = abuf.shape
    half_k = depth_k // 2
    quarter = half_k // NX
    width = depth_k // nz
    unit = width // 16
    chunk = rows // nz
    mblk = rows // 4
    half = rows // 2
    order_z = chunk_order(nz)

    def dev(zz, yy, xx, cc):
        return ((zz + nz) % nz, (yy + ny) % ny, 2 * ((xx + NX) % NX) + cc)

    def remote(src, dst, send_sem, recv_sem, device):
        return pltpu.make_async_remote_copy(src_ref=src, dst_ref=dst, send_sem=send_sem, recv_sem=recv_sem,
                                            device_id=device, device_id_type=MESH)

    sibling = dev(z, y, x, 1 - c)
    left, right, far = dev(z, y, x - 1, c), dev(z, y, x + 1, c), dev(z, y, x + 2, c)

    a_copies = [pltpu.make_async_copy(a_ref.at[pl.ds(m * mblk, mblk)], abuf.at[pl.ds(m * mblk, mblk)], a_sem.at[m])
                for m in range(4)]
    for cp in a_copies:
        cp.start()

    barrier = pltpu.get_barrier_semaphore()
    partners = [sibling]
    partners += [dev(z, y + dy, x + dx, c) for dy in range(ny) for dx in range(NX) if dx or dy]
    partners += [dev(z + r, y, x, c) for r in range(1, nz)]
    for p in partners:
        pl.semaphore_signal(barrier, inc=1, device_id=p, device_id_type=MESH)
    pl.semaphore_wait(barrier, len(partners))

    t_me = (y - x + NX) % NX

    def group_columns(s):
        return pl.ds(GROUPS[s][0] * unit, GROUPS[s][1] * unit)

    def columns(n):
        return group_columns(PIECES[n][1])

    def stage1(n, q, local, act):
        t = PIECES[n][0]
        first, wide = GROUPS[PIECES[n][1]]
        cols = pl.ds(pl.multiple_of(z * width + first * unit, 4 * unit), wide * unit)
        src = b_ref.at[pl.ds(q * quarter, quarter), cols]
        dst = bbuf.at[t, pl.ds(pl.multiple_of(c * half_k + q * quarter, quarter), quarter), columns(n)]
        sem = b_recv.at[n, c * 5]
        if local:
            act(pltpu.make_async_copy(src, dst, sem))
        else:
            act(remote(src, dst, s1_send.at[n, q], sem, dev(z, x, q, c)))

    def stage1_all(n, act, with_local):
        for q in range(NX):
            if PIECES[n][0]:
                stage1(n, q, False, act)
            else:
                @pl.when(x != q)
                def _():
                    stage1(n, q, False, act)

                if with_local:
                    @pl.when(x == q)
                    def _():
                        stage1(n, q, True, act)

    def part(n, lane, k):
        q = (x + (0, 3, 1, 2, 2)[k]) % NX
        start, size = lane * half_k + q * quarter, quarter
        if k >= 3:
            size = quarter // 2
            start = start + (k - 3) * size
        return bbuf.at[PIECES[n][0], pl.ds(pl.multiple_of(start, size), size), columns(n)]

    def arrived(n, lane, k):
        ref = part(n, lane, k)
        remote(ref, ref, fw_send.at[n, 0], b_recv.at[n, lane * 5 + k], sibling).wait_recv()

    def to_sibling(n, k):
        ref = part(n, c, k)
        return remote(ref, ref, fw_send.at[n, k], b_recv.at[n, c * 5 + k], sibling)

    def to_side(n, which):
        straight = PIECES[n][2]
        if which < 2:
            ref = part(n, c, 0)
        else:
            q = x if straight else (x + (3, 1)[which - 2]) % NX
            size = quarter // 2
            start = c * half_k + q * quarter + (which - 2) * size
            ref = bbuf.at[PIECES[n][0], pl.ds(pl.multiple_of(start, size), size), columns(n)]
        target = far if straight and which >= 2 else (right, left)[which % 2]
        return remote(ref, ref, ag_send.at[n, which], b_recv.at[n, c * 5 + 1 + which], target)

    def pass_own(n):
        arrived(n, c, 0)
        for which in (2, 3, 0, 1) if PIECES[n][2] else (0, 1):
            to_side(n, which).start()
        to_sibling(n, 0).start()

    def pass_side(n, k):
        arrived(n, c, k)
        if not PIECES[n][2]:
            to_side(n, k + 1).start()
        to_sibling(n, k).start()

    def pass_far(n):
        for k in (3, 4):
            arrived(n, c, k)
            to_sibling(n, k).start()

    def opposite_copy(s, d):
        return remote(pbuf.at[0, pl.ds(d * half, half), group_columns(s)], ro.at[d, :, group_columns(s)],
                      op_send.at[s, d], op_recv.at[s, d], dev(z, y + 1 - 2 * d, x, c))

    def half_matmul(n, h):
        t = PIECES[n][0]
        if h == 0:
            for k in range(5):
                arrived(n, 1 - c, k)
            if n == 0:
                for cp in a_copies:
                    cp.wait()
            if t == 0:
                for m in range(NG):
                    for d in (0, 1):
                        opposite_copy(m, d).wait_send()

        def body(m, carry):
            r = pl.ds(pl.multiple_of(m * mblk, mblk), mblk)
            pbuf[SLOT[t], r, columns(n)] = jnp.dot(abuf[r, :], bbuf[t, :, columns(n)],
                                                   preferred_element_type=jnp.float32)
            return carry

        lax.fori_loop(2 * h, 2 * h + 2, body, 0)
        if t == 2:
            opposite_copy(PIECES[n][1], h).start()

    def chunk_rows(zz):
        return pl.ds(pl.multiple_of(zz * chunk, chunk), chunk)

    def neighbour_copy(d, s, zz):
        cr, cols = chunk_rows(zz), group_columns(s)
        return remote(pbuf.at[1 + d, cr, cols], rn.at[d, cr, cols], nb_send.at[d, s, zz], nb_recv.at[d, s, zz],
                      dev(z, y + 1 - 2 * d, x, c))

    def send_half(s, merged):
        nh = max(nz // 2, 1)
        for j in range(nh):
            for d in (0, 1):
                neighbour_copy(d, s, ((d if merged else 1 - d) * nh + (z + j) % nh) % nz).start()

    def merge(s):
        cols = group_columns(s)
        for d in (0, 1):
            opposite_copy(s, d).wait_recv()
        for d in (0, 1):
            def body(m, carry):
                r = pl.ds(pl.multiple_of(m * (half // 4), half // 4), half // 4)
                rp = pl.ds(pl.multiple_of(d * half + m * (half // 4), half // 4), half // 4)
                pbuf[1 + d, rp, cols] = pbuf[1 + d, rp, cols] + ro[d, r, cols]
                return carry

            lax.fori_loop(0, 4, body, 0)

    def send_all(s):
        for r in order_z:
            for d in (0, 1):
                neighbour_copy(d, s, (z + r) % nz).start()

    def out_columns(zz, s):
        return pl.ds(pl.multiple_of(zz * width + GROUPS[s][0] * unit, 4 * unit), GROUPS[s][1] * unit)

    def out_copy(s, r):
        src = obuf.at[chunk_rows((z + r) % nz), group_columns(s)]
        if r == 0:
            return pltpu.make_async_copy(src, o_ref.at[:, out_columns(z, s)], out_recv.at[s, 0])
        return remote(src, o_ref.at[:, out_columns(z, s)], out_send.at[s, r], out_recv.at[s, r], dev(z + r, y, x, c))

    def out_arrived(s, r):
        if r == 0:
            out_copy(s, 0).wait()
        else:
            remote(obuf.at[chunk_rows((z + r) % nz), group_columns(s)], o_ref.at[:, out_columns((z - r + nz) % nz, s)],
                   out_send.at[s, r], out_recv.at[s, r], dev(z + r, y, x, c)).wait_recv()

    def finish(s):
        cols = group_columns(s)
        for r in order_z:
            for d in (0, 1):
                neighbour_copy(d, s, (z + r) % nz).wait_recv()
            cr = chunk_rows((z + r) % nz)
            total = pbuf[0, cr, cols] + rn[0, cr, cols] + rn[1, cr, cols]
            obuf[cr, cols] = total.astype(jnp.bfloat16)
            out_copy(s, r).start()

    for item in SCRIPT.split():
        op, rest = item[0], item[1:]
        if op == "S":
            for n in range(len(PIECES)):
                if PIECES[n][1] == int(rest):
                    @pl.when(t_me == PIECES[n][0])
                    def _():
                        stage1_all(n, lambda cp: cp.start(), True)
        elif op == "G":
            pass_own(int(rest))
        elif op == "L":
            pass_side(int(rest), 1)
        elif op == "R":
            pass_side(int(rest), 2)
        elif op == "O":
            pass_far(int(rest))
        elif op == "C":
            half_matmul(int(rest[0]), "ab".index(rest[1]))
        elif op == "U":
            send_half(int(rest), False)
        elif op == "M":
            merge(int(rest))
            send_half(int(rest), True)
        elif op == "A":
            merge(int(rest))
            send_all(int(rest))
        elif op == "F":
            finish(int(rest))

    for n in range(len(PIECES)):
        @pl.when(t_me == PIECES[n][0])
        def _():
            stage1_all(n, lambda cp: cp.wait_send(), False)

        for which in range(4):
            to_side(n, which).wait_send()
        for k in range(5):
            to_sibling(n, k).wait_send()
    for s in range(NG):
        for r in order_z:
            for d in (0, 1):
                neighbour_copy(d, s, (z + r) % nz).wait_send()
            if r:
                out_copy(s, r).wait_send()
            out_arrived(s, r)


def local_product(nz, ny, a_blk, b_blk):
    rows, depth_k = a_blk.shape
    half_k = b_blk.shape[0]
    width = depth_k // nz
    f32, bf16 = jnp.float32, jnp.bfloat16
    dma = pltpu.SemaphoreType.DMA
    n = len(PIECES)
    return pl.pallas_call(
        functools.partial(kernel, nz, ny),
        name="stationary_a",
        out_shape=jax.ShapeDtypeStruct((rows // nz, depth_k), bf16),
        in_specs=[pl.BlockSpec(memory_space=pl.ANY)] * 2,
        out_specs=pl.BlockSpec(memory_space=pl.ANY),
        scratch_shapes=[
            pltpu.VMEM((rows, depth_k), bf16),
            pltpu.VMEM((NX, 2 * half_k, width), bf16),
            pltpu.VMEM((2, rows // 2, width), f32),
            pltpu.VMEM((2, rows, width), f32),
            pltpu.VMEM((3, rows, width), f32),
            pltpu.VMEM((rows, width), bf16),
            dma((4,)),
            dma((n, NX)),
            dma((n, 10)),
            dma((n, 4)),
            dma((n, 5)),
            dma((NG, 2)),
            dma((NG, 2)),
            dma((2, NG, nz)),
            dma((2, NG, nz)),
            dma((NG, nz)),
            dma((NG, nz)),
        ],
        compiler_params=pltpu.CompilerParams(collective_id=0, has_side_effects=True, vmem_limit_bytes=67043328),
    )(a_blk, b_blk)


def solution(mesh):
    nz, ny = mesh.shape["depth"], mesh.shape["col"]
    return jax.shard_map(
        functools.partial(local_product, nz, ny),
        mesh=mesh,
        in_specs=(P("row", "col"), P("row", "col")),
        out_specs=P(("row", "depth"), "col"),
        check_vma=False,
    )
```

```python
import functools

import jax
import jax.numpy as jnp
from jax import lax
from jax.experimental import pallas as pl
from jax.experimental.pallas import tpu as pltpu
from jax.sharding import PartitionSpec as P

MESH = pl.DeviceIdType.MESH
NX = 4
PIECES = [(2, 0, True), (1, 0, True), (3, 0, True), (2, 1, True), (2, 2, True), (1, 1, True), (3, 1, True),
          (1, 2, True), (3, 2, True), (0, 3, True)]
GROUPS = [(0, 4), (4, 4), (8, 8), (0, 16)]
NG = 3
SLOT = {2: 0, 1: 1, 3: 2, 0: 0}
SCRIPT = """X0 S0 X1 X2 X3 S3 G0 S1 S2 G3 X5 X6 X4 X7 X8 X9 L0 R0 O0 C0a G1 G2 C0b S5 S6 S4 L3 R3 O3 C3a L1 R1 C3b O1 L2 R2 O2
C1a S7 S8 C1b C2a S9 C2b U0 M0 G4 G5 G6 L4 R4 O4 C4a G7 G8 C4b L5 R5 O5 C5a G9 C5b L6 R6 O6 C6a C6b A1
L7 R7 O7 C7a C7b L8 R8 O8 C8a C8b A2 L9 R9 O9 C9a C9b W F0 F1 V F2"""


def chunk_order(nz):
    return sorted(range(nz), key=lambda r: -min(r, nz - r))


def kernel(nz, ny, a_ref, b_ref, o_ref, abuf, bbuf, ro, rn, pbuf, obuf,
           a_sem, s1_send, b_recv, ag_send, fw_send, op_send, op_recv, nb_send, nb_recv, out_send, out_recv):
    z = lax.axis_index("depth")
    y = lax.axis_index("col")
    i = lax.axis_index("row")
    x, c = i // 2, i % 2
    rows, depth_k = abuf.shape
    half_k = depth_k // 2
    quarter = half_k // NX
    width = depth_k // nz
    unit = width // 16
    chunk = rows // nz
    mblk = rows // 4
    half = rows // 2
    order_z = chunk_order(nz)

    def dev(zz, yy, xx, cc):
        return ((zz + nz) % nz, (yy + ny) % ny, 2 * ((xx + NX) % NX) + cc)

    def remote(src, dst, send_sem, recv_sem, device):
        return pltpu.make_async_remote_copy(src_ref=src, dst_ref=dst, send_sem=send_sem, recv_sem=recv_sem,
                                            device_id=device, device_id_type=MESH)

    sibling = dev(z, y, x, 1 - c)
    left, right, far = dev(z, y, x - 1, c), dev(z, y, x + 1, c), dev(z, y, x + 2, c)

    a_copies = [pltpu.make_async_copy(a_ref.at[pl.ds(m * mblk, mblk)], abuf.at[pl.ds(m * mblk, mblk)], a_sem.at[m])
                for m in range(4)]
    for cp in a_copies:
        cp.start()

    barrier = pltpu.get_barrier_semaphore()
    partners = [sibling]
    partners += [dev(z, y + dy, x + dx, c) for dy in range(ny) for dx in range(NX) if dx or dy]
    partners += [dev(z + r, y, x, c) for r in range(1, nz)]
    for p in partners:
        pl.semaphore_signal(barrier, inc=1, device_id=p, device_id_type=MESH)
    pl.semaphore_wait(barrier, len(partners))

    t_me = (y - x + NX) % NX

    def group_columns(s):
        return pl.ds(GROUPS[s][0] * unit, GROUPS[s][1] * unit)

    def columns(n):
        return group_columns(PIECES[n][1])

    def stage1(n, d):
        t, group, _ = PIECES[n]
        first, wide = GROUPS[group]
        q = (x + d) % NX
        cols = pl.ds(pl.multiple_of(z * width + first * unit, 4 * unit), wide * unit)
        src = b_ref.at[pl.ds(pl.multiple_of(q * quarter, quarter), quarter), cols]
        dst = bbuf.at[t, pl.ds(pl.multiple_of(c * half_k + q * quarter, quarter), quarter), columns(n)]
        if t == 0 and d == 0:
            return pltpu.make_async_copy(src, dst, b_recv.at[n, c * 5])
        return remote(src, dst, s1_send.at[n, d], b_recv.at[n, c * 5], dev(z, x, q, c))

    def stage1_start(n, ds):
        @pl.when(t_me == PIECES[n][0])
        def _():
            for d in ds:
                stage1(n, d).start()

    def stage1_sent(n):
        @pl.when(t_me == PIECES[n][0])
        def _():
            for d in range(NX):
                if PIECES[n][0] or d:
                    stage1(n, d).wait_send()

    def part(n, lane, k):
        q = (x + (0, 3, 1, 2, 2)[k]) % NX
        start, size = lane * half_k + q * quarter, quarter
        if k >= 3:
            size = quarter // 2
            start = start + (k - 3) * size
        return bbuf.at[PIECES[n][0], pl.ds(pl.multiple_of(start, size), size), columns(n)]

    def arrived(n, lane, k):
        ref = part(n, lane, k)
        remote(ref, ref, fw_send.at[n, 0], b_recv.at[n, lane * 5 + k], sibling).wait_recv()

    def to_sibling(n, k):
        ref = part(n, c, k)
        return remote(ref, ref, fw_send.at[n, k], b_recv.at[n, c * 5 + k], sibling)

    def to_side(n, which):
        straight = PIECES[n][2]
        if which < 2:
            ref = part(n, c, 0)
        else:
            q = x if straight else (x + (3, 1)[which - 2]) % NX
            size = quarter // 2
            start = c * half_k + q * quarter + (which - 2) * size
            ref = bbuf.at[PIECES[n][0], pl.ds(pl.multiple_of(start, size), size), columns(n)]
        target = far if straight and which >= 2 else (right, left)[which % 2]
        return remote(ref, ref, ag_send.at[n, which], b_recv.at[n, c * 5 + 1 + which], target)

    def pass_own(n):
        arrived(n, c, 0)
        for which in (2, 3, 0, 1) if PIECES[n][2] else (0, 1):
            to_side(n, which).start()
        to_sibling(n, 0).start()

    def pass_side(n, k):
        arrived(n, c, k)
        if not PIECES[n][2]:
            to_side(n, k + 1).start()
        to_sibling(n, k).start()

    def pass_far(n):
        for k in (3, 4):
            arrived(n, c, k)
            to_sibling(n, k).start()

    def opposite_copy(s, d, h):
        src = pbuf.at[0, pl.ds(pl.multiple_of(d * half + h * mblk, mblk), mblk), group_columns(s)]
        return remote(src, ro.at[d, pl.ds(h * mblk, mblk), group_columns(s)], op_send.at[s, d, h], op_recv.at[s, d, h],
                      dev(z, y + 1 - 2 * d, x, c))

    def half_matmul(n, h):
        t, group, _ = PIECES[n]
        if h == 0:
            for k in range(5):
                arrived(n, 1 - c, k)
            if n == 0:
                for cp in a_copies:
                    cp.wait()
            if t == 0:
                for m in range(NG):
                    for d in (0, 1):
                        for hh in (0, 1):
                            opposite_copy(m, d, hh).wait_send()

        def body(d, carry):
            r = pl.ds(pl.multiple_of(d * half + h * mblk, mblk), mblk)
            pbuf[SLOT[t], r, columns(n)] = jnp.dot(abuf[r, :], bbuf[t, :, columns(n)],
                                                   preferred_element_type=jnp.float32)
            if t == 2:
                opposite_copy(group, d, h).start()
            return carry

        lax.fori_loop(0, 2, body, 0)

    def chunk_rows(zz):
        return pl.ds(pl.multiple_of(zz * chunk, chunk), chunk)

    def neighbour_copy(d, s, zz):
        cr, cols = chunk_rows(zz), group_columns(s)
        return remote(pbuf.at[1 + d, cr, cols], rn.at[d, cr, cols], nb_send.at[d, s, zz], nb_recv.at[d, s, zz],
                      dev(z, y + 1 - 2 * d, x, c))

    def send_half(s, merged):
        nh = max(nz // 2, 1)
        for j in range(nh):
            for d in (0, 1):
                neighbour_copy(d, s, ((d if merged else 1 - d) * nh + (z + j) % nh) % nz).start()

    def merge(s):
        cols = group_columns(s)
        for d in (0, 1):
            for h in (0, 1):
                opposite_copy(s, d, h).wait_recv()
        for d in (0, 1):
            def body(m, carry):
                r = pl.ds(pl.multiple_of(m * (half // 4), half // 4), half // 4)
                rp = pl.ds(pl.multiple_of(d * half + m * (half // 4), half // 4), half // 4)
                pbuf[1 + d, rp, cols] = pbuf[1 + d, rp, cols] + ro[d, r, cols]
                return carry

            lax.fori_loop(0, 4, body, 0)

    def send_all(s):
        for r in order_z:
            for d in (0, 1):
                neighbour_copy(d, s, (z + r) % nz).start()

    def out_columns(zz, s):
        return pl.ds(pl.multiple_of(zz * width + GROUPS[s][0] * unit, 4 * unit), GROUPS[s][1] * unit)

    def out_copy(s, r):
        src = obuf.at[chunk_rows((z + r) % nz), group_columns(s)]
        if r == 0:
            return pltpu.make_async_copy(src, o_ref.at[:, out_columns(z, s)], out_recv.at[s, 0])
        return remote(src, o_ref.at[:, out_columns(z, s)], out_send.at[s, r], out_recv.at[s, r], dev(z + r, y, x, c))

    def out_arrived(s, r):
        if r == 0:
            out_copy(s, 0).wait()
        else:
            remote(obuf.at[chunk_rows((z + r) % nz), group_columns(s)], o_ref.at[:, out_columns((z - r + nz) % nz, s)],
                   out_send.at[s, r], out_recv.at[s, r], dev(z + r, y, x, c)).wait_recv()

    def finish(s):
        cols = group_columns(s)
        for r in order_z:
            for d in (0, 1):
                neighbour_copy(d, s, (z + r) % nz).wait_recv()
            cr = chunk_rows((z + r) % nz)
            total = pbuf[0, cr, cols] + rn[0, cr, cols] + rn[1, cr, cols]
            obuf[cr, cols] = total.astype(jnp.bfloat16)
            out_copy(s, r).start()

    def out_done(s):
        for r in order_z:
            for d in (0, 1):
                neighbour_copy(d, s, (z + r) % nz).wait_send()
            if r:
                out_copy(s, r).wait_send()
            out_arrived(s, r)

    for item in SCRIPT.split():
        op, rest = item[0], item[1:]
        if op == "X":
            stage1_start(int(rest), (0,))
        elif op == "S":
            stage1_start(int(rest), (2, 1, 3))
        elif op == "G":
            pass_own(int(rest))
        elif op == "L":
            pass_side(int(rest), 1)
        elif op == "R":
            pass_side(int(rest), 2)
        elif op == "O":
            pass_far(int(rest))
        elif op == "C":
            half_matmul(int(rest[0]), "ab".index(rest[1]))
        elif op == "U":
            send_half(int(rest), False)
        elif op == "M":
            merge(int(rest))
            send_half(int(rest), True)
        elif op == "A":
            merge(int(rest))
            send_all(int(rest))
        elif op == "F":
            finish(int(rest))
        elif op == "W":
            for n in range(len(PIECES)):
                stage1_sent(n)
                for which in range(4):
                    to_side(n, which).wait_send()
                for k in range(5):
                    to_sibling(n, k).wait_send()
        elif op == "V":
            for s in range(NG - 1):
                out_done(s)

    out_done(NG - 1)


def local_product(nz, ny, a_blk, b_blk):
    rows, depth_k = a_blk.shape
    half_k = b_blk.shape[0]
    width = depth_k // nz
    f32, bf16 = jnp.float32, jnp.bfloat16
    dma = pltpu.SemaphoreType.DMA
    n = len(PIECES)
    return pl.pallas_call(
        functools.partial(kernel, nz, ny),
        name="stationary_a",
        out_shape=jax.ShapeDtypeStruct((rows // nz, depth_k), bf16),
        in_specs=[pl.BlockSpec(memory_space=pl.ANY)] * 2,
        out_specs=pl.BlockSpec(memory_space=pl.ANY),
        scratch_shapes=[
            pltpu.VMEM((rows, depth_k), bf16),
            pltpu.VMEM((NX, 2 * half_k, width), bf16),
            pltpu.VMEM((2, rows // 2, width), f32),
            pltpu.VMEM((2, rows, width), f32),
            pltpu.VMEM((3, rows, width), f32),
            pltpu.VMEM((rows, width), bf16),
            dma((4,)),
            dma((n, NX)),
            dma((n, 10)),
            dma((n, 4)),
            dma((n, 5)),
            dma((NG, 2, 2)),
            dma((NG, 2, 2)),
            dma((2, NG, nz)),
            dma((2, NG, nz)),
            dma((NG, nz)),
            dma((NG, nz)),
        ],
        compiler_params=pltpu.CompilerParams(collective_id=0, has_side_effects=True, vmem_limit_bytes=67043328),
    )(a_blk, b_blk)


def solution(mesh):
    nz, ny = mesh.shape["depth"], mesh.shape["col"]
    return jax.shard_map(
        functools.partial(local_product, nz, ny),
        mesh=mesh,
        in_specs=(P("row", "col"), P("row", "col")),
        out_specs=P(("row", "depth"), "col"),
        check_vma=False,
    )
```

```python
import functools

import jax
import jax.numpy as jnp
from jax import lax
from jax.experimental import pallas as pl
from jax.experimental.pallas import tpu as pltpu
from jax.sharding import PartitionSpec as P

MESH = pl.DeviceIdType.MESH
NX = 4
PIECES = [(2, 0, True), (2, 1, True), (2, 2, True), (1, 0, True), (3, 0, True), (1, 1, True), (3, 1, True),
          (1, 2, True), (3, 2, True), (0, 3, True)]
GROUPS = [(0, 4), (4, 4), (8, 8), (0, 16)]
NG = 3
SLOT = {2: 0, 1: 1, 3: 2, 0: 0}
SCRIPT = """P0 P3 P4 P1 P5 P6 G0 P2 P7 P8 P9 G1 L0 R0 O0 C0a C0b G2 G3 G4 L1 R1 O1 C1a C1b G5 G6 L2 R2 O2 C2a C2b G9
L3 R3 O3 C3a L4 R4 O4 C3b C4a C4b A0 G7 G8 L5 R5 O5 C5a L6 R6 O6 C5b C6a C6b A1 L9 R9 O9 C9a C9b F0
L7 R7 O7 C7a L8 R8 O8 C7b C8a C8b A2 W F1 F2 V"""


def chunk_order(nz):
    return sorted(range(nz), key=lambda r: -min(r, nz - r))


def kernel(nz, ny, a_ref, b_ref, o_ref, abuf, bbuf, ro, rn, pbuf, obuf,
           a_sem, s1_send, b_recv, ag_send, fw_send, op_send, op_recv, nb_send, nb_recv, out_send, out_recv):
    z = lax.axis_index("depth")
    y = lax.axis_index("col")
    i = lax.axis_index("row")
    x, c = i // 2, i % 2
    rows, depth_k = abuf.shape
    half_k = depth_k // 2
    quarter = half_k // NX
    width = depth_k // nz
    unit = width // 16
    chunk = rows // nz
    mblk = rows // 4
    half = rows // 2
    order_z = chunk_order(nz)

    def dev(zz, yy, xx, cc):
        return ((zz + nz) % nz, (yy + ny) % ny, 2 * ((xx + NX) % NX) + cc)

    def remote(src, dst, send_sem, recv_sem, device):
        return pltpu.make_async_remote_copy(src_ref=src, dst_ref=dst, send_sem=send_sem, recv_sem=recv_sem,
                                            device_id=device, device_id_type=MESH)

    sibling = dev(z, y, x, 1 - c)
    left, right, far = dev(z, y, x - 1, c), dev(z, y, x + 1, c), dev(z, y, x + 2, c)

    a_copies = [pltpu.make_async_copy(a_ref.at[pl.ds(m * mblk, mblk)], abuf.at[pl.ds(m * mblk, mblk)], a_sem.at[m])
                for m in range(4)]
    for cp in a_copies:
        cp.start()

    barrier = pltpu.get_barrier_semaphore()
    partners = [sibling]
    partners += [dev(z, y + dy, x + dx, c) for dy in range(ny) for dx in range(NX) if dx or dy]
    partners += [dev(z + r, y, x, c) for r in range(1, nz)]
    for p in partners:
        pl.semaphore_signal(barrier, inc=1, device_id=p, device_id_type=MESH)
    pl.semaphore_wait(barrier, len(partners))

    t_me = (y - x + NX) % NX

    def group_columns(s):
        return pl.ds(GROUPS[s][0] * unit, GROUPS[s][1] * unit)

    def columns(n):
        return group_columns(PIECES[n][1])

    def stage1(n, d):
        t, group, _ = PIECES[n]
        first, wide = GROUPS[group]
        q = (x + d) % NX
        cols = pl.ds(pl.multiple_of(z * width + first * unit, 4 * unit), wide * unit)
        src = b_ref.at[pl.ds(pl.multiple_of(q * quarter, quarter), quarter), cols]
        dst = bbuf.at[t, pl.ds(pl.multiple_of(c * half_k + q * quarter, quarter), quarter), columns(n)]
        if t == 0 and d == 0:
            return pltpu.make_async_copy(src, dst, b_recv.at[n, c * 5])
        return remote(src, dst, s1_send.at[n, d], b_recv.at[n, c * 5], dev(z, x, q, c))

    def stage1_start(n, ds):
        @pl.when(t_me == PIECES[n][0])
        def _():
            for d in ds:
                stage1(n, d).start()

    def stage1_sent(n):
        @pl.when(t_me == PIECES[n][0])
        def _():
            for d in range(NX):
                if PIECES[n][0] or d:
                    stage1(n, d).wait_send()

    def part(n, lane, k):
        q = (x + (0, 3, 1, 2, 2)[k]) % NX
        start, size = lane * half_k + q * quarter, quarter
        if k >= 3:
            size = quarter // 2
            start = start + (k - 3) * size
        return bbuf.at[PIECES[n][0], pl.ds(pl.multiple_of(start, size), size), columns(n)]

    def arrived(n, lane, k):
        ref = part(n, lane, k)
        remote(ref, ref, fw_send.at[n, 0], b_recv.at[n, lane * 5 + k], sibling).wait_recv()

    def to_sibling(n, k):
        ref = part(n, c, k)
        return remote(ref, ref, fw_send.at[n, k], b_recv.at[n, c * 5 + k], sibling)

    def to_side(n, which):
        straight = PIECES[n][2]
        if which < 2:
            ref = part(n, c, 0)
        else:
            q = x if straight else (x + (3, 1)[which - 2]) % NX
            size = quarter // 2
            start = c * half_k + q * quarter + (which - 2) * size
            ref = bbuf.at[PIECES[n][0], pl.ds(pl.multiple_of(start, size), size), columns(n)]
        target = far if straight and which >= 2 else (right, left)[which % 2]
        return remote(ref, ref, ag_send.at[n, which], b_recv.at[n, c * 5 + 1 + which], target)

    def pass_own(n):
        arrived(n, c, 0)
        for which in (2, 3, 0, 1) if PIECES[n][2] else (0, 1):
            to_side(n, which).start()
        to_sibling(n, 0).start()

    def pass_side(n, k):
        arrived(n, c, k)
        if not PIECES[n][2]:
            to_side(n, k + 1).start()
        to_sibling(n, k).start()

    def pass_far(n):
        for k in (3, 4):
            arrived(n, c, k)
            to_sibling(n, k).start()

    def opposite_copy(s, d, h):
        src = pbuf.at[0, pl.ds(pl.multiple_of(d * half + h * mblk, mblk), mblk), group_columns(s)]
        return remote(src, ro.at[d, pl.ds(h * mblk, mblk), group_columns(s)], op_send.at[s, d, h], op_recv.at[s, d, h],
                      dev(z, y + 1 - 2 * d, x, c))

    def half_matmul(n, h):
        t, group, _ = PIECES[n]
        if h == 0:
            for k in range(5):
                arrived(n, 1 - c, k)
            if n == 0:
                for cp in a_copies:
                    cp.wait()
            if t == 0:
                for m in range(NG):
                    for d in (0, 1):
                        for hh in (0, 1):
                            opposite_copy(m, d, hh).wait_send()

        def body(d, carry):
            r = pl.ds(pl.multiple_of(d * half + h * mblk, mblk), mblk)
            pbuf[SLOT[t], r, columns(n)] = jnp.dot(abuf[r, :], bbuf[t, :, columns(n)],
                                                   preferred_element_type=jnp.float32)
            if t == 2:
                opposite_copy(group, d, h).start()
            return carry

        lax.fori_loop(0, 2, body, 0)

    def chunk_rows(zz):
        return pl.ds(pl.multiple_of(zz * chunk, chunk), chunk)

    def neighbour_copy(d, s, zz):
        cr, cols = chunk_rows(zz), group_columns(s)
        return remote(pbuf.at[1 + d, cr, cols], rn.at[d, cr, cols], nb_send.at[d, s, zz], nb_recv.at[d, s, zz],
                      dev(z, y + 1 - 2 * d, x, c))

    def send_half(s, merged):
        nh = max(nz // 2, 1)
        for j in range(nh):
            for d in (0, 1):
                neighbour_copy(d, s, ((d if merged else 1 - d) * nh + (z + j) % nh) % nz).start()

    def merge(s):
        cols = group_columns(s)
        for d in (0, 1):
            for h in (0, 1):
                opposite_copy(s, d, h).wait_recv()
        for d in (0, 1):
            def body(m, carry):
                r = pl.ds(pl.multiple_of(m * (half // 4), half // 4), half // 4)
                rp = pl.ds(pl.multiple_of(d * half + m * (half // 4), half // 4), half // 4)
                pbuf[1 + d, rp, cols] = pbuf[1 + d, rp, cols] + ro[d, r, cols]
                return carry

            lax.fori_loop(0, 4, body, 0)

    def send_all(s):
        for r in order_z:
            for d in (0, 1):
                neighbour_copy(d, s, (z + r) % nz).start()

    def out_columns(zz, s):
        return pl.ds(pl.multiple_of(zz * width + GROUPS[s][0] * unit, 4 * unit), GROUPS[s][1] * unit)

    def out_copy(s, r):
        src = obuf.at[chunk_rows((z + r) % nz), group_columns(s)]
        if r == 0:
            return pltpu.make_async_copy(src, o_ref.at[:, out_columns(z, s)], out_recv.at[s, 0])
        return remote(src, o_ref.at[:, out_columns(z, s)], out_send.at[s, r], out_recv.at[s, r], dev(z + r, y, x, c))

    def out_arrived(s, r):
        if r == 0:
            out_copy(s, 0).wait()
        else:
            remote(obuf.at[chunk_rows((z + r) % nz), group_columns(s)], o_ref.at[:, out_columns((z - r + nz) % nz, s)],
                   out_send.at[s, r], out_recv.at[s, r], dev(z + r, y, x, c)).wait_recv()

    def finish(s):
        cols = group_columns(s)
        for r in order_z:
            for d in (0, 1):
                neighbour_copy(d, s, (z + r) % nz).wait_recv()
            cr = chunk_rows((z + r) % nz)
            total = pbuf[0, cr, cols] + rn[0, cr, cols] + rn[1, cr, cols]
            obuf[cr, cols] = total.astype(jnp.bfloat16)
            out_copy(s, r).start()

    def out_done(s):
        for r in order_z:
            for d in (0, 1):
                neighbour_copy(d, s, (z + r) % nz).wait_send()
            if r:
                out_copy(s, r).wait_send()
            out_arrived(s, r)

    for item in SCRIPT.split():
        op, rest = item[0], item[1:]
        if op == "P":
            stage1_start(int(rest), (0, 2, 1, 3))
        elif op == "G":
            pass_own(int(rest))
        elif op == "L":
            pass_side(int(rest), 1)
        elif op == "R":
            pass_side(int(rest), 2)
        elif op == "O":
            pass_far(int(rest))
        elif op == "C":
            half_matmul(int(rest[0]), "ab".index(rest[1]))
        elif op == "U":
            send_half(int(rest), False)
        elif op == "M":
            merge(int(rest))
            send_half(int(rest), True)
        elif op == "A":
            merge(int(rest))
            send_all(int(rest))
        elif op == "F":
            finish(int(rest))
        elif op == "W":
            for n in range(len(PIECES)):
                stage1_sent(n)
                for which in range(4):
                    to_side(n, which).wait_send()
                for k in range(5):
                    to_sibling(n, k).wait_send()
        elif op == "V":
            for s in range(NG - 1):
                out_done(s)

    out_done(NG - 1)


def local_product(nz, ny, a_blk, b_blk):
    rows, depth_k = a_blk.shape
    half_k = b_blk.shape[0]
    width = depth_k // nz
    f32, bf16 = jnp.float32, jnp.bfloat16
    dma = pltpu.SemaphoreType.DMA
    n = len(PIECES)
    return pl.pallas_call(
        functools.partial(kernel, nz, ny),
        name="stationary_a",
        out_shape=jax.ShapeDtypeStruct((rows // nz, depth_k), bf16),
        in_specs=[pl.BlockSpec(memory_space=pl.ANY)] * 2,
        out_specs=pl.BlockSpec(memory_space=pl.ANY),
        scratch_shapes=[
            pltpu.VMEM((rows, depth_k), bf16),
            pltpu.VMEM((NX, 2 * half_k, width), bf16),
            pltpu.VMEM((2, rows // 2, width), f32),
            pltpu.VMEM((2, rows, width), f32),
            pltpu.VMEM((3, rows, width), f32),
            pltpu.VMEM((rows, width), bf16),
            dma((4,)),
            dma((n, NX)),
            dma((n, 10)),
            dma((n, 4)),
            dma((n, 5)),
            dma((NG, 2, 2)),
            dma((NG, 2, 2)),
            dma((2, NG, nz)),
            dma((2, NG, nz)),
            dma((NG, nz)),
            dma((NG, nz)),
        ],
        compiler_params=pltpu.CompilerParams(collective_id=0, has_side_effects=True, vmem_limit_bytes=67043328),
    )(a_blk, b_blk)


def solution(mesh):
    nz, ny = mesh.shape["depth"], mesh.shape["col"]
    return jax.shard_map(
        functools.partial(local_product, nz, ny),
        mesh=mesh,
        in_specs=(P("row", "col"), P("row", "col")),
        out_specs=P(("row", "depth"), "col"),
        check_vma=False,
    )
```

```python
import functools

import jax
import jax.numpy as jnp
from jax import lax
from jax.experimental import pallas as pl
from jax.experimental.pallas import tpu as pltpu
from jax.sharding import PartitionSpec as P

MESH = pl.DeviceIdType.MESH
NX = 4
PIECES = [(2, 0, True), (2, 1, True), (2, 2, True), (1, 0, True), (3, 0, True), (1, 1, True), (3, 1, True),
          (1, 2, True), (3, 2, True), (0, 3, True), (0, 2, True)]
GROUPS = [(0, 4), (4, 4), (8, 8), (0, 8)]
NG = 3
SLOT = {2: 0, 1: 1, 3: 2, 0: 0}
SCRIPT = """P0 P3 P4 P1 P5 P6 G0 P2 G1 L0 R0 O0 C0a G2 C0b P7 P8 G3 G4 L1 R1 O1 C1a C1b G5 G6 P9 P10 L2 R2 O2 C2a C2b
L3 R3 O3 C3a L4 R4 O4 C3b C4a C4b A0 G9 G7 G8 L5 R5 O5 C5a L6 R6 O6 C5b C6a C6b A1 G10 L9 R9 O9 C9a C9b F0
L7 R7 O7 C7a L8 R8 O8 C7b C8a C8b A2 F1 L10 R10 O10 C10a C10b W F2 V"""


def chunk_order(nz):
    return sorted(range(nz), key=lambda r: -min(r, nz - r))


def kernel(nz, ny, a_ref, b_ref, o_ref, abuf, bbuf, ro, rn, pbuf, obuf,
           a_sem, s1_send, b_recv, ag_send, fw_send, op_send, op_recv, nb_send, nb_recv, out_send, out_recv):
    z = lax.axis_index("depth")
    y = lax.axis_index("col")
    i = lax.axis_index("row")
    x, c = i // 2, i % 2
    rows, depth_k = abuf.shape
    half_k = depth_k // 2
    quarter = half_k // NX
    width = depth_k // nz
    unit = width // 16
    chunk = rows // nz
    mblk = rows // 4
    half = rows // 2
    order_z = chunk_order(nz)

    def dev(zz, yy, xx, cc):
        return ((zz + nz) % nz, (yy + ny) % ny, 2 * ((xx + NX) % NX) + cc)

    def remote(src, dst, send_sem, recv_sem, device):
        return pltpu.make_async_remote_copy(src_ref=src, dst_ref=dst, send_sem=send_sem, recv_sem=recv_sem,
                                            device_id=device, device_id_type=MESH)

    sibling = dev(z, y, x, 1 - c)
    left, right, far = dev(z, y, x - 1, c), dev(z, y, x + 1, c), dev(z, y, x + 2, c)

    a_copies = [pltpu.make_async_copy(a_ref.at[pl.ds(m * mblk, mblk)], abuf.at[pl.ds(m * mblk, mblk)], a_sem.at[m])
                for m in range(4)]
    for cp in a_copies:
        cp.start()

    barrier = pltpu.get_barrier_semaphore()
    partners = [sibling]
    partners += [dev(z, y + dy, x + dx, c) for dy in range(ny) for dx in range(NX) if dx or dy]
    partners += [dev(z + r, y, x, c) for r in range(1, nz)]
    for p in partners:
        pl.semaphore_signal(barrier, inc=1, device_id=p, device_id_type=MESH)
    pl.semaphore_wait(barrier, len(partners))

    t_me = (y - x + NX) % NX

    def group_columns(s):
        return pl.ds(GROUPS[s][0] * unit, GROUPS[s][1] * unit)

    def columns(n):
        return group_columns(PIECES[n][1])

    def stage1(n, d):
        t, group, _ = PIECES[n]
        first, wide = GROUPS[group]
        q = (x + d) % NX
        cols = pl.ds(pl.multiple_of(z * width + first * unit, 4 * unit), wide * unit)
        src = b_ref.at[pl.ds(pl.multiple_of(q * quarter, quarter), quarter), cols]
        dst = bbuf.at[t, pl.ds(pl.multiple_of(c * half_k + q * quarter, quarter), quarter), columns(n)]
        if t == 0 and d == 0:
            return pltpu.make_async_copy(src, dst, b_recv.at[n, c * 5])
        return remote(src, dst, s1_send.at[n, d], b_recv.at[n, c * 5], dev(z, x, q, c))

    def stage1_start(n, ds):
        @pl.when(t_me == PIECES[n][0])
        def _():
            for d in ds:
                stage1(n, d).start()

    def stage1_sent(n):
        @pl.when(t_me == PIECES[n][0])
        def _():
            for d in range(NX):
                if PIECES[n][0] or d:
                    stage1(n, d).wait_send()

    def part(n, lane, k):
        q = (x + (0, 3, 1, 2, 2)[k]) % NX
        start, size = lane * half_k + q * quarter, quarter
        if k >= 3:
            size = quarter // 2
            start = start + (k - 3) * size
        return bbuf.at[PIECES[n][0], pl.ds(pl.multiple_of(start, size), size), columns(n)]

    def arrived(n, lane, k):
        ref = part(n, lane, k)
        remote(ref, ref, fw_send.at[n, 0], b_recv.at[n, lane * 5 + k], sibling).wait_recv()

    def to_sibling(n, k):
        ref = part(n, c, k)
        return remote(ref, ref, fw_send.at[n, k], b_recv.at[n, c * 5 + k], sibling)

    def to_side(n, which):
        straight = PIECES[n][2]
        if which < 2:
            ref = part(n, c, 0)
        else:
            q = x if straight else (x + (3, 1)[which - 2]) % NX
            size = quarter // 2
            start = c * half_k + q * quarter + (which - 2) * size
            ref = bbuf.at[PIECES[n][0], pl.ds(pl.multiple_of(start, size), size), columns(n)]
        target = far if straight and which >= 2 else (right, left)[which % 2]
        return remote(ref, ref, ag_send.at[n, which], b_recv.at[n, c * 5 + 1 + which], target)

    def pass_own(n):
        arrived(n, c, 0)
        for which in (2, 3, 0, 1) if PIECES[n][2] else (0, 1):
            to_side(n, which).start()
        to_sibling(n, 0).start()

    def pass_side(n, k):
        arrived(n, c, k)
        if not PIECES[n][2]:
            to_side(n, k + 1).start()
        to_sibling(n, k).start()

    def pass_far(n):
        for k in (3, 4):
            arrived(n, c, k)
            to_sibling(n, k).start()

    def opposite_copy(s, d, h):
        src = pbuf.at[0, pl.ds(pl.multiple_of(d * half + h * mblk, mblk), mblk), group_columns(s)]
        return remote(src, ro.at[d, pl.ds(h * mblk, mblk), group_columns(s)], op_send.at[s, d, h], op_recv.at[s, d, h],
                      dev(z, y + 1 - 2 * d, x, c))

    def half_matmul(n, h):
        t, group, _ = PIECES[n]
        if h == 0:
            for k in range(5):
                arrived(n, 1 - c, k)
            if n == 0:
                for cp in a_copies:
                    cp.wait()
            if t == 0:
                for m in (0, 1) if group == 3 else (2,):
                    for d in (0, 1):
                        for hh in (0, 1):
                            opposite_copy(m, d, hh).wait_send()

        def body(d, carry):
            r = pl.ds(pl.multiple_of(d * half + h * mblk, mblk), mblk)
            pbuf[SLOT[t], r, columns(n)] = jnp.dot(abuf[r, :], bbuf[t, :, columns(n)],
                                                   preferred_element_type=jnp.float32)
            if t == 2:
                opposite_copy(group, d, h).start()
            return carry

        lax.fori_loop(0, 2, body, 0)

    def chunk_rows(zz):
        return pl.ds(pl.multiple_of(zz * chunk, chunk), chunk)

    def neighbour_copy(d, s, zz):
        cr, cols = chunk_rows(zz), group_columns(s)
        return remote(pbuf.at[1 + d, cr, cols], rn.at[d, cr, cols], nb_send.at[d, s, zz], nb_recv.at[d, s, zz],
                      dev(z, y + 1 - 2 * d, x, c))

    def send_half(s, merged):
        nh = max(nz // 2, 1)
        for j in range(nh):
            for d in (0, 1):
                neighbour_copy(d, s, ((d if merged else 1 - d) * nh + (z + j) % nh) % nz).start()

    def merge(s):
        cols = group_columns(s)
        for d in (0, 1):
            for h in (0, 1):
                opposite_copy(s, d, h).wait_recv()
        for d in (0, 1):
            def body(m, carry):
                r = pl.ds(pl.multiple_of(m * (half // 4), half // 4), half // 4)
                rp = pl.ds(pl.multiple_of(d * half + m * (half // 4), half // 4), half // 4)
                pbuf[1 + d, rp, cols] = pbuf[1 + d, rp, cols] + ro[d, r, cols]
                return carry

            lax.fori_loop(0, 4, body, 0)

    def send_all(s):
        for r in order_z:
            for d in (0, 1):
                neighbour_copy(d, s, (z + r) % nz).start()

    def out_columns(zz, s):
        return pl.ds(pl.multiple_of(zz * width + GROUPS[s][0] * unit, 4 * unit), GROUPS[s][1] * unit)

    def out_copy(s, r):
        src = obuf.at[chunk_rows((z + r) % nz), group_columns(s)]
        if r == 0:
            return pltpu.make_async_copy(src, o_ref.at[:, out_columns(z, s)], out_recv.at[s, 0])
        return remote(src, o_ref.at[:, out_columns(z, s)], out_send.at[s, r], out_recv.at[s, r], dev(z + r, y, x, c))

    def out_arrived(s, r):
        if r == 0:
            out_copy(s, 0).wait()
        else:
            remote(obuf.at[chunk_rows((z + r) % nz), group_columns(s)], o_ref.at[:, out_columns((z - r + nz) % nz, s)],
                   out_send.at[s, r], out_recv.at[s, r], dev(z + r, y, x, c)).wait_recv()

    def finish(s):
        cols = group_columns(s)
        for r in order_z:
            for d in (0, 1):
                neighbour_copy(d, s, (z + r) % nz).wait_recv()
            cr = chunk_rows((z + r) % nz)
            total = pbuf[0, cr, cols] + rn[0, cr, cols] + rn[1, cr, cols]
            obuf[cr, cols] = total.astype(jnp.bfloat16)
            out_copy(s, r).start()

    def out_done(s):
        for r in order_z:
            for d in (0, 1):
                neighbour_copy(d, s, (z + r) % nz).wait_send()
            if r:
                out_copy(s, r).wait_send()
            out_arrived(s, r)

    for item in SCRIPT.split():
        op, rest = item[0], item[1:]
        if op == "P":
            stage1_start(int(rest), (0, 2, 1, 3))
        elif op == "G":
            pass_own(int(rest))
        elif op == "L":
            pass_side(int(rest), 1)
        elif op == "R":
            pass_side(int(rest), 2)
        elif op == "O":
            pass_far(int(rest))
        elif op == "C":
            half_matmul(int(rest[:-1]), "ab".index(rest[-1]))
        elif op == "U":
            send_half(int(rest), False)
        elif op == "M":
            merge(int(rest))
            send_half(int(rest), True)
        elif op == "A":
            merge(int(rest))
            send_all(int(rest))
        elif op == "F":
            finish(int(rest))
        elif op == "W":
            for n in range(len(PIECES)):
                stage1_sent(n)
                for which in range(4):
                    to_side(n, which).wait_send()
                for k in range(5):
                    to_sibling(n, k).wait_send()
        elif op == "V":
            for s in range(NG - 1):
                out_done(s)

    out_done(NG - 1)


def local_product(nz, ny, a_blk, b_blk):
    rows, depth_k = a_blk.shape
    half_k = b_blk.shape[0]
    width = depth_k // nz
    f32, bf16 = jnp.float32, jnp.bfloat16
    dma = pltpu.SemaphoreType.DMA
    n = len(PIECES)
    return pl.pallas_call(
        functools.partial(kernel, nz, ny),
        name="stationary_a",
        out_shape=jax.ShapeDtypeStruct((rows // nz, depth_k), bf16),
        in_specs=[pl.BlockSpec(memory_space=pl.ANY)] * 2,
        out_specs=pl.BlockSpec(memory_space=pl.ANY),
        scratch_shapes=[
            pltpu.VMEM((rows, depth_k), bf16),
            pltpu.VMEM((NX, 2 * half_k, width), bf16),
            pltpu.VMEM((2, rows // 2, width), f32),
            pltpu.VMEM((2, rows, width), f32),
            pltpu.VMEM((3, rows, width), f32),
            pltpu.VMEM((rows, width), bf16),
            dma((4,)),
            dma((n, NX)),
            dma((n, 10)),
            dma((n, 4)),
            dma((n, 5)),
            dma((NG, 2, 2)),
            dma((NG, 2, 2)),
            dma((2, NG, nz)),
            dma((2, NG, nz)),
            dma((NG, nz)),
            dma((NG, nz)),
        ],
        compiler_params=pltpu.CompilerParams(collective_id=0, has_side_effects=True, vmem_limit_bytes=67043328),
    )(a_blk, b_blk)


def solution(mesh):
    nz, ny = mesh.shape["depth"], mesh.shape["col"]
    return jax.shard_map(
        functools.partial(local_product, nz, ny),
        mesh=mesh,
        in_specs=(P("row", "col"), P("row", "col")),
        out_specs=P(("row", "depth"), "col"),
        check_vma=False,
    )
```

```python
import functools

import jax
import jax.numpy as jnp
from jax import lax
from jax.experimental import pallas as pl
from jax.experimental.pallas import tpu as pltpu
from jax.sharding import PartitionSpec as P

MESH = pl.DeviceIdType.MESH
NX = 4
PIECES = [(2, 0), (2, 1), (2, 2), (1, 0), (3, 0), (1, 1), (3, 1), (1, 2), (3, 2), (0, 3), (0, 2)]
GROUPS = [(0, 4), (4, 4), (8, 8), (0, 8)]
NG = 3
SLOT = {2: 0, 1: 1, 3: 2, 0: 0}
SCRIPT = """P0 P3 P4 P1 P5 P6 G0 P2 G1 L0 R0 O0 C0a C0b G2 P7 P8 G3 G4 L1 R1 O1 C1a C1b G5 G6 P9 P10 L2 R2 O2 C2a C2b
L3 R3 O3 C3a L4 R4 O4 C3b C4a C4b A0 G9 G7 G8 L5 R5 O5 C5a L6 R6 O6 C5b C6a C6b A1 G10 L9 R9 O9 C9a C9b F0
L7 R7 O7 C7a L8 R8 O8 C7b C8a C8b A2 F1 L10 R10 O10 C10a C10b W F2"""


def chunk_order(nz):
    return sorted(range(nz), key=lambda r: -min(r, nz - r))


def kernel(nz, ny, a_ref, b_ref, o_ref, abuf, bbuf, ro, rn, pbuf, obuf,
           a_sem, b_send, b_recv, s_recv, op_send, op_recv, nb_send, nb_recv, out_send, out_recv, own_sem):
    z = lax.axis_index("depth")
    y = lax.axis_index("col")
    i = lax.axis_index("row")
    x, c = i // 2, i % 2
    rows, depth_k = abuf.shape
    half_k = depth_k // 2
    quarter = half_k // NX
    width = depth_k // nz
    unit = width // 16
    chunk = rows // nz
    mblk = rows // 4
    half = rows // 2
    order_z = chunk_order(nz)

    def dev(zz, yy, xx, cc):
        return ((zz + nz) % nz, (yy + ny) % ny, 2 * ((xx + NX) % NX) + cc)

    def remote(src, dst, send_sem, recv_sem, device):
        return pltpu.make_async_remote_copy(src_ref=src, dst_ref=dst, send_sem=send_sem, recv_sem=recv_sem,
                                            device_id=device, device_id_type=MESH)

    sibling = dev(z, y, x, 1 - c)
    left, right, far = dev(z, y, x - 1, c), dev(z, y, x + 1, c), dev(z, y, x + 2, c)

    a_copies = [pltpu.make_async_copy(a_ref.at[pl.ds(m * mblk, mblk)], abuf.at[pl.ds(m * mblk, mblk)], a_sem)
                for m in range(4)]
    for cp in a_copies:
        cp.start()

    barrier = pltpu.get_barrier_semaphore()
    partners = [sibling]
    partners += [dev(z, y + dy, x + dx, c) for dy in range(ny) for dx in range(NX) if dx or dy]
    partners += [dev(z + r, y, x, c) for r in range(1, nz)]
    for p in partners:
        pl.semaphore_signal(barrier, inc=1, device_id=p, device_id_type=MESH)
    pl.semaphore_wait(barrier, len(partners))

    t_me = (y - x + NX) % NX

    def group_columns(s):
        return pl.ds(GROUPS[s][0] * unit, GROUPS[s][1] * unit)

    def columns(n):
        return group_columns(PIECES[n][1])

    def stage1(n, d):
        t, group = PIECES[n]
        first, wide = GROUPS[group]
        q = (x + d) % NX
        cols = pl.ds(pl.multiple_of(z * width + first * unit, 4 * unit), wide * unit)
        src = b_ref.at[pl.ds(pl.multiple_of(q * quarter, quarter), quarter), cols]
        dst = bbuf.at[t, pl.ds(pl.multiple_of(c * half_k + q * quarter, quarter), quarter), columns(n)]
        if t == 0 and d == 0:
            return pltpu.make_async_copy(src, dst, b_recv.at[n, 0])
        return remote(src, dst, b_send, b_recv.at[n, 0], dev(z, x, q, c))

    def stage1_start(n, ds):
        @pl.when(t_me == PIECES[n][0])
        def _():
            for d in ds:
                stage1(n, d).start()

    def part(n, k):
        q = (x + (0, 3, 1, 2)[k]) % NX
        start = c * half_k + q * quarter
        return bbuf.at[PIECES[n][0], pl.ds(pl.multiple_of(start, quarter), quarter), columns(n)]

    def lane(n, cc):
        return bbuf.at[PIECES[n][0], pl.ds(pl.multiple_of(cc * half_k, half_k), half_k), columns(n)]

    def arrived(n, k):
        ref = part(n, k)
        remote(ref, ref, b_send, b_recv.at[n, k], sibling).wait_recv()

    def to_sibling(n, k):
        ref = part(n, k)
        remote(ref, ref, b_send, s_recv.at[n], sibling).start()

    def pass_own(n):
        arrived(n, 0)
        ref = part(n, 0)
        for k, target in ((3, far), (1, right), (2, left)):
            remote(ref, ref, b_send, b_recv.at[n, k], target).start()
        to_sibling(n, 0)

    def pass_on(n, k):
        arrived(n, k)
        to_sibling(n, k)

    def group_columns(s):
        return pl.ds(GROUPS[s][0] * unit, GROUPS[s][1] * unit)

    def opposite_copy(s, d, h):
        src = pbuf.at[0, pl.ds(pl.multiple_of(d * half + h * mblk, mblk), mblk), group_columns(s)]
        return remote(src, ro.at[d, pl.ds(h * mblk, mblk), group_columns(s)], op_send.at[s], op_recv.at[s, d],
                      dev(z, y + 1 - 2 * d, x, c))

    def half_matmul(n, h):
        t, group = PIECES[n]
        if h == 0:
            ref = lane(n, 1 - c)
            remote(ref, ref, b_send, s_recv.at[n], sibling).wait_recv()
            if n == 0:
                pltpu.make_async_copy(abuf, abuf, a_sem).wait()
            if t == 0:
                for m in (0, 1) if group == 3 else (2,):
                    ref = pbuf.at[0, :, group_columns(m)]
                    remote(ref, ref, op_send.at[m], op_recv.at[m, 0], sibling).wait_send()

        def body(d, carry):
            r = pl.ds(pl.multiple_of(d * half + h * mblk, mblk), mblk)
            pbuf[SLOT[t], r, columns(n)] = jnp.dot(abuf[r, :], bbuf[t, :, columns(n)],
                                                   preferred_element_type=jnp.float32)
            if t == 2:
                opposite_copy(group, d, h).start()
            return carry

        lax.fori_loop(0, 2, body, 0)

    def chunk_rows(zz):
        return pl.ds(pl.multiple_of(zz * chunk, chunk), chunk)

    def neighbour_copy(d, s, zz):
        cr, cols = chunk_rows(zz), group_columns(s)
        return remote(pbuf.at[1 + d, cr, cols], rn.at[d, cr, cols], nb_send, nb_recv.at[d, s, zz],
                      dev(z, y + 1 - 2 * d, x, c))

    def send_half(s, merged):
        nh = max(nz // 2, 1)
        for j in range(nh):
            for d in (0, 1):
                neighbour_copy(d, s, ((d if merged else 1 - d) * nh + (z + j) % nh) % nz).start()

    def merge(s):
        cols = group_columns(s)
        for d in (0, 1):
            ref = ro.at[d, :, group_columns(s)]
            remote(ref, ref, op_send.at[s], op_recv.at[s, d], sibling).wait_recv()
        for d in (0, 1):
            def body(m, carry):
                r = pl.ds(pl.multiple_of(m * (half // 4), half // 4), half // 4)
                rp = pl.ds(pl.multiple_of(d * half + m * (half // 4), half // 4), half // 4)
                pbuf[1 + d, rp, cols] = pbuf[1 + d, rp, cols] + ro[d, r, cols]
                return carry

            lax.fori_loop(0, 4, body, 0)

    def send_all(s):
        for r in order_z:
            for d in (0, 1):
                neighbour_copy(d, s, (z + r) % nz).start()

    def out_columns(zz, s):
        return pl.ds(pl.multiple_of(zz * width + GROUPS[s][0] * unit, 4 * unit), GROUPS[s][1] * unit)

    def out_copy(s, r):
        src = obuf.at[chunk_rows((z + r) % nz), group_columns(s)]
        dst = o_ref.at[:, out_columns(z, s)]
        if r == 0:
            return pltpu.make_async_copy(src, dst, own_sem.at[s])
        return remote(src, dst, out_send, out_recv, dev(z + r, y, x, c))

    def finish(s):
        cols = group_columns(s)
        for r in order_z:
            for d in (0, 1):
                neighbour_copy(d, s, (z + r) % nz).wait_recv()
            cr = chunk_rows((z + r) % nz)
            total = pbuf[0, cr, cols] + rn[0, cr, cols] + rn[1, cr, cols]
            obuf[cr, cols] = total.astype(jnp.bfloat16)
            out_copy(s, r).start()

    for item in SCRIPT.split():
        op, rest = item[0], item[1:]
        if op == "P":
            stage1_start(int(rest), (0, 2, 1, 3))
        elif op == "G":
            pass_own(int(rest))
        elif op == "L":
            pass_on(int(rest), 1)
        elif op == "R":
            pass_on(int(rest), 2)
        elif op == "O":
            pass_on(int(rest), 3)
        elif op == "C":
            half_matmul(int(rest[:-1]), "ab".index(rest[-1]))
        elif op == "U":
            send_half(int(rest), False)
        elif op == "M":
            merge(int(rest))
            send_half(int(rest), True)
        elif op == "A":
            merge(int(rest))
            send_all(int(rest))
        elif op == "F":
            finish(int(rest))
        elif op == "W":
            @pl.when(t_me != 0)
            def _():
                remote(bbuf, bbuf, b_send, out_recv, sibling).wait_send()

            @pl.when(t_me == 0)
            def _():
                ref = bbuf.at[:, pl.ds(0, 2 * half_k - quarter // NX)]
                remote(ref, ref, b_send, out_recv, sibling).wait_send()

    remote(rn, rn, nb_send, out_recv, sibling).wait_send()
    for s in range(NG):
        out_copy(s, 0).wait()
    sent = obuf.at[pl.ds(0, rows - chunk)]
    remote(sent, sent, out_send, out_recv, sibling).wait_send()
    got = o_ref.at[pl.ds(0, chunk - chunk // nz)]
    remote(got, got, out_send, out_recv, sibling).wait_recv()


COPIES = 4


def copy_kernel(src_ref, dst_ref, buf, in_sem, out_sem):
    n = buf.shape[0] // COPIES
    blocks = [pl.ds(m * n, n) for m in range(COPIES)]
    ins = [pltpu.make_async_copy(src_ref.at[b], buf.at[b], in_sem.at[m]) for m, b in enumerate(blocks)]
    outs = [pltpu.make_async_copy(buf.at[b], dst_ref.at[b], out_sem.at[m]) for m, b in enumerate(blocks)]
    for cp in ins:
        cp.start()
    for cp_in, cp_out in zip(ins, outs):
        cp_in.wait()
        cp_out.start()
    for cp in outs:
        cp.wait()


def copy_out(c_rows):
    return pl.pallas_call(
        copy_kernel,
        name="copy_out",
        out_shape=jax.ShapeDtypeStruct(c_rows.shape, c_rows.dtype),
        in_specs=[pl.BlockSpec(memory_space=pl.ANY)],
        out_specs=pl.BlockSpec(memory_space=pl.ANY),
        scratch_shapes=[pltpu.VMEM(c_rows.shape, c_rows.dtype), pltpu.SemaphoreType.DMA((COPIES,)),
                        pltpu.SemaphoreType.DMA((COPIES,))],
    )(c_rows)


def local_product(nz, ny, a_blk, b_blk):
    rows, depth_k = a_blk.shape
    half_k = b_blk.shape[0]
    width = depth_k // nz
    f32, bf16 = jnp.float32, jnp.bfloat16
    dma = pltpu.SemaphoreType.DMA
    n = len(PIECES)
    return copy_out(pl.pallas_call(
        functools.partial(kernel, nz, ny),
        name="stationary_a",
        out_shape=jax.ShapeDtypeStruct((rows // nz, depth_k), bf16),
        in_specs=[pl.BlockSpec(memory_space=pl.ANY)] * 2,
        out_specs=pl.BlockSpec(memory_space=pl.ANY),
        scratch_shapes=[
            pltpu.VMEM((rows, depth_k), bf16),
            pltpu.VMEM((NX, 2 * half_k, width), bf16),
            pltpu.VMEM((2, rows // 2, width), f32),
            pltpu.VMEM((2, rows, width), f32),
            pltpu.VMEM((3, rows, width), f32),
            pltpu.VMEM((rows, width), bf16),
            dma,
            dma,
            dma((n, 4)),
            dma((n,)),
            dma((NG,)),
            dma((NG, 2)),
            dma,
            dma((2, NG, nz)),
            dma,
            dma,
            dma((NG,)),
        ],
        compiler_params=pltpu.CompilerParams(collective_id=0, has_side_effects=True, vmem_limit_bytes=67043328),
    )(a_blk, b_blk))


def solution(mesh):
    nz, ny = mesh.shape["depth"], mesh.shape["col"]
    return jax.shard_map(
        functools.partial(local_product, nz, ny),
        mesh=mesh,
        in_specs=(P("row", "col"), P("row", "col")),
        out_specs=P(("row", "depth"), "col"),
        check_vma=False,
    )
```

```python
import functools

import jax
import jax.numpy as jnp
from jax import lax
from jax.experimental import pallas as pl
from jax.experimental.pallas import tpu as pltpu
from jax.sharding import PartitionSpec as P

MESH = pl.DeviceIdType.MESH
NX = 4
PIECES = [(2, 0), (2, 1), (2, 2), (1, 0), (3, 0), (1, 1), (3, 1), (1, 2), (3, 2), (0, 3), (0, 2)]
GROUPS = [(0, 4), (4, 4), (8, 8), (0, 8)]
NG = 3
SLOT = {2: 0, 1: 1, 3: 2, 0: 0}
SCRIPT = """P0 P1 G0 P3 P4 G1 P2 P5 P6 L0 R0 O0 C0a C0b G2 G3 G4 P7 P8 L1 R1 O1 C1a C1b G5 G6 P9 P10 L2 R2 O2 C2a C2b
L3 R3 O3 C3a G9 L4 R4 O4 C3b G7 G8 C4a C4b A0 L5 R5 O5 C5a L6 R6 O6 C5b C6a C6b A1 G10 L9 R9 O9 C9a C9b F0
L7 R7 O7 C7a L8 R8 O8 C7b C8a C8b A2 F1 L10 R10 O10 C10a C10b W F2"""


def chunk_order(nz):
    return sorted(range(nz), key=lambda r: -min(r, nz - r))


def kernel(nz, ny, a_ref, b_ref, o_ref, abuf, bbuf, ro, rn, pbuf, obuf,
           a_sem, b_send, b_recv, s_recv, op_send, op_recv, nb_send, nb_recv, out_send, out_recv, own_sem):
    z = lax.axis_index("depth")
    y = lax.axis_index("col")
    i = lax.axis_index("row")
    x, c = i // 2, i % 2
    rows, depth_k = abuf.shape
    half_k = depth_k // 2
    quarter = half_k // NX
    width = depth_k // nz
    unit = width // 16
    chunk = rows // nz
    mblk = rows // 4
    half = rows // 2
    order_z = chunk_order(nz)

    def dev(zz, yy, xx, cc):
        return ((zz + nz) % nz, (yy + ny) % ny, 2 * ((xx + NX) % NX) + cc)

    def remote(src, dst, send_sem, recv_sem, device):
        return pltpu.make_async_remote_copy(src_ref=src, dst_ref=dst, send_sem=send_sem, recv_sem=recv_sem,
                                            device_id=device, device_id_type=MESH)

    sibling = dev(z, y, x, 1 - c)
    left, right, far = dev(z, y, x - 1, c), dev(z, y, x + 1, c), dev(z, y, x + 2, c)

    a_copies = [pltpu.make_async_copy(a_ref.at[pl.ds(m * mblk, mblk)], abuf.at[pl.ds(m * mblk, mblk)], a_sem)
                for m in range(4)]
    for cp in a_copies:
        cp.start()

    barrier = pltpu.get_barrier_semaphore()
    partners = [sibling]
    partners += [dev(z, y + dy, x + dx, c) for dy in range(ny) for dx in range(NX) if dx or dy]
    partners += [dev(z + r, y, x, c) for r in range(1, nz)]
    for p in partners:
        pl.semaphore_signal(barrier, inc=1, device_id=p, device_id_type=MESH)
    pl.semaphore_wait(barrier, len(partners))

    t_me = (y - x + NX) % NX

    def group_columns(s):
        return pl.ds(GROUPS[s][0] * unit, GROUPS[s][1] * unit)

    def columns(n):
        return group_columns(PIECES[n][1])

    def stage1(n, d):
        t, group = PIECES[n]
        first, wide = GROUPS[group]
        q = (x + d) % NX
        cols = pl.ds(pl.multiple_of(z * width + first * unit, 4 * unit), wide * unit)
        src = b_ref.at[pl.ds(pl.multiple_of(q * quarter, quarter), quarter), cols]
        dst = bbuf.at[t, pl.ds(pl.multiple_of(c * half_k + q * quarter, quarter), quarter), columns(n)]
        if t == 0 and d == 0:
            return pltpu.make_async_copy(src, dst, b_recv.at[n, 0])
        return remote(src, dst, b_send, b_recv.at[n, 0], dev(z, x, q, c))

    def stage1_start(n, ds):
        @pl.when(t_me == PIECES[n][0])
        def _():
            for d in ds:
                stage1(n, d).start()

    def part(n, k):
        q = (x + (0, 3, 1, 2)[k]) % NX
        start = c * half_k + q * quarter
        return bbuf.at[PIECES[n][0], pl.ds(pl.multiple_of(start, quarter), quarter), columns(n)]

    def lane(n, cc):
        return bbuf.at[PIECES[n][0], pl.ds(pl.multiple_of(cc * half_k, half_k), half_k), columns(n)]

    def arrived(n, k):
        ref = part(n, k)
        remote(ref, ref, b_send, b_recv.at[n, k], sibling).wait_recv()

    def to_sibling(n, k):
        ref = part(n, k)
        remote(ref, ref, b_send, s_recv.at[n], sibling).start()

    def pass_own(n):
        arrived(n, 0)
        ref = part(n, 0)
        for k, target in ((3, far), (1, right), (2, left)):
            remote(ref, ref, b_send, b_recv.at[n, k], target).start()
        to_sibling(n, 0)

    def pass_on(n, k):
        arrived(n, k)
        to_sibling(n, k)

    def group_columns(s):
        return pl.ds(GROUPS[s][0] * unit, GROUPS[s][1] * unit)

    def opposite_copy(s, d, h):
        src = pbuf.at[0, pl.ds(pl.multiple_of(d * half + h * mblk, mblk), mblk), group_columns(s)]
        return remote(src, ro.at[d, pl.ds(h * mblk, mblk), group_columns(s)], op_send.at[s], op_recv.at[s, d],
                      dev(z, y + 1 - 2 * d, x, c))

    def half_matmul(n, h):
        t, group = PIECES[n]
        if h == 0:
            ref = lane(n, 1 - c)
            remote(ref, ref, b_send, s_recv.at[n], sibling).wait_recv()
            if n == 0:
                pltpu.make_async_copy(abuf, abuf, a_sem).wait()
            if t == 0:
                for m in (0, 1) if group == 3 else (2,):
                    ref = pbuf.at[0, :, group_columns(m)]
                    remote(ref, ref, op_send.at[m], op_recv.at[m, 0], sibling).wait_send()

        def body(d, carry):
            r = pl.ds(pl.multiple_of(d * half + h * mblk, mblk), mblk)
            pbuf[SLOT[t], r, columns(n)] = jnp.dot(abuf[r, :], bbuf[t, :, columns(n)],
                                                   preferred_element_type=jnp.float32)
            if t == 2:
                opposite_copy(group, d, h).start()
            return carry

        lax.fori_loop(0, 2, body, 0)

    def chunk_rows(zz):
        return pl.ds(pl.multiple_of(zz * chunk, chunk), chunk)

    def neighbour_copy(d, s, zz):
        cr, cols = chunk_rows(zz), group_columns(s)
        return remote(pbuf.at[1 + d, cr, cols], rn.at[d, cr, cols], nb_send, nb_recv.at[d, s, zz],
                      dev(z, y + 1 - 2 * d, x, c))

    def send_half(s, merged):
        nh = max(nz // 2, 1)
        for j in range(nh):
            for d in (0, 1):
                neighbour_copy(d, s, ((d if merged else 1 - d) * nh + (z + j) % nh) % nz).start()

    def merge(s):
        cols = group_columns(s)
        for d in (0, 1):
            ref = ro.at[d, :, group_columns(s)]
            remote(ref, ref, op_send.at[s], op_recv.at[s, d], sibling).wait_recv()
        for d in (0, 1):
            def body(m, carry):
                r = pl.ds(pl.multiple_of(m * (half // 4), half // 4), half // 4)
                rp = pl.ds(pl.multiple_of(d * half + m * (half // 4), half // 4), half // 4)
                pbuf[1 + d, rp, cols] = pbuf[1 + d, rp, cols] + ro[d, r, cols]
                return carry

            lax.fori_loop(0, 4, body, 0)

    def send_all(s):
        for r in order_z:
            for d in (0, 1):
                neighbour_copy(d, s, (z + r) % nz).start()

    def out_columns(zz, s):
        return pl.ds(pl.multiple_of(zz * width + GROUPS[s][0] * unit, 4 * unit), GROUPS[s][1] * unit)

    def out_copy(s, r):
        src = obuf.at[chunk_rows((z + r) % nz), group_columns(s)]
        dst = o_ref.at[:, out_columns(z, s)]
        if r == 0:
            return pltpu.make_async_copy(src, dst, own_sem.at[s])
        return remote(src, dst, out_send, out_recv, dev(z + r, y, x, c))

    def finish(s):
        cols = group_columns(s)
        for r in order_z:
            for d in (0, 1):
                neighbour_copy(d, s, (z + r) % nz).wait_recv()
            cr = chunk_rows((z + r) % nz)
            total = pbuf[0, cr, cols] + rn[0, cr, cols] + rn[1, cr, cols]
            obuf[cr, cols] = total.astype(jnp.bfloat16)
            out_copy(s, r).start()

    for item in SCRIPT.split():
        op, rest = item[0], item[1:]
        if op == "P":
            stage1_start(int(rest), (0, 2, 1, 3))
        elif op == "G":
            pass_own(int(rest))
        elif op == "L":
            pass_on(int(rest), 1)
        elif op == "R":
            pass_on(int(rest), 2)
        elif op == "O":
            pass_on(int(rest), 3)
        elif op == "C":
            half_matmul(int(rest[:-1]), "ab".index(rest[-1]))
        elif op == "U":
            send_half(int(rest), False)
        elif op == "M":
            merge(int(rest))
            send_half(int(rest), True)
        elif op == "A":
            merge(int(rest))
            send_all(int(rest))
        elif op == "F":
            finish(int(rest))
        elif op == "W":
            @pl.when(t_me != 0)
            def _():
                remote(bbuf, bbuf, b_send, out_recv, sibling).wait_send()

            @pl.when(t_me == 0)
            def _():
                ref = bbuf.at[:, pl.ds(0, 2 * half_k - quarter // NX)]
                remote(ref, ref, b_send, out_recv, sibling).wait_send()

    remote(rn, rn, nb_send, out_recv, sibling).wait_send()
    for s in range(NG):
        out_copy(s, 0).wait()
    sent = obuf.at[pl.ds(0, rows - chunk)]
    remote(sent, sent, out_send, out_recv, sibling).wait_send()
    got = o_ref.at[pl.ds(0, chunk - chunk // nz)]
    remote(got, got, out_send, out_recv, sibling).wait_recv()


COPIES = 4


def copy_kernel(src_ref, dst_ref, buf, in_sem, out_sem):
    n = buf.shape[0] // COPIES
    blocks = [pl.ds(m * n, n) for m in range(COPIES)]
    ins = [pltpu.make_async_copy(src_ref.at[b], buf.at[b], in_sem.at[m]) for m, b in enumerate(blocks)]
    outs = [pltpu.make_async_copy(buf.at[b], dst_ref.at[b], out_sem.at[m]) for m, b in enumerate(blocks)]
    for cp in ins:
        cp.start()
    for cp_in, cp_out in zip(ins, outs):
        cp_in.wait()
        cp_out.start()
    for cp in outs:
        cp.wait()


def copy_out(c_rows):
    return pl.pallas_call(
        copy_kernel,
        name="copy_out",
        out_shape=jax.ShapeDtypeStruct(c_rows.shape, c_rows.dtype),
        in_specs=[pl.BlockSpec(memory_space=pl.ANY)],
        out_specs=pl.BlockSpec(memory_space=pl.ANY),
        scratch_shapes=[pltpu.VMEM(c_rows.shape, c_rows.dtype), pltpu.SemaphoreType.DMA((COPIES,)),
                        pltpu.SemaphoreType.DMA((COPIES,))],
    )(c_rows)


def local_product(nz, ny, a_blk, b_blk):
    rows, depth_k = a_blk.shape
    half_k = b_blk.shape[0]
    width = depth_k // nz
    f32, bf16 = jnp.float32, jnp.bfloat16
    dma = pltpu.SemaphoreType.DMA
    n = len(PIECES)
    return copy_out(pl.pallas_call(
        functools.partial(kernel, nz, ny),
        name="stationary_a",
        out_shape=jax.ShapeDtypeStruct((rows // nz, depth_k), bf16),
        in_specs=[pl.BlockSpec(memory_space=pl.ANY)] * 2,
        out_specs=pl.BlockSpec(memory_space=pl.ANY),
        scratch_shapes=[
            pltpu.VMEM((rows, depth_k), bf16),
            pltpu.VMEM((NX, 2 * half_k, width), bf16),
            pltpu.VMEM((2, rows // 2, width), f32),
            pltpu.VMEM((2, rows, width), f32),
            pltpu.VMEM((3, rows, width), f32),
            pltpu.VMEM((rows, width), bf16),
            dma,
            dma,
            dma((n, 4)),
            dma((n,)),
            dma((NG,)),
            dma((NG, 2)),
            dma,
            dma((2, NG, nz)),
            dma,
            dma,
            dma((NG,)),
        ],
        compiler_params=pltpu.CompilerParams(collective_id=0, has_side_effects=True, vmem_limit_bytes=67043328),
    )(a_blk, b_blk))


def solution(mesh):
    nz, ny = mesh.shape["depth"], mesh.shape["col"]
    return jax.shard_map(
        functools.partial(local_product, nz, ny),
        mesh=mesh,
        in_specs=(P("row", "col"), P("row", "col")),
        out_specs=P(("row", "depth"), "col"),
        check_vma=False,
    )
```

```python
import functools

import jax
import jax.numpy as jnp
from jax import lax
from jax.experimental import pallas as pl
from jax.experimental.pallas import tpu as pltpu
from jax.sharding import PartitionSpec as P

MESH = pl.DeviceIdType.MESH
NX = 4
PIECES = [(2, 0), (2, 1), (2, 2), (1, 0), (3, 0), (1, 1), (3, 1), (1, 2), (3, 2), (0, 3), (0, 2)]
GROUPS = [(0, 4), (4, 4), (8, 8), (0, 8)]
NG = 3
SLOT = {2: 0, 1: 1, 3: 2, 0: 0}
SCRIPT = """P0 P3 P4 P1 P5 P6 G0 P2 G1 L0 R0 O0 C0a G2 C0b P7 P8 G3 G4 L1 R1 O1 C1a C1b G5 G6 P9 P10 L2 R2 O2 C2a C2b
L3 R3 O3 C3a L4 R4 O4 C3b C4a C4b A0 G7 G8 G9 L5 R5 O5 C5a L6 R6 O6 C5b C6a C6b A1 G10 L9 R9 O9 C9a C9b F0
L7 R7 O7 C7a L8 R8 O8 C7b C8a C8b A2 F1 L10 R10 O10 C10a C10b W F2"""


def chunk_order(nz):
    return sorted(range(nz), key=lambda r: -min(r, nz - r))


def kernel(nz, ny, a_ref, b_ref, o_ref, abuf, bbuf, ro, rn, pbuf, obuf,
           a_sem, b_send, b_recv, s_recv, op_send, op_recv, nb_send, nb_recv, out_send, out_recv, own_sem):
    z = lax.axis_index("depth")
    y = lax.axis_index("col")
    i = lax.axis_index("row")
    x, c = i // 2, i % 2
    rows, depth_k = abuf.shape
    half_k = depth_k // 2
    quarter = half_k // NX
    width = depth_k // nz
    unit = width // 16
    chunk = rows // nz
    mblk = rows // 4
    half = rows // 2
    order_z = chunk_order(nz)

    def dev(zz, yy, xx, cc):
        return ((zz + nz) % nz, (yy + ny) % ny, 2 * ((xx + NX) % NX) + cc)

    def remote(src, dst, send_sem, recv_sem, device):
        return pltpu.make_async_remote_copy(src_ref=src, dst_ref=dst, send_sem=send_sem, recv_sem=recv_sem,
                                            device_id=device, device_id_type=MESH)

    sibling = dev(z, y, x, 1 - c)
    left, right, far = dev(z, y, x - 1, c), dev(z, y, x + 1, c), dev(z, y, x + 2, c)

    a_copies = [pltpu.make_async_copy(a_ref.at[pl.ds(m * mblk, mblk)], abuf.at[pl.ds(m * mblk, mblk)], a_sem)
                for m in range(4)]
    for cp in a_copies:
        cp.start()

    barrier = pltpu.get_barrier_semaphore()
    partners = [sibling]
    partners += [dev(z, y + dy, x + dx, c) for dy in range(ny) for dx in range(NX) if dx or dy]
    partners += [dev(z + r, y, x, c) for r in range(1, nz)]
    for p in partners:
        pl.semaphore_signal(barrier, inc=1, device_id=p, device_id_type=MESH)
    pl.semaphore_wait(barrier, len(partners))

    t_me = (y - x + NX) % NX

    def group_columns(s):
        return pl.ds(GROUPS[s][0] * unit, GROUPS[s][1] * unit)

    def columns(n):
        return group_columns(PIECES[n][1])

    def stage1(n, d):
        t, group = PIECES[n]
        first, wide = GROUPS[group]
        q = (x + d) % NX
        cols = pl.ds(pl.multiple_of(z * width + first * unit, 4 * unit), wide * unit)
        src = b_ref.at[pl.ds(pl.multiple_of(q * quarter, quarter), quarter), cols]
        dst = bbuf.at[t, pl.ds(pl.multiple_of(c * half_k + q * quarter, quarter), quarter), columns(n)]
        if t == 0 and d == 0:
            return pltpu.make_async_copy(src, dst, b_recv.at[n, 0])
        return remote(src, dst, b_send, b_recv.at[n, 0], dev(z, x, q, c))

    def stage1_start(n, ds):
        @pl.when(t_me == PIECES[n][0])
        def _():
            for d in ds:
                stage1(n, d).start()

    def part(n, k):
        q = (x + (0, 3, 1, 2)[k]) % NX
        start = c * half_k + q * quarter
        return bbuf.at[PIECES[n][0], pl.ds(pl.multiple_of(start, quarter), quarter), columns(n)]

    def lane(n, cc):
        return bbuf.at[PIECES[n][0], pl.ds(pl.multiple_of(cc * half_k, half_k), half_k), columns(n)]

    def arrived(n, k):
        ref = part(n, k)
        remote(ref, ref, b_send, b_recv.at[n, k], sibling).wait_recv()

    def to_sibling(n, k):
        ref = part(n, k)
        remote(ref, ref, b_send, s_recv.at[n], sibling).start()

    def pass_own(n):
        arrived(n, 0)
        ref = part(n, 0)
        for k, target in ((3, far), (1, right), (2, left)):
            remote(ref, ref, b_send, b_recv.at[n, k], target).start()
        to_sibling(n, 0)

    def pass_on(n, k):
        arrived(n, k)
        to_sibling(n, k)

    def group_columns(s):
        return pl.ds(GROUPS[s][0] * unit, GROUPS[s][1] * unit)

    def opposite_copy(s, d, h):
        src = pbuf.at[0, pl.ds(pl.multiple_of(d * half + h * mblk, mblk), mblk), group_columns(s)]
        return remote(src, ro.at[d, pl.ds(h * mblk, mblk), group_columns(s)], op_send.at[s], op_recv.at[s, d],
                      dev(z, y + 1 - 2 * d, x, c))

    def half_matmul(n, h):
        t, group = PIECES[n]
        if h == 0:
            ref = lane(n, 1 - c)
            remote(ref, ref, b_send, s_recv.at[n], sibling).wait_recv()
            if n == 0:
                pltpu.make_async_copy(abuf, abuf, a_sem).wait()
            if t == 0:
                for m in (0, 1) if group == 3 else (2,):
                    ref = pbuf.at[0, :, group_columns(m)]
                    remote(ref, ref, op_send.at[m], op_recv.at[m, 0], sibling).wait_send()

        def body(d, carry):
            r = pl.ds(pl.multiple_of(d * half + h * mblk, mblk), mblk)
            pbuf[SLOT[t], r, columns(n)] = jnp.dot(abuf[r, :], bbuf[t, :, columns(n)],
                                                   preferred_element_type=jnp.float32)
            if t == 2:
                opposite_copy(group, d, h).start()
            return carry

        lax.fori_loop(0, 2, body, 0)

    def chunk_rows(zz):
        return pl.ds(pl.multiple_of(zz * chunk, chunk), chunk)

    def neighbour_copy(d, s, zz):
        cr, cols = chunk_rows(zz), group_columns(s)
        return remote(pbuf.at[1 + d, cr, cols], rn.at[d, cr, cols], nb_send, nb_recv.at[d, s, zz],
                      dev(z, y + 1 - 2 * d, x, c))

    def send_half(s, merged):
        nh = max(nz // 2, 1)
        for j in range(nh):
            for d in (0, 1):
                neighbour_copy(d, s, ((d if merged else 1 - d) * nh + (z + j) % nh) % nz).start()

    def merge(s):
        cols = group_columns(s)
        for d in (0, 1):
            ref = ro.at[d, :, group_columns(s)]
            remote(ref, ref, op_send.at[s], op_recv.at[s, d], sibling).wait_recv()
        for d in (0, 1):
            def body(m, carry):
                r = pl.ds(pl.multiple_of(m * (half // 4), half // 4), half // 4)
                rp = pl.ds(pl.multiple_of(d * half + m * (half // 4), half // 4), half // 4)
                pbuf[1 + d, rp, cols] = pbuf[1 + d, rp, cols] + ro[d, r, cols]
                return carry

            lax.fori_loop(0, 4, body, 0)

    def send_all(s):
        for r in order_z:
            for d in (0, 1):
                neighbour_copy(d, s, (z + r) % nz).start()

    def out_columns(zz, s):
        return pl.ds(pl.multiple_of(zz * width + GROUPS[s][0] * unit, 4 * unit), GROUPS[s][1] * unit)

    def out_copy(s, r):
        src = obuf.at[chunk_rows((z + r) % nz), group_columns(s)]
        dst = o_ref.at[:, out_columns(z, s)]
        if r == 0:
            return pltpu.make_async_copy(src, dst, own_sem.at[s])
        return remote(src, dst, out_send, out_recv, dev(z + r, y, x, c))

    def finish(s):
        cols = group_columns(s)
        for r in order_z:
            for d in (0, 1):
                neighbour_copy(d, s, (z + r) % nz).wait_recv()
            cr = chunk_rows((z + r) % nz)
            total = pbuf[0, cr, cols] + rn[0, cr, cols] + rn[1, cr, cols]
            obuf[cr, cols] = total.astype(jnp.bfloat16)
            out_copy(s, r).start()

    for item in SCRIPT.split():
        op, rest = item[0], item[1:]
        if op == "P":
            stage1_start(int(rest), (0, 2, 1, 3))
        elif op == "G":
            pass_own(int(rest))
        elif op == "L":
            pass_on(int(rest), 1)
        elif op == "R":
            pass_on(int(rest), 2)
        elif op == "O":
            pass_on(int(rest), 3)
        elif op == "C":
            half_matmul(int(rest[:-1]), "ab".index(rest[-1]))
        elif op == "U":
            send_half(int(rest), False)
        elif op == "M":
            merge(int(rest))
            send_half(int(rest), True)
        elif op == "A":
            merge(int(rest))
            send_all(int(rest))
        elif op == "F":
            finish(int(rest))
        elif op == "W":
            @pl.when(t_me != 0)
            def _():
                remote(bbuf, bbuf, b_send, out_recv, sibling).wait_send()

            @pl.when(t_me == 0)
            def _():
                ref = bbuf.at[:, pl.ds(0, 2 * half_k - quarter // NX)]
                remote(ref, ref, b_send, out_recv, sibling).wait_send()

    remote(rn, rn, nb_send, out_recv, sibling).wait_send()
    for s in range(NG):
        out_copy(s, 0).wait()
    sent = obuf.at[pl.ds(0, rows - chunk)]
    remote(sent, sent, out_send, out_recv, sibling).wait_send()
    got = o_ref.at[pl.ds(0, chunk - chunk // nz)]
    remote(got, got, out_send, out_recv, sibling).wait_recv()


COPIES = 4


def copy_kernel(src_ref, dst_ref, buf, in_sem, out_sem):
    n = buf.shape[0] // COPIES
    blocks = [pl.ds(m * n, n) for m in range(COPIES)]
    ins = [pltpu.make_async_copy(src_ref.at[b], buf.at[b], in_sem.at[m]) for m, b in enumerate(blocks)]
    outs = [pltpu.make_async_copy(buf.at[b], dst_ref.at[b], out_sem.at[m]) for m, b in enumerate(blocks)]
    for cp in ins:
        cp.start()
    for cp_in, cp_out in zip(ins, outs):
        cp_in.wait()
        cp_out.start()
    for cp in outs:
        cp.wait()


def copy_out(c_rows):
    return pl.pallas_call(
        copy_kernel,
        name="copy_out",
        out_shape=jax.ShapeDtypeStruct(c_rows.shape, c_rows.dtype),
        in_specs=[pl.BlockSpec(memory_space=pl.ANY)],
        out_specs=pl.BlockSpec(memory_space=pl.ANY),
        scratch_shapes=[pltpu.VMEM(c_rows.shape, c_rows.dtype), pltpu.SemaphoreType.DMA((COPIES,)),
                        pltpu.SemaphoreType.DMA((COPIES,))],
    )(c_rows)


def local_product(nz, ny, a_blk, b_blk):
    rows, depth_k = a_blk.shape
    half_k = b_blk.shape[0]
    width = depth_k // nz
    f32, bf16 = jnp.float32, jnp.bfloat16
    dma = pltpu.SemaphoreType.DMA
    n = len(PIECES)
    return copy_out(pl.pallas_call(
        functools.partial(kernel, nz, ny),
        name="stationary_a",
        out_shape=jax.ShapeDtypeStruct((rows // nz, depth_k), bf16),
        in_specs=[pl.BlockSpec(memory_space=pl.ANY)] * 2,
        out_specs=pl.BlockSpec(memory_space=pl.ANY),
        scratch_shapes=[
            pltpu.VMEM((rows, depth_k), bf16),
            pltpu.VMEM((NX, 2 * half_k, width), bf16),
            pltpu.VMEM((2, rows // 2, width), f32),
            pltpu.VMEM((2, rows, width), f32),
            pltpu.VMEM((3, rows, width), f32),
            pltpu.VMEM((rows, width), bf16),
            dma,
            dma,
            dma((n, 4)),
            dma((n,)),
            dma((NG,)),
            dma((NG, 2)),
            dma,
            dma((2, NG, nz)),
            dma,
            dma,
            dma((NG,)),
        ],
        compiler_params=pltpu.CompilerParams(collective_id=0, has_side_effects=True, vmem_limit_bytes=67043328),
    )(a_blk, b_blk))


def solution(mesh):
    nz, ny = mesh.shape["depth"], mesh.shape["col"]
    return jax.shard_map(
        functools.partial(local_product, nz, ny),
        mesh=mesh,
        in_specs=(P("row", "col"), P("row", "col")),
        out_specs=P(("row", "depth"), "col"),
        check_vma=False,
    )
```

```python
import functools

import jax
import jax.numpy as jnp
from jax import lax
from jax.experimental import pallas as pl
from jax.experimental.pallas import tpu as pltpu
from jax.sharding import PartitionSpec as P

MESH = pl.DeviceIdType.MESH
NX = 4
PIECES = [(2, 0), (2, 1), (2, 2), (1, 0), (3, 0), (1, 1), (3, 1), (1, 2), (3, 2), (0, 3), (0, 2)]
GROUPS = [(0, 4), (4, 4), (8, 8), (0, 8)]
NG = 3
SLOT = {2: 0, 1: 1, 3: 2, 0: 0}
SCRIPT = """P0 P3 P4 P1 P5 P6 G0 P2 G1 L0 R0 O0 C0a G2 C0b P7 P8 G3 G4 L1 R1 O1 C1a C1b G5 G6 P9 P10 L2 R2 O2 C2a C2b
L3 R3 O3 C3a L4 R4 O4 C3b C4a C4b A0 G9 G7 G8 L5 R5 O5 C5a L6 R6 O6 C5b C6a C6b A1 G10 L9 R9 O9 C9a C9b F0
L7 R7 O7 C7a L8 R8 O8 C7b C8a C8b A2 F1 L10 R10 O10 C10a C10b W F2"""


def chunk_order(nz):
    return sorted(range(nz), key=lambda r: -min(r, nz - r))


def kernel(nz, ny, a_ref, b_ref, o_ref, abuf, bbuf, ro, rn, pbuf, obuf,
           a_sem, b_send, b_recv, s_recv, op_send, op_recv, nb_send, nb_recv, out_send, out_recv, own_sem):
    z = lax.axis_index("depth")
    y = lax.axis_index("col")
    i = lax.axis_index("row")
    x, c = i // 2, i % 2
    rows, depth_k = abuf.shape
    half_k = depth_k // 2
    quarter = half_k // NX
    width = depth_k // nz
    unit = width // 16
    chunk = rows // nz
    mblk = rows // 4
    half = rows // 2
    order_z = chunk_order(nz)

    def dev(zz, yy, xx, cc):
        return ((zz + nz) % nz, (yy + ny) % ny, 2 * ((xx + NX) % NX) + cc)

    def remote(src, dst, send_sem, recv_sem, device):
        return pltpu.make_async_remote_copy(src_ref=src, dst_ref=dst, send_sem=send_sem, recv_sem=recv_sem,
                                            device_id=device, device_id_type=MESH)

    sibling = dev(z, y, x, 1 - c)
    left, right, far = dev(z, y, x - 1, c), dev(z, y, x + 1, c), dev(z, y, x + 2, c)

    a_copies = [pltpu.make_async_copy(a_ref.at[pl.ds(m * mblk, mblk)], abuf.at[pl.ds(m * mblk, mblk)], a_sem)
                for m in range(4)]
    for cp in a_copies:
        cp.start()

    barrier = pltpu.get_barrier_semaphore()
    partners = [sibling]
    partners += [dev(z, y + dy, x + dx, c) for dy in range(ny) for dx in range(NX) if dx or dy]
    partners += [dev(z + r, y, x, c) for r in range(1, nz)]
    for p in partners:
        pl.semaphore_signal(barrier, inc=1, device_id=p, device_id_type=MESH)
    pl.semaphore_wait(barrier, len(partners))

    t_me = (y - x + NX) % NX

    def group_columns(s):
        return pl.ds(GROUPS[s][0] * unit, GROUPS[s][1] * unit)

    def columns(n):
        return group_columns(PIECES[n][1])

    def stage1(n, d):
        t, group = PIECES[n]
        first, wide = GROUPS[group]
        q = (x + d) % NX
        cols = pl.ds(pl.multiple_of(z * width + first * unit, 4 * unit), wide * unit)
        src = b_ref.at[pl.ds(pl.multiple_of(q * quarter, quarter), quarter), cols]
        dst = bbuf.at[t, pl.ds(pl.multiple_of(c * half_k + q * quarter, quarter), quarter), columns(n)]
        if t == 0 and d == 0:
            return pltpu.make_async_copy(src, dst, b_recv.at[n, 0])
        return remote(src, dst, b_send, b_recv.at[n, 0], dev(z, x, q, c))

    def stage1_start(n, ds):
        @pl.when(t_me == PIECES[n][0])
        def _():
            for d in ds:
                stage1(n, d).start()

    def part(n, k):
        q = (x + (0, 3, 1, 2)[k]) % NX
        start = c * half_k + q * quarter
        return bbuf.at[PIECES[n][0], pl.ds(pl.multiple_of(start, quarter), quarter), columns(n)]

    def lane(n, cc):
        return bbuf.at[PIECES[n][0], pl.ds(pl.multiple_of(cc * half_k, half_k), half_k), columns(n)]

    def arrived(n, k):
        ref = part(n, k)
        remote(ref, ref, b_send, b_recv.at[n, k], sibling).wait_recv()

    def to_sibling(n, k):
        ref = part(n, k)
        remote(ref, ref, b_send, s_recv.at[n], sibling).start()

    def pass_own(n):
        arrived(n, 0)
        ref = part(n, 0)
        for k, target in ((3, far), (1, right), (2, left)):
            remote(ref, ref, b_send, b_recv.at[n, k], target).start()
        to_sibling(n, 0)

    def pass_on(n, k):
        arrived(n, k)
        to_sibling(n, k)

    def group_columns(s):
        return pl.ds(GROUPS[s][0] * unit, GROUPS[s][1] * unit)

    def opposite_copy(s, d, h):
        src = pbuf.at[0, pl.ds(pl.multiple_of(d * half + h * mblk, mblk), mblk), group_columns(s)]
        return remote(src, ro.at[d, pl.ds(h * mblk, mblk), group_columns(s)], op_send.at[s], op_recv.at[s, d],
                      dev(z, y + 1 - 2 * d, x, c))

    def half_matmul(n, h):
        t, group = PIECES[n]
        if h == 0:
            ref = lane(n, 1 - c)
            remote(ref, ref, b_send, s_recv.at[n], sibling).wait_recv()
            if n == 0:
                pltpu.make_async_copy(abuf, abuf, a_sem).wait()
            if t == 0:
                for m in (0, 1) if group == 3 else (2,):
                    ref = pbuf.at[0, :, group_columns(m)]
                    remote(ref, ref, op_send.at[m], op_recv.at[m, 0], sibling).wait_send()

        def body(d, carry):
            r = pl.ds(pl.multiple_of(d * half + h * mblk, mblk), mblk)
            pbuf[SLOT[t], r, columns(n)] = jnp.dot(abuf[r, :], bbuf[t, :, columns(n)],
                                                   preferred_element_type=jnp.float32)
            if t == 2:
                opposite_copy(group, d, h).start()
            return carry

        lax.fori_loop(0, 2, body, 0)

    def chunk_rows(zz):
        return pl.ds(pl.multiple_of(zz * chunk, chunk), chunk)

    def neighbour_copy(d, s, zz):
        cr, cols = chunk_rows(zz), group_columns(s)
        return remote(pbuf.at[1 + d, cr, cols], rn.at[d, cr, cols], nb_send, nb_recv.at[d, s, zz],
                      dev(z, y + 1 - 2 * d, x, c))

    def send_half(s, merged):
        nh = max(nz // 2, 1)
        for j in range(nh):
            for d in (0, 1):
                neighbour_copy(d, s, ((d if merged else 1 - d) * nh + (z + j) % nh) % nz).start()

    def merge(s):
        cols = group_columns(s)
        for d in (0, 1):
            ref = ro.at[d, :, group_columns(s)]
            remote(ref, ref, op_send.at[s], op_recv.at[s, d], sibling).wait_recv()
        for d in (0, 1):
            def body(m, carry):
                r = pl.ds(pl.multiple_of(m * (half // 4), half // 4), half // 4)
                rp = pl.ds(pl.multiple_of(d * half + m * (half // 4), half // 4), half // 4)
                pbuf[1 + d, rp, cols] = pbuf[1 + d, rp, cols] + ro[d, r, cols]
                return carry

            lax.fori_loop(0, 4, body, 0)

    def send_all(s):
        for r in order_z:
            for d in (0, 1):
                neighbour_copy(d, s, (z + r) % nz).start()

    def out_columns(zz, s):
        return pl.ds(pl.multiple_of(zz * width + GROUPS[s][0] * unit, 4 * unit), GROUPS[s][1] * unit)

    def out_copy(s, r):
        src = obuf.at[chunk_rows((z + r) % nz), group_columns(s)]
        dst = o_ref.at[:, out_columns(z, s)]
        if r == 0:
            return pltpu.make_async_copy(src, dst, own_sem.at[s])
        return remote(src, dst, out_send, out_recv, dev(z + r, y, x, c))

    def finish(s):
        cols = group_columns(s)
        for r in order_z:
            for d in (0, 1):
                neighbour_copy(d, s, (z + r) % nz).wait_recv()
            cr = chunk_rows((z + r) % nz)
            total = pbuf[0, cr, cols] + rn[0, cr, cols] + rn[1, cr, cols]
            obuf[cr, cols] = total.astype(jnp.bfloat16)
            out_copy(s, r).start()

    for item in SCRIPT.split():
        op, rest = item[0], item[1:]
        if op == "P":
            stage1_start(int(rest), (0, 2, 1, 3))
        elif op == "G":
            pass_own(int(rest))
        elif op == "L":
            pass_on(int(rest), 1)
        elif op == "R":
            pass_on(int(rest), 2)
        elif op == "O":
            pass_on(int(rest), 3)
        elif op == "C":
            half_matmul(int(rest[:-1]), "ab".index(rest[-1]))
        elif op == "U":
            send_half(int(rest), False)
        elif op == "M":
            merge(int(rest))
            send_half(int(rest), True)
        elif op == "A":
            merge(int(rest))
            send_all(int(rest))
        elif op == "F":
            finish(int(rest))
        elif op == "W":
            @pl.when(t_me != 0)
            def _():
                remote(bbuf, bbuf, b_send, out_recv, sibling).wait_send()

            @pl.when(t_me == 0)
            def _():
                ref = bbuf.at[:, pl.ds(0, 2 * half_k - quarter // NX)]
                remote(ref, ref, b_send, out_recv, sibling).wait_send()

    remote(rn, rn, nb_send, out_recv, sibling).wait_send()
    for s in range(NG):
        out_copy(s, 0).wait()
    sent = obuf.at[pl.ds(0, rows - chunk)]
    remote(sent, sent, out_send, out_recv, sibling).wait_send()
    got = o_ref.at[pl.ds(0, chunk - chunk // nz)]
    remote(got, got, out_send, out_recv, sibling).wait_recv()


COPIES = 4


def copy_kernel(src_ref, dst_ref, buf, in_sem, out_sem):
    n = buf.shape[0] // COPIES
    blocks = [pl.ds(m * n, n) for m in range(COPIES)]
    ins = [pltpu.make_async_copy(src_ref.at[b], buf.at[b], in_sem.at[m]) for m, b in enumerate(blocks)]
    outs = [pltpu.make_async_copy(buf.at[b], dst_ref.at[b], out_sem.at[m]) for m, b in enumerate(blocks)]
    for cp in ins:
        cp.start()
    for cp_in, cp_out in zip(ins, outs):
        cp_in.wait()
        cp_out.start()
    for cp in outs:
        cp.wait()


def copy_out(c_rows):
    return pl.pallas_call(
        copy_kernel,
        name="copy_out",
        out_shape=jax.ShapeDtypeStruct(c_rows.shape, c_rows.dtype),
        in_specs=[pl.BlockSpec(memory_space=pl.ANY)],
        out_specs=pl.BlockSpec(memory_space=pl.ANY),
        scratch_shapes=[pltpu.VMEM(c_rows.shape, c_rows.dtype), pltpu.SemaphoreType.DMA((COPIES,)),
                        pltpu.SemaphoreType.DMA((COPIES,))],
    )(c_rows)


def local_product(nz, ny, a_blk, b_blk):
    rows, depth_k = a_blk.shape
    half_k = b_blk.shape[0]
    width = depth_k // nz
    f32, bf16 = jnp.float32, jnp.bfloat16
    dma = pltpu.SemaphoreType.DMA
    n = len(PIECES)
    return copy_out(pl.pallas_call(
        functools.partial(kernel, nz, ny),
        name="stationary_a",
        out_shape=jax.ShapeDtypeStruct((rows // nz, depth_k), bf16),
        in_specs=[pl.BlockSpec(memory_space=pl.ANY)] * 2,
        out_specs=pl.BlockSpec(memory_space=pl.ANY),
        scratch_shapes=[
            pltpu.VMEM((rows, depth_k), bf16),
            pltpu.VMEM((NX, 2 * half_k, width), bf16),
            pltpu.VMEM((2, rows // 2, width), f32),
            pltpu.VMEM((2, rows, width), f32),
            pltpu.VMEM((3, rows, width), f32),
            pltpu.VMEM((rows, width), bf16),
            dma,
            dma,
            dma((n, 4)),
            dma((n,)),
            dma((NG,)),
            dma((NG, 2)),
            dma,
            dma((2, NG, nz)),
            dma,
            dma,
            dma((NG,)),
        ],
        compiler_params=pltpu.CompilerParams(collective_id=0, has_side_effects=True, vmem_limit_bytes=67043328),
    )(a_blk, b_blk))


def solution(mesh):
    nz, ny = mesh.shape["depth"], mesh.shape["col"]
    return jax.shard_map(
        functools.partial(local_product, nz, ny),
        mesh=mesh,
        in_specs=(P("row", "col"), P("row", "col")),
        out_specs=P(("row", "depth"), "col"),
        check_vma=False,
    )
```

```python
import functools

import jax
import jax.numpy as jnp
from jax import lax
from jax.experimental import pallas as pl
from jax.experimental.pallas import tpu as pltpu
from jax.sharding import PartitionSpec as P

MESH = pl.DeviceIdType.MESH
NX = 4
PIECES = [(2, 0), (2, 1), (2, 2), (1, 0), (3, 0), (1, 1), (3, 1), (1, 2), (3, 2), (0, 3), (0, 2)]
GROUPS = [(0, 4), (4, 4), (8, 8), (0, 8)]
NG = 3
SLOT = {2: 0, 1: 1, 3: 2, 0: 0}
SCRIPT = """P0 P3 P4 P1 G0 P2 G1 P5 P6 L0 R0 O0 C0a G2 C0b P7 P8 G3 G4 L1 R1 O1 C1a C1b G5 G6 P9 P10 L2 R2 O2 C2a C2b
L3 R3 O3 C3a L4 R4 O4 C3b C4a C4b A0 G9 G7 G8 L5 R5 O5 C5a L6 R6 O6 C5b C6a C6b A1 G10 L9 R9 O9 C9a C9b F0
L7 R7 O7 C7a L8 R8 O8 C7b C8a C8b A2 F1 L10 R10 O10 C10a C10b W F2"""


def chunk_order(nz):
    return sorted(range(nz), key=lambda r: -min(r, nz - r))


def kernel(nz, ny, a_ref, b_ref, o_ref, abuf, bbuf, ro, rn, pbuf, obuf,
           a_sem, b_send, b_recv, s_recv, op_send, op_recv, nb_send, nb_recv, out_send, out_recv, own_sem):
    z = lax.axis_index("depth")
    y = lax.axis_index("col")
    i = lax.axis_index("row")
    x, c = i // 2, i % 2
    rows, depth_k = abuf.shape
    half_k = depth_k // 2
    quarter = half_k // NX
    width = depth_k // nz
    unit = width // 16
    chunk = rows // nz
    mblk = rows // 4
    half = rows // 2
    order_z = chunk_order(nz)

    def dev(zz, yy, xx, cc):
        return ((zz + nz) % nz, (yy + ny) % ny, 2 * ((xx + NX) % NX) + cc)

    def remote(src, dst, send_sem, recv_sem, device):
        return pltpu.make_async_remote_copy(src_ref=src, dst_ref=dst, send_sem=send_sem, recv_sem=recv_sem,
                                            device_id=device, device_id_type=MESH)

    sibling = dev(z, y, x, 1 - c)
    left, right, far = dev(z, y, x - 1, c), dev(z, y, x + 1, c), dev(z, y, x + 2, c)

    a_copies = [pltpu.make_async_copy(a_ref.at[pl.ds(m * mblk, mblk)], abuf.at[pl.ds(m * mblk, mblk)], a_sem)
                for m in range(4)]
    for cp in a_copies:
        cp.start()

    barrier = pltpu.get_barrier_semaphore()
    partners = [sibling]
    partners += [dev(z, y + dy, x + dx, c) for dy in range(ny) for dx in range(NX) if dx or dy]
    partners += [dev(z + r, y, x, c) for r in range(1, nz)]
    for p in partners:
        pl.semaphore_signal(barrier, inc=1, device_id=p, device_id_type=MESH)
    pl.semaphore_wait(barrier, len(partners))

    t_me = (y - x + NX) % NX

    def group_columns(s):
        return pl.ds(GROUPS[s][0] * unit, GROUPS[s][1] * unit)

    def columns(n):
        return group_columns(PIECES[n][1])

    def stage1(n, d):
        t, group = PIECES[n]
        first, wide = GROUPS[group]
        q = (x + d) % NX
        cols = pl.ds(pl.multiple_of(z * width + first * unit, 4 * unit), wide * unit)
        src = b_ref.at[pl.ds(pl.multiple_of(q * quarter, quarter), quarter), cols]
        dst = bbuf.at[t, pl.ds(pl.multiple_of(c * half_k + q * quarter, quarter), quarter), columns(n)]
        if t == 0 and d == 0:
            return pltpu.make_async_copy(src, dst, b_recv.at[n, 0])
        return remote(src, dst, b_send, b_recv.at[n, 0], dev(z, x, q, c))

    def stage1_start(n, ds):
        @pl.when(t_me == PIECES[n][0])
        def _():
            for d in ds:
                stage1(n, d).start()

    def part(n, k):
        q = (x + (0, 3, 1, 2)[k]) % NX
        start = c * half_k + q * quarter
        return bbuf.at[PIECES[n][0], pl.ds(pl.multiple_of(start, quarter), quarter), columns(n)]

    def lane(n, cc):
        return bbuf.at[PIECES[n][0], pl.ds(pl.multiple_of(cc * half_k, half_k), half_k), columns(n)]

    def arrived(n, k):
        ref = part(n, k)
        remote(ref, ref, b_send, b_recv.at[n, k], sibling).wait_recv()

    def to_sibling(n, k):
        ref = part(n, k)
        remote(ref, ref, b_send, s_recv.at[n], sibling).start()

    def pass_own(n):
        arrived(n, 0)
        ref = part(n, 0)
        for k, target in ((3, far), (1, right), (2, left)):
            remote(ref, ref, b_send, b_recv.at[n, k], target).start()
        to_sibling(n, 0)

    def pass_on(n, k):
        arrived(n, k)
        to_sibling(n, k)

    def group_columns(s):
        return pl.ds(GROUPS[s][0] * unit, GROUPS[s][1] * unit)

    def opposite_copy(s, d, h):
        src = pbuf.at[0, pl.ds(pl.multiple_of(d * half + h * mblk, mblk), mblk), group_columns(s)]
        return remote(src, ro.at[d, pl.ds(h * mblk, mblk), group_columns(s)], op_send.at[s], op_recv.at[s, d],
                      dev(z, y + 1 - 2 * d, x, c))

    def half_matmul(n, h):
        t, group = PIECES[n]
        if h == 0:
            ref = lane(n, 1 - c)
            remote(ref, ref, b_send, s_recv.at[n], sibling).wait_recv()
            if n == 0:
                pltpu.make_async_copy(abuf, abuf, a_sem).wait()
            if t == 0:
                for m in (0, 1) if group == 3 else (2,):
                    ref = pbuf.at[0, :, group_columns(m)]
                    remote(ref, ref, op_send.at[m], op_recv.at[m, 0], sibling).wait_send()

        def body(d, carry):
            r = pl.ds(pl.multiple_of(d * half + h * mblk, mblk), mblk)
            pbuf[SLOT[t], r, columns(n)] = jnp.dot(abuf[r, :], bbuf[t, :, columns(n)],
                                                   preferred_element_type=jnp.float32)
            if t == 2:
                opposite_copy(group, d, h).start()
            return carry

        lax.fori_loop(0, 2, body, 0)

    def chunk_rows(zz):
        return pl.ds(pl.multiple_of(zz * chunk, chunk), chunk)

    def neighbour_copy(d, s, zz):
        cr, cols = chunk_rows(zz), group_columns(s)
        return remote(pbuf.at[1 + d, cr, cols], rn.at[d, cr, cols], nb_send, nb_recv.at[d, s, zz],
                      dev(z, y + 1 - 2 * d, x, c))

    def send_half(s, merged):
        nh = max(nz // 2, 1)
        for j in range(nh):
            for d in (0, 1):
                neighbour_copy(d, s, ((d if merged else 1 - d) * nh + (z + j) % nh) % nz).start()

    def merge(s):
        cols = group_columns(s)
        for d in (0, 1):
            ref = ro.at[d, :, group_columns(s)]
            remote(ref, ref, op_send.at[s], op_recv.at[s, d], sibling).wait_recv()
        for d in (0, 1):
            def body(m, carry):
                r = pl.ds(pl.multiple_of(m * (half // 4), half // 4), half // 4)
                rp = pl.ds(pl.multiple_of(d * half + m * (half // 4), half // 4), half // 4)
                pbuf[1 + d, rp, cols] = pbuf[1 + d, rp, cols] + ro[d, r, cols]
                return carry

            lax.fori_loop(0, 4, body, 0)

    def send_all(s):
        for r in order_z:
            for d in (0, 1):
                neighbour_copy(d, s, (z + r) % nz).start()

    def out_columns(zz, s):
        return pl.ds(pl.multiple_of(zz * width + GROUPS[s][0] * unit, 4 * unit), GROUPS[s][1] * unit)

    def out_copy(s, r):
        src = obuf.at[chunk_rows((z + r) % nz), group_columns(s)]
        dst = o_ref.at[:, out_columns(z, s)]
        if r == 0:
            return pltpu.make_async_copy(src, dst, own_sem.at[s])
        return remote(src, dst, out_send, out_recv, dev(z + r, y, x, c))

    def finish(s):
        cols = group_columns(s)
        for r in order_z:
            for d in (0, 1):
                neighbour_copy(d, s, (z + r) % nz).wait_recv()
            cr = chunk_rows((z + r) % nz)
            total = pbuf[0, cr, cols] + rn[0, cr, cols] + rn[1, cr, cols]
            obuf[cr, cols] = total.astype(jnp.bfloat16)
            out_copy(s, r).start()

    for item in SCRIPT.split():
        op, rest = item[0], item[1:]
        if op == "P":
            stage1_start(int(rest), (0, 2, 1, 3))
        elif op == "G":
            pass_own(int(rest))
        elif op == "L":
            pass_on(int(rest), 1)
        elif op == "R":
            pass_on(int(rest), 2)
        elif op == "O":
            pass_on(int(rest), 3)
        elif op == "C":
            half_matmul(int(rest[:-1]), "ab".index(rest[-1]))
        elif op == "U":
            send_half(int(rest), False)
        elif op == "M":
            merge(int(rest))
            send_half(int(rest), True)
        elif op == "A":
            merge(int(rest))
            send_all(int(rest))
        elif op == "F":
            finish(int(rest))
        elif op == "W":
            @pl.when(t_me != 0)
            def _():
                remote(bbuf, bbuf, b_send, out_recv, sibling).wait_send()

            @pl.when(t_me == 0)
            def _():
                ref = bbuf.at[:, pl.ds(0, 2 * half_k - quarter // NX)]
                remote(ref, ref, b_send, out_recv, sibling).wait_send()

    remote(rn, rn, nb_send, out_recv, sibling).wait_send()
    for s in range(NG):
        out_copy(s, 0).wait()
    sent = obuf.at[pl.ds(0, rows - chunk)]
    remote(sent, sent, out_send, out_recv, sibling).wait_send()
    got = o_ref.at[pl.ds(0, chunk - chunk // nz)]
    remote(got, got, out_send, out_recv, sibling).wait_recv()


COPIES = 4


def copy_kernel(src_ref, dst_ref, buf, in_sem, out_sem):
    n = buf.shape[0] // COPIES
    blocks = [pl.ds(m * n, n) for m in range(COPIES)]
    ins = [pltpu.make_async_copy(src_ref.at[b], buf.at[b], in_sem.at[m]) for m, b in enumerate(blocks)]
    outs = [pltpu.make_async_copy(buf.at[b], dst_ref.at[b], out_sem.at[m]) for m, b in enumerate(blocks)]
    for cp in ins:
        cp.start()
    for cp_in, cp_out in zip(ins, outs):
        cp_in.wait()
        cp_out.start()
    for cp in outs:
        cp.wait()


def copy_out(c_rows):
    return pl.pallas_call(
        copy_kernel,
        name="copy_out",
        out_shape=jax.ShapeDtypeStruct(c_rows.shape, c_rows.dtype),
        in_specs=[pl.BlockSpec(memory_space=pl.ANY)],
        out_specs=pl.BlockSpec(memory_space=pl.ANY),
        scratch_shapes=[pltpu.VMEM(c_rows.shape, c_rows.dtype), pltpu.SemaphoreType.DMA((COPIES,)),
                        pltpu.SemaphoreType.DMA((COPIES,))],
    )(c_rows)


def local_product(nz, ny, a_blk, b_blk):
    rows, depth_k = a_blk.shape
    half_k = b_blk.shape[0]
    width = depth_k // nz
    f32, bf16 = jnp.float32, jnp.bfloat16
    dma = pltpu.SemaphoreType.DMA
    n = len(PIECES)
    return copy_out(pl.pallas_call(
        functools.partial(kernel, nz, ny),
        name="stationary_a",
        out_shape=jax.ShapeDtypeStruct((rows // nz, depth_k), bf16),
        in_specs=[pl.BlockSpec(memory_space=pl.ANY)] * 2,
        out_specs=pl.BlockSpec(memory_space=pl.ANY),
        scratch_shapes=[
            pltpu.VMEM((rows, depth_k), bf16),
            pltpu.VMEM((NX, 2 * half_k, width), bf16),
            pltpu.VMEM((2, rows // 2, width), f32),
            pltpu.VMEM((2, rows, width), f32),
            pltpu.VMEM((3, rows, width), f32),
            pltpu.VMEM((rows, width), bf16),
            dma,
            dma,
            dma((n, 4)),
            dma((n,)),
            dma((NG,)),
            dma((NG, 2)),
            dma,
            dma((2, NG, nz)),
            dma,
            dma,
            dma((NG,)),
        ],
        compiler_params=pltpu.CompilerParams(collective_id=0, has_side_effects=True, vmem_limit_bytes=67043328),
    )(a_blk, b_blk))


def solution(mesh):
    nz, ny = mesh.shape["depth"], mesh.shape["col"]
    return jax.shard_map(
        functools.partial(local_product, nz, ny),
        mesh=mesh,
        in_specs=(P("row", "col"), P("row", "col")),
        out_specs=P(("row", "depth"), "col"),
        check_vma=False,
    )
```

```python
import functools

import jax
import jax.numpy as jnp
from jax import lax
from jax.experimental import pallas as pl
from jax.experimental.pallas import tpu as pltpu
from jax.sharding import PartitionSpec as P

MESH = pl.DeviceIdType.MESH
NX = 4
PIECES = [(2, 0), (2, 1), (2, 2), (1, 0), (3, 0), (1, 1), (3, 1), (1, 2), (3, 2), (0, 3), (0, 2)]
GROUPS = [(0, 4), (4, 4), (8, 8), (0, 8)]
NG = 3
SLOT = {2: 0, 1: 1, 3: 2, 0: 0}
SCRIPT = """P0 P3 P4 P1 G0 P2 G1 P5 P6 L0 R0 O0 C0a G2 C0b P7 P8 G3 G4 L1 R1 O1 C1a C1b G5 G6 P9 P10 L2 R2 O2 C2a C2b
L3 R3 O3 C3a L4 R4 O4 C3b C4a C4b A0 G9 G7 G8 L5 R5 O5 C5a L6 R6 O6 C5b C6a C6b A1 G10 L9 R9 O9 C9a C9b F0
L7 R7 O7 C7a L8 R8 O8 C7b C8a C8b A2 F1 L10 R10 O10 C10a C10b W F2"""


def chunk_order(nz):
    return sorted(range(nz), key=lambda r: -min(r, nz - r))


def kernel(nz, ny, a_ref, b_ref, o_ref, abuf, bbuf, ro, rn, pbuf, obuf,
           a_sem, b_send, b_recv, s_recv, op_send, op_recv, nb_send, nb_recv, out_send, out_recv, own_sem):
    z = lax.axis_index("depth")
    y = lax.axis_index("col")
    i = lax.axis_index("row")
    x, c = i // 2, i % 2
    rows, depth_k = abuf.shape
    half_k = depth_k // 2
    quarter = half_k // NX
    width = depth_k // nz
    unit = width // 16
    chunk = rows // nz
    mblk = rows // 4
    half = rows // 2
    order_z = chunk_order(nz)

    def dev(zz, yy, xx, cc):
        return ((zz + nz) % nz, (yy + ny) % ny, 2 * ((xx + NX) % NX) + cc)

    def remote(src, dst, send_sem, recv_sem, device):
        return pltpu.make_async_remote_copy(src_ref=src, dst_ref=dst, send_sem=send_sem, recv_sem=recv_sem,
                                            device_id=device, device_id_type=MESH)

    sibling = dev(z, y, x, 1 - c)
    left, right, far = dev(z, y, x - 1, c), dev(z, y, x + 1, c), dev(z, y, x + 2, c)

    a_copies = [pltpu.make_async_copy(a_ref.at[pl.ds(m * mblk, mblk)], abuf.at[pl.ds(m * mblk, mblk)], a_sem)
                for m in range(4)]
    for cp in a_copies:
        cp.start()

    barrier = pltpu.get_barrier_semaphore()
    partners = [sibling]
    partners += [dev(z, y + dy, x + dx, c) for dy in range(ny) for dx in range(NX) if dx or dy]
    partners += [dev(z + r, y, x, c) for r in range(1, nz)]
    for p in partners:
        pl.semaphore_signal(barrier, inc=1, device_id=p, device_id_type=MESH)
    pl.semaphore_wait(barrier, len(partners))

    t_me = (y - x + NX) % NX

    def group_columns(s):
        return pl.ds(GROUPS[s][0] * unit, GROUPS[s][1] * unit)

    def columns(n):
        return group_columns(PIECES[n][1])

    def stage1(n, d):
        t, group = PIECES[n]
        first, wide = GROUPS[group]
        q = (x + d) % NX
        cols = pl.ds(pl.multiple_of(z * width + first * unit, 4 * unit), wide * unit)
        src = b_ref.at[pl.ds(pl.multiple_of(q * quarter, quarter), quarter), cols]
        dst = bbuf.at[t, pl.ds(pl.multiple_of(c * half_k + q * quarter, quarter), quarter), columns(n)]
        if t == 0 and d == 0:
            return pltpu.make_async_copy(src, dst, b_recv.at[n, 0])
        return remote(src, dst, b_send, b_recv.at[n, 0], dev(z, x, q, c))

    def stage1_start(n, ds):
        @pl.when(t_me == PIECES[n][0])
        def _():
            for d in ds:
                stage1(n, d).start()

    def part(n, k):
        q = (x + (0, 3, 1, 2)[k]) % NX
        start = c * half_k + q * quarter
        return bbuf.at[PIECES[n][0], pl.ds(pl.multiple_of(start, quarter), quarter), columns(n)]

    def lane(n, cc):
        return bbuf.at[PIECES[n][0], pl.ds(pl.multiple_of(cc * half_k, half_k), half_k), columns(n)]

    def arrived(n, k):
        ref = part(n, k)
        remote(ref, ref, b_send, b_recv.at[n, k], sibling).wait_recv()

    def to_sibling(n, k):
        ref = part(n, k)
        remote(ref, ref, b_send, s_recv.at[n], sibling).start()

    def pass_own(n):
        arrived(n, 0)
        ref = part(n, 0)
        for k, target in ((3, far), (1, right), (2, left)):
            remote(ref, ref, b_send, b_recv.at[n, k], target).start()
        to_sibling(n, 0)

    def pass_on(n, k):
        arrived(n, k)
        to_sibling(n, k)

    def group_columns(s):
        return pl.ds(GROUPS[s][0] * unit, GROUPS[s][1] * unit)

    def opposite_copy(s, d, h):
        src = pbuf.at[0, pl.ds(pl.multiple_of(d * half + h * mblk, mblk), mblk), group_columns(s)]
        return remote(src, ro.at[d, pl.ds(h * mblk, mblk), group_columns(s)], op_send.at[s], op_recv.at[s, d],
                      dev(z, y + 1 - 2 * d, x, c))

    def half_matmul(n, h):
        t, group = PIECES[n]
        k_own = pl.ds(pl.multiple_of(c * half_k, half_k), half_k)
        k_other = pl.ds(pl.multiple_of((1 - c) * half_k, half_k), half_k)
        split = t == 2 and h == 0

        def block_rows(d):
            return pl.ds(pl.multiple_of(d * half + h * mblk, mblk), mblk)

        def product(r, ks):
            return jnp.dot(abuf[r, ks], bbuf[t, ks, columns(n)], preferred_element_type=jnp.float32)

        if n == 0 and h == 0:
            pltpu.make_async_copy(abuf, abuf, a_sem).wait()
        if split:
            def own_half(d, carry):
                pbuf[SLOT[t], block_rows(d), columns(n)] = product(block_rows(d), k_own)
                return carry

            lax.fori_loop(0, 2, own_half, 0)
        if h == 0:
            ref = lane(n, 1 - c)
            remote(ref, ref, b_send, s_recv.at[n], sibling).wait_recv()
            if t == 0:
                for m in (0, 1) if group == 3 else (2,):
                    ref = pbuf.at[0, :, group_columns(m)]
                    remote(ref, ref, op_send.at[m], op_recv.at[m, 0], sibling).wait_send()

        def body(d, carry):
            r = block_rows(d)
            if split:
                pbuf[SLOT[t], r, columns(n)] = pbuf[SLOT[t], r, columns(n)] + product(r, k_other)
            else:
                pbuf[SLOT[t], r, columns(n)] = product(r, pl.ds(0, 2 * half_k))
            if t == 2:
                opposite_copy(group, d, h).start()
            return carry

        lax.fori_loop(0, 2, body, 0)

    def chunk_rows(zz):
        return pl.ds(pl.multiple_of(zz * chunk, chunk), chunk)

    def neighbour_copy(d, s, zz):
        cr, cols = chunk_rows(zz), group_columns(s)
        return remote(pbuf.at[1 + d, cr, cols], rn.at[d, cr, cols], nb_send, nb_recv.at[d, s, zz],
                      dev(z, y + 1 - 2 * d, x, c))

    def send_half(s, merged):
        nh = max(nz // 2, 1)
        for j in range(nh):
            for d in (0, 1):
                neighbour_copy(d, s, ((d if merged else 1 - d) * nh + (z + j) % nh) % nz).start()

    def merge(s):
        cols = group_columns(s)
        for d in (0, 1):
            ref = ro.at[d, :, group_columns(s)]
            remote(ref, ref, op_send.at[s], op_recv.at[s, d], sibling).wait_recv()
        for d in (0, 1):
            def body(m, carry):
                r = pl.ds(pl.multiple_of(m * (half // 4), half // 4), half // 4)
                rp = pl.ds(pl.multiple_of(d * half + m * (half // 4), half // 4), half // 4)
                pbuf[1 + d, rp, cols] = pbuf[1 + d, rp, cols] + ro[d, r, cols]
                return carry

            lax.fori_loop(0, 4, body, 0)

    def send_all(s):
        for r in order_z:
            for d in (0, 1):
                neighbour_copy(d, s, (z + r) % nz).start()

    def out_columns(zz, s):
        return pl.ds(pl.multiple_of(zz * width + GROUPS[s][0] * unit, 4 * unit), GROUPS[s][1] * unit)

    def out_copy(s, r):
        src = obuf.at[chunk_rows((z + r) % nz), group_columns(s)]
        dst = o_ref.at[:, out_columns(z, s)]
        if r == 0:
            return pltpu.make_async_copy(src, dst, own_sem.at[s])
        return remote(src, dst, out_send, out_recv, dev(z + r, y, x, c))

    def finish(s):
        cols = group_columns(s)
        for r in order_z:
            for d in (0, 1):
                neighbour_copy(d, s, (z + r) % nz).wait_recv()
            cr = chunk_rows((z + r) % nz)
            total = pbuf[0, cr, cols] + rn[0, cr, cols] + rn[1, cr, cols]
            obuf[cr, cols] = total.astype(jnp.bfloat16)
            out_copy(s, r).start()

    for item in SCRIPT.split():
        op, rest = item[0], item[1:]
        if op == "P":
            stage1_start(int(rest), (0, 2, 1, 3))
        elif op == "G":
            pass_own(int(rest))
        elif op == "L":
            pass_on(int(rest), 1)
        elif op == "R":
            pass_on(int(rest), 2)
        elif op == "O":
            pass_on(int(rest), 3)
        elif op == "C":
            half_matmul(int(rest[:-1]), "ab".index(rest[-1]))
        elif op == "U":
            send_half(int(rest), False)
        elif op == "M":
            merge(int(rest))
            send_half(int(rest), True)
        elif op == "A":
            merge(int(rest))
            send_all(int(rest))
        elif op == "F":
            finish(int(rest))
        elif op == "W":
            @pl.when(t_me != 0)
            def _():
                remote(bbuf, bbuf, b_send, out_recv, sibling).wait_send()

            @pl.when(t_me == 0)
            def _():
                ref = bbuf.at[:, pl.ds(0, 2 * half_k - quarter // NX)]
                remote(ref, ref, b_send, out_recv, sibling).wait_send()

    remote(rn, rn, nb_send, out_recv, sibling).wait_send()
    for s in range(NG):
        out_copy(s, 0).wait()
    sent = obuf.at[pl.ds(0, rows - chunk)]
    remote(sent, sent, out_send, out_recv, sibling).wait_send()
    got = o_ref.at[pl.ds(0, chunk - chunk // nz)]
    remote(got, got, out_send, out_recv, sibling).wait_recv()


COPIES = 4


def copy_kernel(src_ref, dst_ref, buf, in_sem, out_sem):
    n = buf.shape[0] // COPIES
    blocks = [pl.ds(m * n, n) for m in range(COPIES)]
    ins = [pltpu.make_async_copy(src_ref.at[b], buf.at[b], in_sem.at[m]) for m, b in enumerate(blocks)]
    outs = [pltpu.make_async_copy(buf.at[b], dst_ref.at[b], out_sem.at[m]) for m, b in enumerate(blocks)]
    for cp in ins:
        cp.start()
    for cp_in, cp_out in zip(ins, outs):
        cp_in.wait()
        cp_out.start()
    for cp in outs:
        cp.wait()


def copy_out(c_rows):
    return pl.pallas_call(
        copy_kernel,
        name="copy_out",
        out_shape=jax.ShapeDtypeStruct(c_rows.shape, c_rows.dtype),
        in_specs=[pl.BlockSpec(memory_space=pl.ANY)],
        out_specs=pl.BlockSpec(memory_space=pl.ANY),
        scratch_shapes=[pltpu.VMEM(c_rows.shape, c_rows.dtype), pltpu.SemaphoreType.DMA((COPIES,)),
                        pltpu.SemaphoreType.DMA((COPIES,))],
    )(c_rows)


def local_product(nz, ny, a_blk, b_blk):
    rows, depth_k = a_blk.shape
    half_k = b_blk.shape[0]
    width = depth_k // nz
    f32, bf16 = jnp.float32, jnp.bfloat16
    dma = pltpu.SemaphoreType.DMA
    n = len(PIECES)
    return copy_out(pl.pallas_call(
        functools.partial(kernel, nz, ny),
        name="stationary_a",
        out_shape=jax.ShapeDtypeStruct((rows // nz, depth_k), bf16),
        in_specs=[pl.BlockSpec(memory_space=pl.ANY)] * 2,
        out_specs=pl.BlockSpec(memory_space=pl.ANY),
        scratch_shapes=[
            pltpu.VMEM((rows, depth_k), bf16),
            pltpu.VMEM((NX, 2 * half_k, width), bf16),
            pltpu.VMEM((2, rows // 2, width), f32),
            pltpu.VMEM((2, rows, width), f32),
            pltpu.VMEM((3, rows, width), f32),
            pltpu.VMEM((rows, width), bf16),
            dma,
            dma,
            dma((n, 4)),
            dma((n,)),
            dma((NG,)),
            dma((NG, 2)),
            dma,
            dma((2, NG, nz)),
            dma,
            dma,
            dma((NG,)),
        ],
        compiler_params=pltpu.CompilerParams(collective_id=0, has_side_effects=True, vmem_limit_bytes=67043328),
    )(a_blk, b_blk))


def solution(mesh):
    nz, ny = mesh.shape["depth"], mesh.shape["col"]
    return jax.shard_map(
        functools.partial(local_product, nz, ny),
        mesh=mesh,
        in_specs=(P("row", "col"), P("row", "col")),
        out_specs=P(("row", "depth"), "col"),
        check_vma=False,
    )
```

```python
import functools

import jax
import jax.numpy as jnp
from jax import lax
from jax.experimental import pallas as pl
from jax.experimental.pallas import tpu as pltpu
from jax.sharding import PartitionSpec as P

MESH = pl.DeviceIdType.MESH
NX = 4
PIECES = [(2, 0), (2, 1), (2, 2), (1, 0), (3, 0), (1, 1), (3, 1), (1, 2), (3, 2), (0, 3), (0, 2)]
GROUPS = [(0, 4), (4, 4), (8, 8), (0, 8)]
NG = 3
SLOT = {2: 0, 1: 1, 3: 2, 0: 0}
SCRIPT = """P0 P1 G0 P2 P3 P4 G1 P5 P6 L0 R0 O0 C0a G2 C0b P7 P8 G3 G4 L1 R1 O1 C1a C1b G5 G6 P9 P10 L2 R2 O2 C2a C2b
L3 R3 O3 C3a L4 R4 O4 C3b C4a C4b A0 G9 G7 G8 L5 R5 O5 C5a L6 R6 O6 C5b C6a C6b A1 G10 L9 R9 O9 C9a C9b F0
L7 R7 O7 C7a L8 R8 O8 C7b C8a C8b A2 F1 L10 R10 O10 C10a C10b W F2"""


def chunk_order(nz):
    return sorted(range(nz), key=lambda r: -min(r, nz - r))


def kernel(nz, ny, a_ref, b_ref, o_ref, abuf, bbuf, ro, rn, pbuf, obuf,
           a_sem, b_send, b_recv, s_recv, op_send, op_recv, nb_send, nb_recv, out_send, out_recv, own_sem):
    z = lax.axis_index("depth")
    y = lax.axis_index("col")
    i = lax.axis_index("row")
    x, c = i // 2, i % 2
    rows, depth_k = abuf.shape
    half_k = depth_k // 2
    quarter = half_k // NX
    width = depth_k // nz
    unit = width // 16
    chunk = rows // nz
    mblk = rows // 4
    half = rows // 2
    order_z = chunk_order(nz)

    def dev(zz, yy, xx, cc):
        return ((zz + nz) % nz, (yy + ny) % ny, 2 * ((xx + NX) % NX) + cc)

    def remote(src, dst, send_sem, recv_sem, device):
        return pltpu.make_async_remote_copy(src_ref=src, dst_ref=dst, send_sem=send_sem, recv_sem=recv_sem,
                                            device_id=device, device_id_type=MESH)

    sibling = dev(z, y, x, 1 - c)
    left, right, far = dev(z, y, x - 1, c), dev(z, y, x + 1, c), dev(z, y, x + 2, c)

    a_copies = [pltpu.make_async_copy(a_ref.at[pl.ds(m * mblk, mblk)], abuf.at[pl.ds(m * mblk, mblk)], a_sem)
                for m in range(4)]
    for cp in a_copies:
        cp.start()

    barrier = pltpu.get_barrier_semaphore()
    partners = [sibling]
    partners += [dev(z, y + dy, x + dx, c) for dy in range(ny) for dx in range(NX) if dx or dy]
    partners += [dev(z + r, y, x, c) for r in range(1, nz)]
    for p in partners:
        pl.semaphore_signal(barrier, inc=1, device_id=p, device_id_type=MESH)
    pl.semaphore_wait(barrier, len(partners))

    t_me = (y - x + NX) % NX

    def group_columns(s):
        return pl.ds(GROUPS[s][0] * unit, GROUPS[s][1] * unit)

    def columns(n):
        return group_columns(PIECES[n][1])

    def stage1(n, d):
        t, group = PIECES[n]
        first, wide = GROUPS[group]
        q = (x + d) % NX
        cols = pl.ds(pl.multiple_of(z * width + first * unit, 4 * unit), wide * unit)
        src = b_ref.at[pl.ds(pl.multiple_of(q * quarter, quarter), quarter), cols]
        dst = bbuf.at[t, pl.ds(pl.multiple_of(c * half_k + q * quarter, quarter), quarter), columns(n)]
        if t == 0 and d == 0:
            return pltpu.make_async_copy(src, dst, b_recv.at[n, 0])
        return remote(src, dst, b_send, b_recv.at[n, 0], dev(z, x, q, c))

    def stage1_start(n, ds):
        @pl.when(t_me == PIECES[n][0])
        def _():
            for d in ds:
                stage1(n, d).start()

    def part(n, k):
        q = (x + (0, 3, 1, 2)[k]) % NX
        start = c * half_k + q * quarter
        return bbuf.at[PIECES[n][0], pl.ds(pl.multiple_of(start, quarter), quarter), columns(n)]

    def lane(n, cc):
        return bbuf.at[PIECES[n][0], pl.ds(pl.multiple_of(cc * half_k, half_k), half_k), columns(n)]

    def arrived(n, k):
        ref = part(n, k)
        remote(ref, ref, b_send, b_recv.at[n, k], sibling).wait_recv()

    def to_sibling(n, k):
        ref = part(n, k)
        remote(ref, ref, b_send, s_recv.at[n], sibling).start()

    def pass_own(n):
        arrived(n, 0)
        ref = part(n, 0)
        for k, target in ((3, far), (1, right), (2, left)):
            remote(ref, ref, b_send, b_recv.at[n, k], target).start()
        to_sibling(n, 0)

    def pass_on(n, k):
        arrived(n, k)
        to_sibling(n, k)

    def group_columns(s):
        return pl.ds(GROUPS[s][0] * unit, GROUPS[s][1] * unit)

    def opposite_copy(s, d, h):
        src = pbuf.at[0, pl.ds(pl.multiple_of(d * half + h * mblk, mblk), mblk), group_columns(s)]
        return remote(src, ro.at[d, pl.ds(h * mblk, mblk), group_columns(s)], op_send.at[s], op_recv.at[s, d],
                      dev(z, y + 1 - 2 * d, x, c))

    def half_matmul(n, h):
        t, group = PIECES[n]
        if h == 0:
            ref = lane(n, 1 - c)
            remote(ref, ref, b_send, s_recv.at[n], sibling).wait_recv()
            if n == 0:
                pltpu.make_async_copy(abuf, abuf, a_sem).wait()
            if t == 0:
                for m in (0, 1) if group == 3 else (2,):
                    ref = pbuf.at[0, :, group_columns(m)]
                    remote(ref, ref, op_send.at[m], op_recv.at[m, 0], sibling).wait_send()

        def body(d, carry):
            r = pl.ds(pl.multiple_of(d * half + h * mblk, mblk), mblk)
            pbuf[SLOT[t], r, columns(n)] = jnp.dot(abuf[r, :], bbuf[t, :, columns(n)],
                                                   preferred_element_type=jnp.float32)
            if t == 2:
                opposite_copy(group, d, h).start()
            return carry

        lax.fori_loop(0, 2, body, 0)

    def chunk_rows(zz):
        return pl.ds(pl.multiple_of(zz * chunk, chunk), chunk)

    def neighbour_copy(d, s, zz):
        cr, cols = chunk_rows(zz), group_columns(s)
        return remote(pbuf.at[1 + d, cr, cols], rn.at[d, cr, cols], nb_send, nb_recv.at[d, s, zz],
                      dev(z, y + 1 - 2 * d, x, c))

    def send_half(s, merged):
        nh = max(nz // 2, 1)
        for j in range(nh):
            for d in (0, 1):
                neighbour_copy(d, s, ((d if merged else 1 - d) * nh + (z + j) % nh) % nz).start()

    def merge(s):
        cols = group_columns(s)
        for d in (0, 1):
            ref = ro.at[d, :, group_columns(s)]
            remote(ref, ref, op_send.at[s], op_recv.at[s, d], sibling).wait_recv()
        for d in (0, 1):
            def body(m, carry):
                r = pl.ds(pl.multiple_of(m * (half // 4), half // 4), half // 4)
                rp = pl.ds(pl.multiple_of(d * half + m * (half // 4), half // 4), half // 4)
                pbuf[1 + d, rp, cols] = pbuf[1 + d, rp, cols] + ro[d, r, cols]
                return carry

            lax.fori_loop(0, 4, body, 0)

    def send_all(s):
        for r in order_z:
            for d in (0, 1):
                neighbour_copy(d, s, (z + r) % nz).start()

    def out_columns(zz, s):
        return pl.ds(pl.multiple_of(zz * width + GROUPS[s][0] * unit, 4 * unit), GROUPS[s][1] * unit)

    def out_copy(s, r):
        src = obuf.at[chunk_rows((z + r) % nz), group_columns(s)]
        dst = o_ref.at[:, out_columns(z, s)]
        if r == 0:
            return pltpu.make_async_copy(src, dst, own_sem.at[s])
        return remote(src, dst, out_send, out_recv, dev(z + r, y, x, c))

    def finish(s):
        cols = group_columns(s)
        for r in order_z:
            for d in (0, 1):
                neighbour_copy(d, s, (z + r) % nz).wait_recv()
            cr = chunk_rows((z + r) % nz)
            total = pbuf[0, cr, cols] + rn[0, cr, cols] + rn[1, cr, cols]
            obuf[cr, cols] = total.astype(jnp.bfloat16)
            out_copy(s, r).start()

    for item in SCRIPT.split():
        op, rest = item[0], item[1:]
        if op == "P":
            stage1_start(int(rest), (0, 2, 1, 3))
        elif op == "G":
            pass_own(int(rest))
        elif op == "L":
            pass_on(int(rest), 1)
        elif op == "R":
            pass_on(int(rest), 2)
        elif op == "O":
            pass_on(int(rest), 3)
        elif op == "C":
            half_matmul(int(rest[:-1]), "ab".index(rest[-1]))
        elif op == "U":
            send_half(int(rest), False)
        elif op == "M":
            merge(int(rest))
            send_half(int(rest), True)
        elif op == "A":
            merge(int(rest))
            send_all(int(rest))
        elif op == "F":
            finish(int(rest))
        elif op == "W":
            @pl.when(t_me != 0)
            def _():
                remote(bbuf, bbuf, b_send, out_recv, sibling).wait_send()

            @pl.when(t_me == 0)
            def _():
                ref = bbuf.at[:, pl.ds(0, 2 * half_k - quarter // NX)]
                remote(ref, ref, b_send, out_recv, sibling).wait_send()

    remote(rn, rn, nb_send, out_recv, sibling).wait_send()
    for s in range(NG):
        out_copy(s, 0).wait()
    sent = obuf.at[pl.ds(0, rows - chunk)]
    remote(sent, sent, out_send, out_recv, sibling).wait_send()
    got = o_ref.at[pl.ds(0, chunk - chunk // nz)]
    remote(got, got, out_send, out_recv, sibling).wait_recv()


COPIES = 4


def copy_kernel(src_ref, dst_ref, buf, in_sem, out_sem):
    n = buf.shape[0] // COPIES
    blocks = [pl.ds(m * n, n) for m in range(COPIES)]
    ins = [pltpu.make_async_copy(src_ref.at[b], buf.at[b], in_sem.at[m]) for m, b in enumerate(blocks)]
    outs = [pltpu.make_async_copy(buf.at[b], dst_ref.at[b], out_sem.at[m]) for m, b in enumerate(blocks)]
    for cp in ins:
        cp.start()
    for cp_in, cp_out in zip(ins, outs):
        cp_in.wait()
        cp_out.start()
    for cp in outs:
        cp.wait()


def copy_out(c_rows):
    return pl.pallas_call(
        copy_kernel,
        name="copy_out",
        out_shape=jax.ShapeDtypeStruct(c_rows.shape, c_rows.dtype),
        in_specs=[pl.BlockSpec(memory_space=pl.ANY)],
        out_specs=pl.BlockSpec(memory_space=pl.ANY),
        scratch_shapes=[pltpu.VMEM(c_rows.shape, c_rows.dtype), pltpu.SemaphoreType.DMA((COPIES,)),
                        pltpu.SemaphoreType.DMA((COPIES,))],
    )(c_rows)


def local_product(nz, ny, a_blk, b_blk):
    rows, depth_k = a_blk.shape
    half_k = b_blk.shape[0]
    width = depth_k // nz
    f32, bf16 = jnp.float32, jnp.bfloat16
    dma = pltpu.SemaphoreType.DMA
    n = len(PIECES)
    return copy_out(pl.pallas_call(
        functools.partial(kernel, nz, ny),
        name="stationary_a",
        out_shape=jax.ShapeDtypeStruct((rows // nz, depth_k), bf16),
        in_specs=[pl.BlockSpec(memory_space=pl.ANY)] * 2,
        out_specs=pl.BlockSpec(memory_space=pl.ANY),
        scratch_shapes=[
            pltpu.VMEM((rows, depth_k), bf16),
            pltpu.VMEM((NX, 2 * half_k, width), bf16),
            pltpu.VMEM((2, rows // 2, width), f32),
            pltpu.VMEM((2, rows, width), f32),
            pltpu.VMEM((3, rows, width), f32),
            pltpu.VMEM((rows, width), bf16),
            dma,
            dma,
            dma((n, 4)),
            dma((n,)),
            dma((NG,)),
            dma((NG, 2)),
            dma,
            dma((2, NG, nz)),
            dma,
            dma,
            dma((NG,)),
        ],
        compiler_params=pltpu.CompilerParams(collective_id=0, has_side_effects=True, vmem_limit_bytes=67043328),
    )(a_blk, b_blk))


def solution(mesh):
    nz, ny = mesh.shape["depth"], mesh.shape["col"]
    return jax.shard_map(
        functools.partial(local_product, nz, ny),
        mesh=mesh,
        in_specs=(P("row", "col"), P("row", "col")),
        out_specs=P(("row", "depth"), "col"),
        check_vma=False,
    )
```

```python
import functools

import jax
import jax.numpy as jnp
from jax import lax
from jax.experimental import pallas as pl
from jax.experimental.pallas import tpu as pltpu
from jax.sharding import PartitionSpec as P

MESH = pl.DeviceIdType.MESH
NX = 4
PIECES = [(2, 0), (2, 1), (2, 2), (1, 0), (3, 0), (1, 1), (3, 1), (1, 2), (3, 2), (0, 3), (0, 2)]
GROUPS = [(0, 4), (4, 4), (8, 8), (0, 8)]
NG = 3
SLOT = {2: 0, 1: 1, 3: 2, 0: 0}
SCRIPT = """P0 P1 G0 P2 P3 P4 G1 P5 P6 L0 R0 O0 C0a C0b G2 P7 P8 G3 G4 L1 R1 O1 C1a C1b G5 G6 P9 P10 L2 R2 O2 C2a C2b
L3 R3 O3 C3a L4 R4 O4 C3b C4a C4b A0 G9 G7 G8 L5 R5 O5 C5a L6 R6 O6 C5b C6a C6b A1 G10 L9 R9 O9 C9a C9b F0
L7 R7 O7 C7a L8 R8 O8 C7b C8a C8b A2 F1 L10 R10 O10 C10a C10b W F2"""


def chunk_order(nz):
    return sorted(range(nz), key=lambda r: -min(r, nz - r))


def kernel(nz, ny, a_ref, b_ref, o_ref, abuf, bbuf, ro, rn, pbuf, obuf,
           a_sem, b_send, b_recv, s_recv, op_send, op_recv, nb_send, nb_recv, out_send, out_recv, own_sem):
    z = lax.axis_index("depth")
    y = lax.axis_index("col")
    i = lax.axis_index("row")
    x, c = i // 2, i % 2
    rows, depth_k = abuf.shape
    half_k = depth_k // 2
    quarter = half_k // NX
    width = depth_k // nz
    unit = width // 16
    chunk = rows // nz
    mblk = rows // 4
    half = rows // 2
    order_z = chunk_order(nz)

    def dev(zz, yy, xx, cc):
        return ((zz + nz) % nz, (yy + ny) % ny, 2 * ((xx + NX) % NX) + cc)

    def remote(src, dst, send_sem, recv_sem, device):
        return pltpu.make_async_remote_copy(src_ref=src, dst_ref=dst, send_sem=send_sem, recv_sem=recv_sem,
                                            device_id=device, device_id_type=MESH)

    sibling = dev(z, y, x, 1 - c)
    left, right, far = dev(z, y, x - 1, c), dev(z, y, x + 1, c), dev(z, y, x + 2, c)

    a_copies = [pltpu.make_async_copy(a_ref.at[pl.ds(m * mblk, mblk)], abuf.at[pl.ds(m * mblk, mblk)], a_sem)
                for m in range(4)]
    for cp in a_copies:
        cp.start()

    barrier = pltpu.get_barrier_semaphore()
    partners = [sibling]
    partners += [dev(z, y + dy, x + dx, c) for dy in range(ny) for dx in range(NX) if dx or dy]
    partners += [dev(z + r, y, x, c) for r in range(1, nz)]
    for p in partners:
        pl.semaphore_signal(barrier, inc=1, device_id=p, device_id_type=MESH)
    pl.semaphore_wait(barrier, len(partners))

    t_me = (y - x + NX) % NX

    def group_columns(s):
        return pl.ds(GROUPS[s][0] * unit, GROUPS[s][1] * unit)

    def columns(n):
        return group_columns(PIECES[n][1])

    def stage1(n, d):
        t, group = PIECES[n]
        first, wide = GROUPS[group]
        q = (x + d) % NX
        cols = pl.ds(pl.multiple_of(z * width + first * unit, 4 * unit), wide * unit)
        src = b_ref.at[pl.ds(pl.multiple_of(q * quarter, quarter), quarter), cols]
        dst = bbuf.at[t, pl.ds(pl.multiple_of(c * half_k + q * quarter, quarter), quarter), columns(n)]
        if t == 0 and d == 0:
            return pltpu.make_async_copy(src, dst, b_recv.at[n, 0])
        return remote(src, dst, b_send, b_recv.at[n, 0], dev(z, x, q, c))

    def stage1_start(n, ds):
        @pl.when(t_me == PIECES[n][0])
        def _():
            for d in ds:
                stage1(n, d).start()

    def part(n, k):
        q = (x + (0, 3, 1, 2)[k]) % NX
        start = c * half_k + q * quarter
        return bbuf.at[PIECES[n][0], pl.ds(pl.multiple_of(start, quarter), quarter), columns(n)]

    def lane(n, cc):
        return bbuf.at[PIECES[n][0], pl.ds(pl.multiple_of(cc * half_k, half_k), half_k), columns(n)]

    def arrived(n, k):
        ref = part(n, k)
        remote(ref, ref, b_send, b_recv.at[n, k], sibling).wait_recv()

    def to_sibling(n, k):
        ref = part(n, k)
        remote(ref, ref, b_send, s_recv.at[n], sibling).start()

    def pass_own(n):
        arrived(n, 0)
        ref = part(n, 0)
        for k, target in ((3, far), (1, right), (2, left)):
            remote(ref, ref, b_send, b_recv.at[n, k], target).start()
        to_sibling(n, 0)

    def pass_on(n, k):
        arrived(n, k)
        to_sibling(n, k)

    def group_columns(s):
        return pl.ds(GROUPS[s][0] * unit, GROUPS[s][1] * unit)

    def opposite_copy(s, d, h):
        src = pbuf.at[0, pl.ds(pl.multiple_of(d * half + h * mblk, mblk), mblk), group_columns(s)]
        return remote(src, ro.at[d, pl.ds(h * mblk, mblk), group_columns(s)], op_send.at[s], op_recv.at[s, d],
                      dev(z, y + 1 - 2 * d, x, c))

    def half_matmul(n, h):
        t, group = PIECES[n]
        if h == 0:
            ref = lane(n, 1 - c)
            remote(ref, ref, b_send, s_recv.at[n], sibling).wait_recv()
            if n == 0:
                pltpu.make_async_copy(abuf, abuf, a_sem).wait()
            if t == 0:
                for m in (0, 1) if group == 3 else (2,):
                    ref = pbuf.at[0, :, group_columns(m)]
                    remote(ref, ref, op_send.at[m], op_recv.at[m, 0], sibling).wait_send()

        def body(d, carry):
            r = pl.ds(pl.multiple_of(d * half + h * mblk, mblk), mblk)
            pbuf[SLOT[t], r, columns(n)] = jnp.dot(abuf[r, :], bbuf[t, :, columns(n)],
                                                   preferred_element_type=jnp.float32)
            if t == 2:
                opposite_copy(group, d, h).start()
            return carry

        lax.fori_loop(0, 2, body, 0)

    def chunk_rows(zz):
        return pl.ds(pl.multiple_of(zz * chunk, chunk), chunk)

    def neighbour_copy(d, s, zz):
        cr, cols = chunk_rows(zz), group_columns(s)
        return remote(pbuf.at[1 + d, cr, cols], rn.at[d, cr, cols], nb_send, nb_recv.at[d, s, zz],
                      dev(z, y + 1 - 2 * d, x, c))

    def send_half(s, merged):
        nh = max(nz // 2, 1)
        for j in range(nh):
            for d in (0, 1):
                neighbour_copy(d, s, ((d if merged else 1 - d) * nh + (z + j) % nh) % nz).start()

    def merge(s):
        cols = group_columns(s)
        for d in (0, 1):
            ref = ro.at[d, :, group_columns(s)]
            remote(ref, ref, op_send.at[s], op_recv.at[s, d], sibling).wait_recv()
        for d in (0, 1):
            def body(m, carry):
                r = pl.ds(pl.multiple_of(m * (half // 4), half // 4), half // 4)
                rp = pl.ds(pl.multiple_of(d * half + m * (half // 4), half // 4), half // 4)
                pbuf[1 + d, rp, cols] = pbuf[1 + d, rp, cols] + ro[d, r, cols]
                return carry

            lax.fori_loop(0, 4, body, 0)

    def send_all(s):
        for r in order_z:
            for d in (0, 1):
                neighbour_copy(d, s, (z + r) % nz).start()

    def out_columns(zz, s):
        return pl.ds(pl.multiple_of(zz * width + GROUPS[s][0] * unit, 4 * unit), GROUPS[s][1] * unit)

    def out_copy(s, r):
        src = obuf.at[chunk_rows((z + r) % nz), group_columns(s)]
        dst = o_ref.at[:, out_columns(z, s)]
        if r == 0:
            return pltpu.make_async_copy(src, dst, own_sem.at[s])
        return remote(src, dst, out_send, out_recv, dev(z + r, y, x, c))

    def finish(s):
        cols = group_columns(s)
        for r in order_z:
            for d in (0, 1):
                neighbour_copy(d, s, (z + r) % nz).wait_recv()
            cr = chunk_rows((z + r) % nz)
            total = pbuf[0, cr, cols] + rn[0, cr, cols] + rn[1, cr, cols]
            obuf[cr, cols] = total.astype(jnp.bfloat16)
            out_copy(s, r).start()

    for item in SCRIPT.split():
        op, rest = item[0], item[1:]
        if op == "P":
            stage1_start(int(rest), (0, 2, 1, 3))
        elif op == "G":
            pass_own(int(rest))
        elif op == "L":
            pass_on(int(rest), 1)
        elif op == "R":
            pass_on(int(rest), 2)
        elif op == "O":
            pass_on(int(rest), 3)
        elif op == "C":
            half_matmul(int(rest[:-1]), "ab".index(rest[-1]))
        elif op == "U":
            send_half(int(rest), False)
        elif op == "M":
            merge(int(rest))
            send_half(int(rest), True)
        elif op == "A":
            merge(int(rest))
            send_all(int(rest))
        elif op == "F":
            finish(int(rest))
        elif op == "W":
            @pl.when(t_me != 0)
            def _():
                remote(bbuf, bbuf, b_send, out_recv, sibling).wait_send()

            @pl.when(t_me == 0)
            def _():
                ref = bbuf.at[:, pl.ds(0, 2 * half_k - quarter // NX)]
                remote(ref, ref, b_send, out_recv, sibling).wait_send()

    remote(rn, rn, nb_send, out_recv, sibling).wait_send()
    for s in range(NG):
        out_copy(s, 0).wait()
    sent = obuf.at[pl.ds(0, rows - chunk)]
    remote(sent, sent, out_send, out_recv, sibling).wait_send()
    got = o_ref.at[pl.ds(0, chunk - chunk // nz)]
    remote(got, got, out_send, out_recv, sibling).wait_recv()


COPIES = 4


def copy_kernel(src_ref, dst_ref, buf, in_sem, out_sem):
    n = buf.shape[0] // COPIES
    blocks = [pl.ds(m * n, n) for m in range(COPIES)]
    ins = [pltpu.make_async_copy(src_ref.at[b], buf.at[b], in_sem.at[m]) for m, b in enumerate(blocks)]
    outs = [pltpu.make_async_copy(buf.at[b], dst_ref.at[b], out_sem.at[m]) for m, b in enumerate(blocks)]
    for cp in ins:
        cp.start()
    for cp_in, cp_out in zip(ins, outs):
        cp_in.wait()
        cp_out.start()
    for cp in outs:
        cp.wait()


def copy_out(c_rows):
    return pl.pallas_call(
        copy_kernel,
        name="copy_out",
        out_shape=jax.ShapeDtypeStruct(c_rows.shape, c_rows.dtype),
        in_specs=[pl.BlockSpec(memory_space=pl.ANY)],
        out_specs=pl.BlockSpec(memory_space=pl.ANY),
        scratch_shapes=[pltpu.VMEM(c_rows.shape, c_rows.dtype), pltpu.SemaphoreType.DMA((COPIES,)),
                        pltpu.SemaphoreType.DMA((COPIES,))],
    )(c_rows)


def local_product(nz, ny, a_blk, b_blk):
    rows, depth_k = a_blk.shape
    half_k = b_blk.shape[0]
    width = depth_k // nz
    f32, bf16 = jnp.float32, jnp.bfloat16
    dma = pltpu.SemaphoreType.DMA
    n = len(PIECES)
    return copy_out(pl.pallas_call(
        functools.partial(kernel, nz, ny),
        name="stationary_a",
        out_shape=jax.ShapeDtypeStruct((rows // nz, depth_k), bf16),
        in_specs=[pl.BlockSpec(memory_space=pl.ANY)] * 2,
        out_specs=pl.BlockSpec(memory_space=pl.ANY),
        scratch_shapes=[
            pltpu.VMEM((rows, depth_k), bf16),
            pltpu.VMEM((NX, 2 * half_k, width), bf16),
            pltpu.VMEM((2, rows // 2, width), f32),
            pltpu.VMEM((2, rows, width), f32),
            pltpu.VMEM((3, rows, width), f32),
            pltpu.VMEM((rows, width), bf16),
            dma,
            dma,
            dma((n, 4)),
            dma((n,)),
            dma((NG,)),
            dma((NG, 2)),
            dma,
            dma((2, NG, nz)),
            dma,
            dma,
            dma((NG,)),
        ],
        compiler_params=pltpu.CompilerParams(collective_id=0, has_side_effects=True, vmem_limit_bytes=67043328),
    )(a_blk, b_blk))


def solution(mesh):
    nz, ny = mesh.shape["depth"], mesh.shape["col"]
    return jax.shard_map(
        functools.partial(local_product, nz, ny),
        mesh=mesh,
        in_specs=(P("row", "col"), P("row", "col")),
        out_specs=P(("row", "depth"), "col"),
        check_vma=False,
    )
```

```python
import functools

import jax
import jax.numpy as jnp
from jax import lax
from jax.experimental import pallas as pl
from jax.experimental.pallas import tpu as pltpu
from jax.sharding import PartitionSpec as P

MESH = pl.DeviceIdType.MESH
NX = 4
PIECES = [(2, 0), (2, 1), (2, 2), (1, 0), (3, 0), (1, 1), (3, 1), (1, 2), (3, 2), (0, 3), (0, 2)]
GROUPS = [(0, 4), (4, 4), (8, 8), (0, 8)]
NG = 3
SLOT = {2: 0, 1: 1, 3: 2, 0: 0}
SCRIPT = """P0 P1 G0 P2 P3 P4 G1 P5 P6 L0 R0 O0 C0a G2 C0b L1 R1 O1 P7 P8 G3 G4 C1a C1b G5 G6 P9 P10 L2 R2 O2 C2a C2b
L3 R3 O3 C3a L4 R4 O4 C3b C4a C4b A0 G9 G7 G8 L5 R5 O5 C5a L6 R6 O6 C5b C6a C6b A1 G10 L9 R9 O9 C9a C9b F0
L7 R7 O7 C7a L8 R8 O8 C7b C8a C8b A2 F1 L10 R10 O10 C10a C10b W F2"""


def chunk_order(nz):
    return sorted(range(nz), key=lambda r: -min(r, nz - r))


def kernel(nz, ny, a_ref, b_ref, o_ref, abuf, bbuf, ro, rn, pbuf, obuf,
           a_sem, b_send, b_recv, s_recv, op_send, op_recv, nb_send, nb_recv, out_send, out_recv, own_sem):
    z = lax.axis_index("depth")
    y = lax.axis_index("col")
    i = lax.axis_index("row")
    x, c = i // 2, i % 2
    rows, depth_k = abuf.shape
    half_k = depth_k // 2
    quarter = half_k // NX
    width = depth_k // nz
    unit = width // 16
    chunk = rows // nz
    mblk = rows // 4
    half = rows // 2
    order_z = chunk_order(nz)

    def dev(zz, yy, xx, cc):
        return ((zz + nz) % nz, (yy + ny) % ny, 2 * ((xx + NX) % NX) + cc)

    def remote(src, dst, send_sem, recv_sem, device):
        return pltpu.make_async_remote_copy(src_ref=src, dst_ref=dst, send_sem=send_sem, recv_sem=recv_sem,
                                            device_id=device, device_id_type=MESH)

    sibling = dev(z, y, x, 1 - c)
    left, right, far = dev(z, y, x - 1, c), dev(z, y, x + 1, c), dev(z, y, x + 2, c)

    a_copies = [pltpu.make_async_copy(a_ref.at[pl.ds(m * mblk, mblk)], abuf.at[pl.ds(m * mblk, mblk)], a_sem)
                for m in range(4)]
    for cp in a_copies:
        cp.start()

    barrier = pltpu.get_barrier_semaphore()
    partners = [sibling]
    partners += [dev(z, y + dy, x + dx, c) for dy in range(ny) for dx in range(NX) if dx or dy]
    partners += [dev(z + r, y, x, c) for r in range(1, nz)]
    for p in partners:
        pl.semaphore_signal(barrier, inc=1, device_id=p, device_id_type=MESH)
    pl.semaphore_wait(barrier, len(partners))

    t_me = (y - x + NX) % NX

    def group_columns(s):
        return pl.ds(GROUPS[s][0] * unit, GROUPS[s][1] * unit)

    def columns(n):
        return group_columns(PIECES[n][1])

    def stage1(n, d):
        t, group = PIECES[n]
        first, wide = GROUPS[group]
        q = (x + d) % NX
        cols = pl.ds(pl.multiple_of(z * width + first * unit, 4 * unit), wide * unit)
        src = b_ref.at[pl.ds(pl.multiple_of(q * quarter, quarter), quarter), cols]
        dst = bbuf.at[t, pl.ds(pl.multiple_of(c * half_k + q * quarter, quarter), quarter), columns(n)]
        if t == 0 and d == 0:
            return pltpu.make_async_copy(src, dst, b_recv.at[n, 0])
        return remote(src, dst, b_send, b_recv.at[n, 0], dev(z, x, q, c))

    def stage1_start(n, ds):
        @pl.when(t_me == PIECES[n][0])
        def _():
            for d in ds:
                stage1(n, d).start()

    def part(n, k):
        q = (x + (0, 3, 1, 2)[k]) % NX
        start = c * half_k + q * quarter
        return bbuf.at[PIECES[n][0], pl.ds(pl.multiple_of(start, quarter), quarter), columns(n)]

    def lane(n, cc):
        return bbuf.at[PIECES[n][0], pl.ds(pl.multiple_of(cc * half_k, half_k), half_k), columns(n)]

    def arrived(n, k):
        ref = part(n, k)
        remote(ref, ref, b_send, b_recv.at[n, k], sibling).wait_recv()

    def to_sibling(n, k):
        ref = part(n, k)
        remote(ref, ref, b_send, s_recv.at[n], sibling).start()

    def pass_own(n):
        arrived(n, 0)
        ref = part(n, 0)
        for k, target in ((3, far), (1, right), (2, left)):
            remote(ref, ref, b_send, b_recv.at[n, k], target).start()
        to_sibling(n, 0)

    def pass_on(n, k):
        arrived(n, k)
        to_sibling(n, k)

    def group_columns(s):
        return pl.ds(GROUPS[s][0] * unit, GROUPS[s][1] * unit)

    def opposite_copy(s, d, h):
        src = pbuf.at[0, pl.ds(pl.multiple_of(d * half + h * mblk, mblk), mblk), group_columns(s)]
        return remote(src, ro.at[d, pl.ds(h * mblk, mblk), group_columns(s)], op_send.at[s], op_recv.at[s, d],
                      dev(z, y + 1 - 2 * d, x, c))

    def half_matmul(n, h):
        t, group = PIECES[n]
        if h == 0:
            ref = lane(n, 1 - c)
            remote(ref, ref, b_send, s_recv.at[n], sibling).wait_recv()
            if n == 0:
                pltpu.make_async_copy(abuf, abuf, a_sem).wait()
            if t == 0:
                for m in (0, 1) if group == 3 else (2,):
                    ref = pbuf.at[0, :, group_columns(m)]
                    remote(ref, ref, op_send.at[m], op_recv.at[m, 0], sibling).wait_send()

        def body(d, carry):
            r = pl.ds(pl.multiple_of(d * half + h * mblk, mblk), mblk)
            pbuf[SLOT[t], r, columns(n)] = jnp.dot(abuf[r, :], bbuf[t, :, columns(n)],
                                                   preferred_element_type=jnp.float32)
            if t == 2:
                opposite_copy(group, d, h).start()
            return carry

        lax.fori_loop(0, 2, body, 0)

    def chunk_rows(zz):
        return pl.ds(pl.multiple_of(zz * chunk, chunk), chunk)

    def neighbour_copy(d, s, zz):
        cr, cols = chunk_rows(zz), group_columns(s)
        return remote(pbuf.at[1 + d, cr, cols], rn.at[d, cr, cols], nb_send, nb_recv.at[d, s, zz],
                      dev(z, y + 1 - 2 * d, x, c))

    def send_half(s, merged):
        nh = max(nz // 2, 1)
        for j in range(nh):
            for d in (0, 1):
                neighbour_copy(d, s, ((d if merged else 1 - d) * nh + (z + j) % nh) % nz).start()

    def merge(s):
        cols = group_columns(s)
        for d in (0, 1):
            ref = ro.at[d, :, group_columns(s)]
            remote(ref, ref, op_send.at[s], op_recv.at[s, d], sibling).wait_recv()
        for d in (0, 1):
            def body(m, carry):
                r = pl.ds(pl.multiple_of(m * (half // 4), half // 4), half // 4)
                rp = pl.ds(pl.multiple_of(d * half + m * (half // 4), half // 4), half // 4)
                pbuf[1 + d, rp, cols] = pbuf[1 + d, rp, cols] + ro[d, r, cols]
                return carry

            lax.fori_loop(0, 4, body, 0)

    def send_all(s):
        for r in order_z:
            for d in (0, 1):
                neighbour_copy(d, s, (z + r) % nz).start()

    def out_columns(zz, s):
        return pl.ds(pl.multiple_of(zz * width + GROUPS[s][0] * unit, 4 * unit), GROUPS[s][1] * unit)

    def out_copy(s, r):
        src = obuf.at[chunk_rows((z + r) % nz), group_columns(s)]
        dst = o_ref.at[:, out_columns(z, s)]
        if r == 0:
            return pltpu.make_async_copy(src, dst, own_sem.at[s])
        return remote(src, dst, out_send, out_recv, dev(z + r, y, x, c))

    def finish(s):
        cols = group_columns(s)
        for r in order_z:
            for d in (0, 1):
                neighbour_copy(d, s, (z + r) % nz).wait_recv()
            cr = chunk_rows((z + r) % nz)
            total = pbuf[0, cr, cols] + rn[0, cr, cols] + rn[1, cr, cols]
            obuf[cr, cols] = total.astype(jnp.bfloat16)
            out_copy(s, r).start()

    for item in SCRIPT.split():
        op, rest = item[0], item[1:]
        if op == "P":
            stage1_start(int(rest), (0, 2, 1, 3))
        elif op == "G":
            pass_own(int(rest))
        elif op == "L":
            pass_on(int(rest), 1)
        elif op == "R":
            pass_on(int(rest), 2)
        elif op == "O":
            pass_on(int(rest), 3)
        elif op == "C":
            half_matmul(int(rest[:-1]), "ab".index(rest[-1]))
        elif op == "U":
            send_half(int(rest), False)
        elif op == "M":
            merge(int(rest))
            send_half(int(rest), True)
        elif op == "A":
            merge(int(rest))
            send_all(int(rest))
        elif op == "F":
            finish(int(rest))
        elif op == "W":
            @pl.when(t_me != 0)
            def _():
                remote(bbuf, bbuf, b_send, out_recv, sibling).wait_send()

            @pl.when(t_me == 0)
            def _():
                ref = bbuf.at[:, pl.ds(0, 2 * half_k - quarter // NX)]
                remote(ref, ref, b_send, out_recv, sibling).wait_send()

    remote(rn, rn, nb_send, out_recv, sibling).wait_send()
    for s in range(NG):
        out_copy(s, 0).wait()
    sent = obuf.at[pl.ds(0, rows - chunk)]
    remote(sent, sent, out_send, out_recv, sibling).wait_send()
    got = o_ref.at[pl.ds(0, chunk - chunk // nz)]
    remote(got, got, out_send, out_recv, sibling).wait_recv()


COPIES = 4


def copy_kernel(src_ref, dst_ref, buf, in_sem, out_sem):
    n = buf.shape[0] // COPIES
    blocks = [pl.ds(m * n, n) for m in range(COPIES)]
    ins = [pltpu.make_async_copy(src_ref.at[b], buf.at[b], in_sem.at[m]) for m, b in enumerate(blocks)]
    outs = [pltpu.make_async_copy(buf.at[b], dst_ref.at[b], out_sem.at[m]) for m, b in enumerate(blocks)]
    for cp in ins:
        cp.start()
    for cp_in, cp_out in zip(ins, outs):
        cp_in.wait()
        cp_out.start()
    for cp in outs:
        cp.wait()


def copy_out(c_rows):
    return pl.pallas_call(
        copy_kernel,
        name="copy_out",
        out_shape=jax.ShapeDtypeStruct(c_rows.shape, c_rows.dtype),
        in_specs=[pl.BlockSpec(memory_space=pl.ANY)],
        out_specs=pl.BlockSpec(memory_space=pl.ANY),
        scratch_shapes=[pltpu.VMEM(c_rows.shape, c_rows.dtype), pltpu.SemaphoreType.DMA((COPIES,)),
                        pltpu.SemaphoreType.DMA((COPIES,))],
    )(c_rows)


def local_product(nz, ny, a_blk, b_blk):
    rows, depth_k = a_blk.shape
    half_k = b_blk.shape[0]
    width = depth_k // nz
    f32, bf16 = jnp.float32, jnp.bfloat16
    dma = pltpu.SemaphoreType.DMA
    n = len(PIECES)
    return copy_out(pl.pallas_call(
        functools.partial(kernel, nz, ny),
        name="stationary_a",
        out_shape=jax.ShapeDtypeStruct((rows // nz, depth_k), bf16),
        in_specs=[pl.BlockSpec(memory_space=pl.ANY)] * 2,
        out_specs=pl.BlockSpec(memory_space=pl.ANY),
        scratch_shapes=[
            pltpu.VMEM((rows, depth_k), bf16),
            pltpu.VMEM((NX, 2 * half_k, width), bf16),
            pltpu.VMEM((2, rows // 2, width), f32),
            pltpu.VMEM((2, rows, width), f32),
            pltpu.VMEM((3, rows, width), f32),
            pltpu.VMEM((rows, width), bf16),
            dma,
            dma,
            dma((n, 4)),
            dma((n,)),
            dma((NG,)),
            dma((NG, 2)),
            dma,
            dma((2, NG, nz)),
            dma,
            dma,
            dma((NG,)),
        ],
        compiler_params=pltpu.CompilerParams(collective_id=0, has_side_effects=True, vmem_limit_bytes=67043328),
    )(a_blk, b_blk))


def solution(mesh):
    nz, ny = mesh.shape["depth"], mesh.shape["col"]
    return jax.shard_map(
        functools.partial(local_product, nz, ny),
        mesh=mesh,
        in_specs=(P("row", "col"), P("row", "col")),
        out_specs=P(("row", "depth"), "col"),
        check_vma=False,
    )
```

```python
import functools

import jax
import jax.numpy as jnp
from jax import lax
from jax.experimental import pallas as pl
from jax.experimental.pallas import tpu as pltpu
from jax.sharding import PartitionSpec as P

MESH = pl.DeviceIdType.MESH
NX = 4
PIECES = [(2, 0), (2, 1), (2, 2), (1, 0), (3, 0), (1, 1), (3, 1), (1, 2), (3, 2), (0, 3), (0, 2)]
GROUPS = [(0, 4), (4, 4), (8, 8), (0, 8)]
NG = 3
SLOT = {2: 0, 1: 1, 3: 2, 0: 0}
SCRIPT = """P0 P1 G0 P2 P3 P4 G1 P5 P6 L0 R0 O0 C0a G2 C0b G3 G4 P7 P8 L1 R1 O1 C1a C1b G5 G6 P9 P10 L2 R2 O2 C2a C2b
L3 R3 O3 C3a L4 R4 O4 C3b C4a C4b A0 G9 G7 G8 L5 R5 O5 C5a L6 R6 O6 C5b C6a C6b A1 G10 L9 R9 O9 C9a C9b F0
L7 R7 O7 C7a L8 R8 O8 C7b C8a C8b A2 F1 L10 R10 O10 C10a C10b W F2"""


def chunk_order(nz):
    return sorted(range(nz), key=lambda r: -min(r, nz - r))


def kernel(nz, ny, a_ref, b_ref, o_ref, abuf, bbuf, ro, rn, pbuf, obuf,
           a_sem, b_send, b_recv, s_recv, op_send, op_recv, nb_send, nb_recv, out_send, out_recv, own_sem):
    z = lax.axis_index("depth")
    y = lax.axis_index("col")
    i = lax.axis_index("row")
    x, c = i // 2, i % 2
    rows, depth_k = abuf.shape
    half_k = depth_k // 2
    quarter = half_k // NX
    width = depth_k // nz
    unit = width // 16
    chunk = rows // nz
    mblk = rows // 4
    half = rows // 2
    order_z = chunk_order(nz)

    def dev(zz, yy, xx, cc):
        return ((zz + nz) % nz, (yy + ny) % ny, 2 * ((xx + NX) % NX) + cc)

    def remote(src, dst, send_sem, recv_sem, device):
        return pltpu.make_async_remote_copy(src_ref=src, dst_ref=dst, send_sem=send_sem, recv_sem=recv_sem,
                                            device_id=device, device_id_type=MESH)

    sibling = dev(z, y, x, 1 - c)
    left, right, far = dev(z, y, x - 1, c), dev(z, y, x + 1, c), dev(z, y, x + 2, c)

    a_copies = [pltpu.make_async_copy(a_ref.at[pl.ds(m * mblk, mblk)], abuf.at[pl.ds(m * mblk, mblk)], a_sem)
                for m in range(4)]
    for cp in a_copies:
        cp.start()

    barrier = pltpu.get_barrier_semaphore()
    partners = [sibling]
    partners += [dev(z, y + dy, x + dx, c) for dy in range(ny) for dx in range(NX) if dx or dy]
    partners += [dev(z + r, y, x, c) for r in range(1, nz)]
    for p in partners:
        pl.semaphore_signal(barrier, inc=1, device_id=p, device_id_type=MESH)
    pl.semaphore_wait(barrier, len(partners))

    t_me = (y - x + NX) % NX

    def group_columns(s):
        return pl.ds(GROUPS[s][0] * unit, GROUPS[s][1] * unit)

    def columns(n):
        return group_columns(PIECES[n][1])

    def stage1(n, d):
        t, group = PIECES[n]
        first, wide = GROUPS[group]
        q = (x + d) % NX
        cols = pl.ds(pl.multiple_of(z * width + first * unit, 4 * unit), wide * unit)
        src = b_ref.at[pl.ds(pl.multiple_of(q * quarter, quarter), quarter), cols]
        dst = bbuf.at[t, pl.ds(pl.multiple_of(c * half_k + q * quarter, quarter), quarter), columns(n)]
        if t == 0 and d == 0:
            return pltpu.make_async_copy(src, dst, b_recv.at[n, 0])
        return remote(src, dst, b_send, b_recv.at[n, 0], dev(z, x, q, c))

    def stage1_start(n, ds):
        @pl.when(t_me == PIECES[n][0])
        def _():
            for d in ds:
                stage1(n, d).start()

    def part(n, k):
        q = (x + (0, 3, 1, 2)[k]) % NX
        start = c * half_k + q * quarter
        return bbuf.at[PIECES[n][0], pl.ds(pl.multiple_of(start, quarter), quarter), columns(n)]

    def lane(n, cc):
        return bbuf.at[PIECES[n][0], pl.ds(pl.multiple_of(cc * half_k, half_k), half_k), columns(n)]

    def arrived(n, k):
        ref = part(n, k)
        remote(ref, ref, b_send, b_recv.at[n, k], sibling).wait_recv()

    def to_sibling(n, k):
        ref = part(n, k)
        remote(ref, ref, b_send, s_recv.at[n], sibling).start()

    def pass_own(n):
        arrived(n, 0)
        ref = part(n, 0)
        for k, target in ((3, far), (1, right), (2, left)):
            remote(ref, ref, b_send, b_recv.at[n, k], target).start()
        to_sibling(n, 0)

    def pass_on(n, k):
        arrived(n, k)
        to_sibling(n, k)

    def group_columns(s):
        return pl.ds(GROUPS[s][0] * unit, GROUPS[s][1] * unit)

    def opposite_copy(s, d, h):
        src = pbuf.at[0, pl.ds(pl.multiple_of(d * half + h * mblk, mblk), mblk), group_columns(s)]
        return remote(src, ro.at[d, pl.ds(h * mblk, mblk), group_columns(s)], op_send.at[s], op_recv.at[s, d],
                      dev(z, y + 1 - 2 * d, x, c))

    def half_matmul(n, h):
        t, group = PIECES[n]
        if h == 0:
            ref = lane(n, 1 - c)
            remote(ref, ref, b_send, s_recv.at[n], sibling).wait_recv()
            if n == 0:
                pltpu.make_async_copy(abuf, abuf, a_sem).wait()
            if t == 0:
                for m in (0, 1) if group == 3 else (2,):
                    ref = pbuf.at[0, :, group_columns(m)]
                    remote(ref, ref, op_send.at[m], op_recv.at[m, 0], sibling).wait_send()

        def body(d, carry):
            r = pl.ds(pl.multiple_of(d * half + h * mblk, mblk), mblk)
            pbuf[SLOT[t], r, columns(n)] = jnp.dot(abuf[r, :], bbuf[t, :, columns(n)],
                                                   preferred_element_type=jnp.float32)
            if t == 2:
                opposite_copy(group, d, h).start()
            return carry

        lax.fori_loop(0, 2, body, 0)

    def chunk_rows(zz):
        return pl.ds(pl.multiple_of(zz * chunk, chunk), chunk)

    def neighbour_copy(d, s, zz):
        cr, cols = chunk_rows(zz), group_columns(s)
        return remote(pbuf.at[1 + d, cr, cols], rn.at[d, cr, cols], nb_send, nb_recv.at[d, s, zz],
                      dev(z, y + 1 - 2 * d, x, c))

    def send_half(s, merged):
        nh = max(nz // 2, 1)
        for j in range(nh):
            for d in (0, 1):
                neighbour_copy(d, s, ((d if merged else 1 - d) * nh + (z + j) % nh) % nz).start()

    def merge(s):
        cols = group_columns(s)
        for d in (0, 1):
            ref = ro.at[d, :, group_columns(s)]
            remote(ref, ref, op_send.at[s], op_recv.at[s, d], sibling).wait_recv()
        for d in (0, 1):
            def body(m, carry):
                r = pl.ds(pl.multiple_of(m * (half // 4), half // 4), half // 4)
                rp = pl.ds(pl.multiple_of(d * half + m * (half // 4), half // 4), half // 4)
                pbuf[1 + d, rp, cols] = pbuf[1 + d, rp, cols] + ro[d, r, cols]
                return carry

            lax.fori_loop(0, 4, body, 0)

    def send_all(s):
        for r in order_z:
            for d in (0, 1):
                neighbour_copy(d, s, (z + r) % nz).start()

    def out_columns(zz, s):
        return pl.ds(pl.multiple_of(zz * width + GROUPS[s][0] * unit, 4 * unit), GROUPS[s][1] * unit)

    def out_copy(s, r):
        src = obuf.at[chunk_rows((z + r) % nz), group_columns(s)]
        dst = o_ref.at[:, out_columns(z, s)]
        if r == 0:
            return pltpu.make_async_copy(src, dst, own_sem.at[s])
        return remote(src, dst, out_send, out_recv, dev(z + r, y, x, c))

    def finish(s):
        cols = group_columns(s)
        for r in order_z:
            for d in (0, 1):
                neighbour_copy(d, s, (z + r) % nz).wait_recv()
            cr = chunk_rows((z + r) % nz)
            total = pbuf[0, cr, cols] + rn[0, cr, cols] + rn[1, cr, cols]
            obuf[cr, cols] = total.astype(jnp.bfloat16)
            out_copy(s, r).start()

    for item in SCRIPT.split():
        op, rest = item[0], item[1:]
        if op == "P":
            stage1_start(int(rest), (0, 2, 1, 3))
        elif op == "G":
            pass_own(int(rest))
        elif op == "L":
            pass_on(int(rest), 1)
        elif op == "R":
            pass_on(int(rest), 2)
        elif op == "O":
            pass_on(int(rest), 3)
        elif op == "C":
            half_matmul(int(rest[:-1]), "ab".index(rest[-1]))
        elif op == "U":
            send_half(int(rest), False)
        elif op == "M":
            merge(int(rest))
            send_half(int(rest), True)
        elif op == "A":
            merge(int(rest))
            send_all(int(rest))
        elif op == "F":
            finish(int(rest))
        elif op == "W":
            @pl.when(t_me != 0)
            def _():
                remote(bbuf, bbuf, b_send, out_recv, sibling).wait_send()

            @pl.when(t_me == 0)
            def _():
                ref = bbuf.at[:, pl.ds(0, 2 * half_k - quarter // NX)]
                remote(ref, ref, b_send, out_recv, sibling).wait_send()

    remote(rn, rn, nb_send, out_recv, sibling).wait_send()
    for s in range(NG):
        out_copy(s, 0).wait()
    sent = obuf.at[pl.ds(0, rows - chunk)]
    remote(sent, sent, out_send, out_recv, sibling).wait_send()
    got = o_ref.at[pl.ds(0, chunk - chunk // nz)]
    remote(got, got, out_send, out_recv, sibling).wait_recv()


COPIES = 4


def copy_kernel(src_ref, dst_ref, buf, in_sem, out_sem):
    n = buf.shape[0] // COPIES
    blocks = [pl.ds(m * n, n) for m in range(COPIES)]
    ins = [pltpu.make_async_copy(src_ref.at[b], buf.at[b], in_sem.at[m]) for m, b in enumerate(blocks)]
    outs = [pltpu.make_async_copy(buf.at[b], dst_ref.at[b], out_sem.at[m]) for m, b in enumerate(blocks)]
    for cp in ins:
        cp.start()
    for cp_in, cp_out in zip(ins, outs):
        cp_in.wait()
        cp_out.start()
    for cp in outs:
        cp.wait()


def copy_out(c_rows):
    return pl.pallas_call(
        copy_kernel,
        name="copy_out",
        out_shape=jax.ShapeDtypeStruct(c_rows.shape, c_rows.dtype),
        in_specs=[pl.BlockSpec(memory_space=pl.ANY)],
        out_specs=pl.BlockSpec(memory_space=pl.ANY),
        scratch_shapes=[pltpu.VMEM(c_rows.shape, c_rows.dtype), pltpu.SemaphoreType.DMA((COPIES,)),
                        pltpu.SemaphoreType.DMA((COPIES,))],
    )(c_rows)


def local_product(nz, ny, a_blk, b_blk):
    rows, depth_k = a_blk.shape
    half_k = b_blk.shape[0]
    width = depth_k // nz
    f32, bf16 = jnp.float32, jnp.bfloat16
    dma = pltpu.SemaphoreType.DMA
    n = len(PIECES)
    return copy_out(pl.pallas_call(
        functools.partial(kernel, nz, ny),
        name="stationary_a",
        out_shape=jax.ShapeDtypeStruct((rows // nz, depth_k), bf16),
        in_specs=[pl.BlockSpec(memory_space=pl.ANY)] * 2,
        out_specs=pl.BlockSpec(memory_space=pl.ANY),
        scratch_shapes=[
            pltpu.VMEM((rows, depth_k), bf16),
            pltpu.VMEM((NX, 2 * half_k, width), bf16),
            pltpu.VMEM((2, rows // 2, width), f32),
            pltpu.VMEM((2, rows, width), f32),
            pltpu.VMEM((3, rows, width), f32),
            pltpu.VMEM((rows, width), bf16),
            dma,
            dma,
            dma((n, 4)),
            dma((n,)),
            dma((NG,)),
            dma((NG, 2)),
            dma,
            dma((2, NG, nz)),
            dma,
            dma,
            dma((NG,)),
        ],
        compiler_params=pltpu.CompilerParams(collective_id=0, has_side_effects=True, vmem_limit_bytes=67043328),
    )(a_blk, b_blk))


def solution(mesh):
    nz, ny = mesh.shape["depth"], mesh.shape["col"]
    return jax.shard_map(
        functools.partial(local_product, nz, ny),
        mesh=mesh,
        in_specs=(P("row", "col"), P("row", "col")),
        out_specs=P(("row", "depth"), "col"),
        check_vma=False,
    )
```
